32 devices in a mesh: segment: 4 (over y, x), amp: 8 (over z, core).
Axes of the slice: x: 2, y: 2, z: 4, core: 2. Of those that a mesh axis runs over, the one named last changes fastest.
Arguments:
- states: float32 [4, 2097152], P('segment', 'amp'), may hold values from -6 to 6
- gate_blocks: float32 [4, 3, 128, 128], P('segment'), may hold values from -1 to 1, as said below
- kraus_picks: int32 [4, 4, 3, 7], P('segment'), may hold values from 0 to 3
- block_targets: int32 [4, 3], replicated, may hold values from 0 to 1
Outputs:
- final_states: float32 [4, 2097152], P('segment', 'amp')
- log_weights: float32 [4, 4], P('segment')
The draws below stay inside these ranges and needn't reach their ends.
Inputs may be any that keep to these rules, and one draw needn't show every extreme that they name: Every block of gate_blocks is an orthogonal matrix, up to rounding.
All inputs are finite; a program needn't handle non-finite values.
Results may differ from the reference program's by a relative error of at most 0.0003.
Values sent between devices are 32-bit elements; how exact they have to be, the bound alone decides.
A program may use at most 64 MiB of HBM per device.

```python
import jax
import jax.numpy as jnp
from jax import lax

QB = 7
REG = 128
MIDC = 16
BLOCKS = 3
SECTIONS = 4
TRAJ = 4
GLOBALS = 8
AMPS = 2097152


def draw_gate_blocks(key, part):
    gaussian = jax.random.normal(key, (SECTIONS, BLOCKS, REG, REG), jnp.float32)
    q_factor, r_factor = jnp.linalg.qr(gaussian)
    return q_factor.astype(jnp.float32)


def place_ends(array, key, low, largest):
    place = [jax.random.randint(jax.random.fold_in(key, axis), (), 0, length) for axis, length in enumerate(array.shape)]
    main_axis = array.shape.index(max(array.shape))
    beside = place[:main_axis] + [(place[main_axis] + 1) % array.shape[main_axis]] + place[main_axis + 1:]
    return array.at[tuple(place)].set(low).at[tuple(beside)].set(largest)


def level_of(rng, extent, shards, smallest, largest):
    factor_of = 1.0
    for axis_at, shards_of in shards:
        heights = jax.random.uniform(jax.random.fold_in(jax.random.fold_in(rng, 6), axis_at), (shards_of,), jnp.float32, smallest / len(shards), largest / len(shards))
        factor_of = factor_of * jnp.repeat(jnp.exp(heights), extent[axis_at] // shards_of).reshape((-1,) + (1,) * (len(extent) - 1 - axis_at))
    return factor_of


def normal_values(own_key, extent, deviation, most, cuts=(), kind=jnp.bfloat16):
    gain = level_of(own_key, extent, cuts, -0.22, 0.18) if cuts else 1.0
    values = jax.random.normal(own_key, extent, jnp.float32) * deviation * gain
    return jnp.minimum(jnp.maximum(values, -most), most).astype(kind)


def setup_inputs(seed: int = 0) -> dict:
    arg_keys = jax.random.split(jax.random.key(seed), 5)
    states = normal_values(arg_keys[0], (TRAJ, AMPS), 1.0, 6.0, ((0, 4), (1, 8)), jnp.float32)
    gate_blocks = draw_gate_blocks(jax.random.fold_in(arg_keys[4], 71), 0)
    kraus_picks = place_ends(jax.random.randint(arg_keys[2], (TRAJ, SECTIONS, BLOCKS, QB), 0, 4), jax.random.fold_in(arg_keys[2], 1), 0, 3).astype(jnp.int32)
    block_targets = place_ends(jax.random.randint(arg_keys[3], (SECTIONS, BLOCKS), 0, 2), jax.random.fold_in(arg_keys[3], 1), 0, 1).astype(jnp.int32)
    return {"states": states, "gate_blocks": gate_blocks, "kraus_picks": kraus_picks, "block_targets": block_targets}


KEEP_FACTORS = (1.0, 0.9, 1.0, 0.97)
FLIP_FACTORS = (0.9, 1.0, 0.97, 1.0)

def noise_factors(kraus_rows):
    qubit_count = kraus_rows.shape[-1]
    register = 2 ** qubit_count
    positions = jnp.arange(register, dtype=jnp.int32)
    product = jnp.ones(kraus_rows.shape[:-1] + (register,), jnp.float32)
    for qubit_pos in range(qubit_count):
        bit_value = jnp.right_shift(positions, qubit_count - 1 - qubit_pos) & 1
        column = kraus_rows[..., qubit_pos:qubit_pos + 1]
        low_value = jnp.zeros(column.shape, jnp.float32)
        high_value = jnp.zeros(column.shape, jnp.float32)
        for option in range(4):
            picked = (column == option).astype(jnp.float32)
            low_value = low_value + picked * KEEP_FACTORS[option]
            high_value = high_value + picked * FLIP_FACTORS[option]
        product = product * jnp.where(bit_value == 1, high_value, low_value)
    return product

def apply_gate(amplitudes, matrix, factors, target):

    def on_low(values):
        mixed_rows = jnp.einsum('bghmk,ik->bghmi', values, matrix, precision=lax.Precision.HIGHEST)
        return mixed_rows * factors[:, None, None, None, :]

    def on_high(values):
        mixed_rows = jnp.einsum('bgjmk,ij->bgimk', values, matrix, precision=lax.Precision.HIGHEST)
        return mixed_rows * factors[:, None, :, None, None]
    return lax.cond(target == 0, on_low, on_high, amplitudes)

def swap_global(amplitudes):
    traj_all, global_count, register, middle, low_count = amplitudes.shape
    split_view = amplitudes.reshape(traj_all, global_count, global_count, register // global_count, middle, low_count)
    swapped = jnp.swapaxes(split_view, 1, 2)
    return swapped.reshape(traj_all, global_count, register, middle, low_count)

def reference(states, gate_blocks, kraus_picks, block_targets):
    register = gate_blocks.shape[-1]
    amplitudes = states.reshape(TRAJ, GLOBALS, register, MIDC, register)
    mean_sq = lax.optimization_barrier(jnp.mean(amplitudes * amplitudes, axis=(1, 2, 3, 4)))
    amplitudes = amplitudes / jnp.sqrt(mean_sq)[:, None, None, None, None]
    log_list = []
    for section in range(SECTIONS):
        for block_pos in range(BLOCKS):
            factors = noise_factors(kraus_picks[:, section, block_pos, :])
            amplitudes = apply_gate(amplitudes, gate_blocks[section, block_pos], factors, block_targets[section, block_pos])
        amplitudes = swap_global(amplitudes)
        mean_sq = lax.optimization_barrier(jnp.mean(amplitudes * amplitudes, axis=(1, 2, 3, 4)))
        log_list.append(jnp.log(mean_sq))
        amplitudes = amplitudes / jnp.sqrt(mean_sq)[:, None, None, None, None]
    return (amplitudes.reshape(TRAJ, AMPS), jnp.stack(log_list, axis=1))
```

```python
import functools

import jax
import jax.numpy as jnp
from jax import lax
from jax.experimental import pallas as pl
from jax.experimental.pallas import tpu as pltpu
from jax.sharding import PartitionSpec as P

KEEP_FACTORS = (1.0, 0.9, 1.0, 0.97)
FLIP_FACTORS = (0.9, 1.0, 0.97, 1.0)
MESH = pl.DeviceIdType.MESH


def broadcast(block, axis, owner):
    block = jnp.where(lax.axis_index(axis) == owner, block, jnp.zeros_like(block))
    return lax.psum(block, axis)


def noise_factors(kraus_rows):
    qubit_count = kraus_rows.shape[-1]
    register = 2**qubit_count
    positions = jnp.arange(register, dtype=jnp.int32)
    product = jnp.ones(kraus_rows.shape[:-1] + (register,), jnp.float32)
    for qubit_pos in range(qubit_count):
        bit_value = jnp.right_shift(positions, qubit_count - 1 - qubit_pos) & 1
        column = kraus_rows[..., qubit_pos : qubit_pos + 1]
        low_value = jnp.zeros(column.shape, jnp.float32)
        high_value = jnp.zeros(column.shape, jnp.float32)
        for option in range(4):
            picked = (column == option).astype(jnp.float32)
            low_value = low_value + picked * KEEP_FACTORS[option]
            high_value = high_value + picked * FLIP_FACTORS[option]
        product = product * jnp.where(bit_value == 1, high_value, low_value)
    return product


def apply_gate(amplitudes, matrix, factors, target):

    def on_low(values):
        mixed_rows = jnp.einsum("bhmk,ik->bhmi", values, matrix, precision=lax.Precision.HIGHEST)
        return mixed_rows * factors[:, None, None, :]

    def on_high(values):
        mixed_rows = jnp.einsum("bjmk,ij->bimk", values, matrix, precision=lax.Precision.HIGHEST)
        return mixed_rows * factors[:, :, None, None]

    return lax.cond(target == 0, on_low, on_high, amplitudes)


def square_sums(values):
    return (values, jnp.sum(values * values, axis=(1, 2, 3)))


def body(states, gate_blocks, kraus_picks, block_targets):
    traj_here = states.shape[0]
    amp_local = states.shape[1]
    register = gate_blocks.shape[-1]
    blocks = gate_blocks.shape[1]
    middle = amp_local // (register * register)
    total_amps = amp_local * lax.axis_size("amp")
    sections = lax.axis_size("segment")
    amplitudes = states.reshape(traj_here, register, middle, register)
    first_local = jnp.sum(amplitudes * amplitudes, axis=(1, 2, 3))
    local_sums = [first_local]
    for section in range(sections):
        section_gates = broadcast(gate_blocks, "segment", section)[0]
        for block_pos in range(blocks):
            factors = noise_factors(kraus_picks[:, section, block_pos, :])
            amplitudes = apply_gate(
                amplitudes, section_gates[block_pos], factors, block_targets[section, block_pos]
            )
        amplitudes, local_sq = square_sums(
            lax.all_to_all(amplitudes, "amp", split_axis=1, concat_axis=1, tiled=True)
        )
        local_sums.append(local_sq)
    totals = lax.psum(jnp.stack(local_sums, axis=1), "amp")
    log_weights = jnp.log(totals[:, 1:] / totals[:, :-1])
    amplitudes = amplitudes / jnp.sqrt(totals[:, -1] / total_amps)[:, None, None, None]
    return (amplitudes.reshape(traj_here, amp_local), log_weights)


def partner(index, k):
    result = index
    bit = 1
    while bit <= k:
        if k & bit:
            result = result + bit * (1 - 2 * ((index // bit) % 2))
        bit *= 2
    return result


def split(values):
    high = values.astype(jnp.bfloat16)
    low = (values - high.astype(jnp.float32)).astype(jnp.bfloat16)
    return high, low


def left_form(matrix):
    return jnp.concatenate(split(matrix), axis=1)


def right_form(matrix):
    row = jnp.concatenate(split(matrix), axis=1)
    return jnp.concatenate([row, row], axis=0)


def multiply(left, right):
    both = jnp.dot(left, right, preferred_element_type=jnp.float32)
    half = both.shape[1] // 2
    return both[:, :half] + both[:, half:]


def fold_rows(values):
    squares = values * values
    return jnp.sum(squares.reshape(-1, 8, squares.shape[-1]), axis=0)


def row_factors(picks_ref, section, block, qubits, shape):
    positions = lax.broadcasted_iota(jnp.int32, shape, 0)
    product = jnp.ones(shape, jnp.float32)
    for q in range(qubits):
        pick = picks_ref[0, block, section, q]
        keep = jnp.float32(KEEP_FACTORS[0])
        flip = jnp.float32(FLIP_FACTORS[0])
        for option in range(1, 4):
            keep = jnp.where(pick == option, jnp.float32(KEEP_FACTORS[option]), keep)
            flip = jnp.where(pick == option, jnp.float32(FLIP_FACTORS[option]), flip)
        bit = jnp.right_shift(positions, qubits - 1 - q) & 1
        product = product * jnp.where(bit == 1, flip, keep)
    return product


def waits(like, semaphore):
    pltpu.make_async_copy(like, like, semaphore).wait()


def circuit_kernel(
    peers, sections, blocks, qubits, chunks, total_amps,
    x_hbm, gates_hbm, picks_hbm, targets_hbm,
    out_ref, logs_ref,
    xs, yin, ov, gates, picks, targets, low_form, high_form, partial, sums,
    x_sem, own_sem, gate_sem, small_sem, gsend, grecv, isend, irecv, osend, orecv, ssend, srecv,
    entered,
):
    seg = lax.axis_index("segment")
    amp = lax.axis_index("amp")
    reg = gates.shape[-1]
    middle = chunks * peers
    far = list(range(3 * peers // 4, peers))
    mid = list(range(peers // 2, 3 * peers // 4))
    near = list(range(peers // 2 - 1, 0, -1))
    groups = [far, mid, near]

    def tell(semaphore, axis, index, k):
        pl.semaphore_signal(
            semaphore, inc=1, device_id={axis: partner(index, k)}, device_id_type=MESH
        )

    barrier = pltpu.get_barrier_semaphore()
    line = peers == 8 and sections == 4
    pair_at = amp // 2
    inner_pair = (pair_at + 1) // 2 % 2
    is_inner = inner_pair == 1
    if line:

        @pl.when(is_inner)
        def _():
            tell(barrier, "amp", amp, 6)
            tell(barrier, "amp", amp, 7)

        for k in (3, 2, 1):
            tell(barrier, "amp", amp, k)
        for k in (1, 2):
            tell(barrier, "segment", seg, k)
    else:
        for k in range(peers - 1, 0, -1):
            tell(barrier, "amp", amp, k)
        for k in range(1, sections):
            tell(barrier, "segment", seg, k)

    def load(chunk, k, semaphore):
        m = chunk * peers + partner(amp, k)
        pltpu.make_async_copy(x_hbm.at[:, m, 0], xs.at[chunk, k - 1], semaphore).start()

    for g, group in enumerate(groups):
        for k in group:
            load(0, k, x_sem.at[g])
    for chunk in range(1, chunks):
        for group in groups:
            for k in group:
                load(chunk, k, x_sem.at[len(groups)])
    gate_load = pltpu.make_async_copy(gates_hbm, gates.at[seg], gate_sem)
    gate_load.start()
    picks_load = pltpu.make_async_copy(picks_hbm, picks, small_sem.at[0])
    picks_load.start()
    targets_load = pltpu.make_async_copy(targets_hbm, targets, small_sem.at[1])
    targets_load.start()
    for chunk in range(chunks):
        pltpu.make_async_copy(
            x_hbm.at[:, chunk * peers + amp, 0], yin.at[chunk, amp], own_sem
        ).start()

    def send_in(chunk, k):
        pltpu.make_async_remote_copy(
            src_ref=xs.at[chunk, k - 1],
            dst_ref=yin.at[chunk, amp],
            send_sem=isend,
            recv_sem=irecv.at[chunk],
            device_id={"amp": partner(amp, k)},
            device_id_type=MESH,
        ).start()

    def loaded(g):
        slots = [k - 1 for k in groups[g]]
        waits(xs.at[0, min(slots) : max(slots) + 1], x_sem.at[g])

    with jax.named_scope("load0"):
        loaded(0)
    if line:
        with jax.named_scope("barrier"):
            pl.semaphore_wait(barrier, 5 + 2 * inner_pair)

        @pl.when(is_inner)
        def _():
            tell(entered.at[0], "amp", amp, 2)
            tell(entered.at[0], "amp", amp, 6)
            send_in(0, 6)
            send_in(0, 7)

        tell(entered.at[2], "segment", seg, 1)
        loaded(1)
        loaded(2)
        with jax.named_scope("ent0"):
            pl.semaphore_wait(entered.at[0], 1)

        @pl.when(is_inner)
        def _():
            tell(entered.at[1], "amp", amp, 2)

        send_in(0, 4)
        send_in(0, 5)

        @pl.when(jnp.logical_not(is_inner))
        def _():
            with jax.named_scope("ent1"):
                pl.semaphore_wait(entered.at[1], 1)
            send_in(0, 6)
            send_in(0, 7)

        for k in near:
            send_in(0, k)
        with jax.named_scope("ent2"):
            pl.semaphore_wait(entered.at[2], 1)
    else:
        pl.semaphore_wait(barrier, peers - 1 + sections - 1)
        loaded(1)
        loaded(2)
        for group in groups:
            for k in group:
                send_in(0, k)
    gate_load.wait()
    for k in range(1, sections):
        pltpu.make_async_remote_copy(
            src_ref=gates.at[seg],
            dst_ref=gates.at[seg],
            send_sem=gsend,
            recv_sem=grecv,
            device_id={"segment": partner(seg, k)},
            device_id_type=MESH,
        ).start()
    if chunks > 1:
        waits(xs.at[1:], x_sem.at[len(groups)])
    for chunk in range(1, chunks):
        for group in groups:
            for k in group:
                send_in(chunk, k)
    picks_load.wait()
    targets_load.wait()
    with jax.named_scope("gates"):
        waits(gates.at[1:], grecv)

    rows_at = lax.broadcasted_iota(jnp.int32, (reg, reg), 0)
    columns_at = lax.broadcasted_iota(jnp.int32, (reg, reg), 1)
    identity = jnp.where(rows_at == columns_at, jnp.float32(1.0), jnp.float32(0.0))

    def build(section, carry):
        low = high = None
        for b in range(blocks):
            factors = row_factors(picks, section, b, qubits, (reg, reg))
            damped = gates[section, b] * factors
            is_low = targets[section, b] == 0
            for_low = jnp.where(is_low, damped, identity)
            for_high = jnp.where(is_low, identity, damped)
            if b == 0:
                low, high = for_low, for_high
            else:
                low = multiply(left_form(for_low), right_form(low))
                high = multiply(left_form(for_high), right_form(high))
        low_form[section] = right_form(low.T)
        high_form[section] = left_form(high)
        return carry

    with jax.named_scope("build"):
        lax.fori_loop(0, sections, build, 0)

    inner = reg // peers
    partial[...] = jnp.zeros_like(partial)

    def apply_section(chunk, section, swapped):
        low = low_form[section]
        high = high_form[section]
        total = jnp.zeros((8, reg), jnp.float32)
        for slab in range(peers):
            if swapped:
                value = yin[chunk, :, slab * inner : (slab + 1) * inner, :].reshape(reg, reg)
            else:
                value = yin[chunk, slab]
            value = multiply(left_form(value), low)
            value = multiply(high, right_form(value))
            total = total + fold_rows(value)
            if swapped:
                yin[chunk, :, slab * inner : (slab + 1) * inner, :] = value.reshape(
                    peers, inner, reg
                )
            else:
                yin[chunk, slab] = value
        partial[section + 1] = partial[section + 1] + total

    waits(ov.at[:, 0], own_sem)
    order_out = mid + far + near

    def run_chunk(chunk, carry):
        with jax.named_scope("in"):
            waits(xs.at[chunk], irecv.at[chunk])
        first = jnp.zeros((8, reg), jnp.float32)
        for slab in range(peers):
            first = first + fold_rows(yin[chunk, slab])
        partial[0] = partial[0] + first

        def pair(i, inner_carry):
            apply_section(chunk, 2 * i, False)
            apply_section(chunk, 2 * i + 1, True)
            return inner_carry

        with jax.named_scope("comp"):
            lax.fori_loop(0, sections // 2, pair, 0)

        @pl.when(chunk == chunks - 1)
        def _():
            for s in range(sections + 1):
                sums[amp, s : s + 1, :] = jnp.sum(partial[s], axis=0, keepdims=True)
            for k in range(peers - 1, 0, -1):
                pltpu.make_async_remote_copy(
                    src_ref=sums.at[amp],
                    dst_ref=sums.at[amp],
                    send_sem=ssend,
                    recv_sem=srecv,
                    device_id={"amp": partner(amp, k)},
                    device_id_type=MESH,
                ).start()

        for k in order_out:
            g = [k in group for group in groups].index(True)
            peer = partner(amp, k)
            pltpu.make_async_remote_copy(
                src_ref=yin.at[chunk, peer],
                dst_ref=ov.at[chunk, amp],
                send_sem=osend,
                recv_sem=orecv.at[chunk, g],
                device_id={"amp": peer},
                device_id_type=MESH,
            ).start()
        return carry

    lax.fori_loop(0, chunks, run_chunk, 0)

    with jax.named_scope("sums"):
        waits(sums.at[1:], srecv)
    totals = []
    for s in range(sections + 1):
        total = sums[0, s : s + 1, :]
        for d in range(1, peers):
            total = total + sums[d, s : s + 1, :]
        totals.append(jnp.sum(total, axis=1, keepdims=True))
    lanes = lax.broadcasted_iota(jnp.int32, (1, reg), 1)
    logs = jnp.zeros((1, reg), jnp.float32)
    for s in range(sections):
        logs = jnp.where(lanes == s, jnp.log(totals[s + 1] / totals[s]), logs)
    logs_ref[...] = logs[:, :sections]
    scale = 1.0 / jnp.sqrt(totals[sections] / total_amps)
    scale = jnp.broadcast_to(scale, (1, reg))

    for chunk in range(chunks):
        m = chunk * peers + amp
        out_ref[pl.ds(m, reg, stride=middle), :] = yin[chunk, amp] * scale
    for chunk in range(chunks):
        for g in (2, 0, 1):
            with jax.named_scope(f"out{chunk}_{g}"):
                waits(xs.at[0, : len(groups[g])], orecv.at[chunk, g])
            for k in groups[g]:
                m = chunk * peers + partner(amp, k)
                out_ref[pl.ds(m, reg, stride=middle), :] = ov[chunk, partner(amp, k)] * scale

    with jax.named_scope("sendwait"):
        waits(xs, isend)
        waits(xs, osend)
        waits(gates.at[1:], gsend)
        waits(sums.at[1:], ssend)


def store_kernel(pieces, out_vmem, logs_vmem, out_hbm, logs_hbm, sems):
    rows = out_vmem.shape[0] // pieces
    copies = [pltpu.make_async_copy(logs_vmem, logs_hbm, sems.at[pieces])]
    for p in range(pieces):
        at = pl.ds(p * rows, rows)
        copies.append(pltpu.make_async_copy(out_vmem.at[at], out_hbm.at[at], sems.at[p]))
    for copy in copies:
        copy.start()
    for copy in copies:
        copy.wait()


def step(states, gate_blocks, kraus_picks, block_targets):
    traj_here, amp_local = states.shape
    reg = gate_blocks.shape[-1]
    blocks = gate_blocks.shape[1]
    qubits = kraus_picks.shape[-1]
    peers = lax.axis_size("amp")
    sections = lax.axis_size("segment")
    middle = amp_local // (reg * reg)
    fits = (
        traj_here == 1
        and gate_blocks.shape[0] == 1
        and middle % peers == 0
        and peers & (peers - 1) == 0
        and peers >= 8
        and sections & (sections - 1) == 0
        and sections % 2 == 0
        and sections < 8
        and reg == 128
        and reg % (8 * peers) == 0
    )
    if not fits:
        return body(states, gate_blocks, kraus_picks, block_targets)
    chunks = middle // peers
    kernel = functools.partial(
        circuit_kernel, peers, sections, blocks, qubits, chunks, amp_local * peers
    )
    f32 = jnp.float32
    dma = pltpu.SemaphoreType.DMA
    out, logs = pl.pallas_call(
        kernel,
        out_shape=(
            pltpu.VMEM((reg * middle, reg), f32),
            pltpu.VMEM((1, sections), f32),
        ),
        in_specs=[pl.BlockSpec(memory_space=pl.ANY)] * 4,
        out_specs=(
            pl.BlockSpec(memory_space=pltpu.VMEM),
            pl.BlockSpec(memory_space=pltpu.VMEM),
        ),
        scratch_shapes=[
            pltpu.VMEM((chunks, peers - 1, reg, reg), f32),
            pltpu.VMEM((chunks, peers, reg, reg), f32),
            pltpu.VMEM((chunks, peers, reg, reg), f32),
            pltpu.VMEM((sections, blocks, reg, reg), f32),
            pltpu.SMEM((1, blocks, sections, qubits), jnp.int32),
            pltpu.SMEM((sections, blocks), jnp.int32),
            pltpu.VMEM((sections, 2 * reg, 2 * reg), jnp.bfloat16),
            pltpu.VMEM((sections, reg, 2 * reg), jnp.bfloat16),
            pltpu.VMEM((sections + 1, 8, reg), f32),
            pltpu.VMEM((peers, 8, reg), f32),
            dma((4,)),
            dma,
            dma,
            dma((2,)),
            dma,
            dma,
            dma,
            dma((chunks,)),
            dma,
            dma((chunks, 3)),
            dma,
            dma,
            pltpu.SemaphoreType.REGULAR((3,)),
        ],
        compiler_params=pltpu.CompilerParams(collective_id=0, has_side_effects=True),
    )(
        states.reshape(reg, middle, 1, reg),
        gate_blocks[0],
        jnp.swapaxes(kraus_picks, 1, 2),
        block_targets,
    )
    pieces = 4
    out, logs = pl.pallas_call(
        functools.partial(store_kernel, pieces),
        out_shape=(
            jax.ShapeDtypeStruct(out.shape, f32),
            jax.ShapeDtypeStruct(logs.shape, f32),
        ),
        in_specs=[pl.BlockSpec(memory_space=pltpu.VMEM)] * 2,
        out_specs=(pl.BlockSpec(memory_space=pl.ANY),) * 2,
        scratch_shapes=[dma((pieces + 1,))],
    )(
        pltpu.with_memory_space_constraint(out, pltpu.VMEM),
        pltpu.with_memory_space_constraint(logs, pltpu.VMEM),
    )
    return out.reshape(1, amp_local), logs


def solution(mesh):
    in_specs = (
        P("segment", "amp"),
        P("segment", None, None, None),
        P("segment", None, None, None),
        P(),
    )
    out_specs = (P("segment", "amp"), P("segment", None))
    return jax.shard_map(step, mesh=mesh, in_specs=in_specs, out_specs=out_specs, check_vma=False)
```

```python
import functools

import jax
import jax.numpy as jnp
from jax import lax
from jax.experimental import pallas as pl
from jax.experimental.pallas import tpu as pltpu
from jax.sharding import PartitionSpec as P

KEEP_FACTORS = (1.0, 0.9, 1.0, 0.97)
FLIP_FACTORS = (0.9, 1.0, 0.97, 1.0)
MESH = pl.DeviceIdType.MESH


def broadcast(block, axis, owner):
    block = jnp.where(lax.axis_index(axis) == owner, block, jnp.zeros_like(block))
    return lax.psum(block, axis)


def noise_factors(kraus_rows):
    qubit_count = kraus_rows.shape[-1]
    register = 2**qubit_count
    positions = jnp.arange(register, dtype=jnp.int32)
    product = jnp.ones(kraus_rows.shape[:-1] + (register,), jnp.float32)
    for qubit_pos in range(qubit_count):
        bit_value = jnp.right_shift(positions, qubit_count - 1 - qubit_pos) & 1
        column = kraus_rows[..., qubit_pos : qubit_pos + 1]
        low_value = jnp.zeros(column.shape, jnp.float32)
        high_value = jnp.zeros(column.shape, jnp.float32)
        for option in range(4):
            picked = (column == option).astype(jnp.float32)
            low_value = low_value + picked * KEEP_FACTORS[option]
            high_value = high_value + picked * FLIP_FACTORS[option]
        product = product * jnp.where(bit_value == 1, high_value, low_value)
    return product


def apply_gate(amplitudes, matrix, factors, target):

    def on_low(values):
        mixed_rows = jnp.einsum("bhmk,ik->bhmi", values, matrix, precision=lax.Precision.HIGHEST)
        return mixed_rows * factors[:, None, None, :]

    def on_high(values):
        mixed_rows = jnp.einsum("bjmk,ij->bimk", values, matrix, precision=lax.Precision.HIGHEST)
        return mixed_rows * factors[:, :, None, None]

    return lax.cond(target == 0, on_low, on_high, amplitudes)


def square_sums(values):
    return (values, jnp.sum(values * values, axis=(1, 2, 3)))


def body(states, gate_blocks, kraus_picks, block_targets):
    traj_here = states.shape[0]
    amp_local = states.shape[1]
    register = gate_blocks.shape[-1]
    blocks = gate_blocks.shape[1]
    middle = amp_local // (register * register)
    total_amps = amp_local * lax.axis_size("amp")
    sections = lax.axis_size("segment")
    amplitudes = states.reshape(traj_here, register, middle, register)
    first_local = jnp.sum(amplitudes * amplitudes, axis=(1, 2, 3))
    local_sums = [first_local]
    for section in range(sections):
        section_gates = broadcast(gate_blocks, "segment", section)[0]
        for block_pos in range(blocks):
            factors = noise_factors(kraus_picks[:, section, block_pos, :])
            amplitudes = apply_gate(
                amplitudes, section_gates[block_pos], factors, block_targets[section, block_pos]
            )
        amplitudes, local_sq = square_sums(
            lax.all_to_all(amplitudes, "amp", split_axis=1, concat_axis=1, tiled=True)
        )
        local_sums.append(local_sq)
    totals = lax.psum(jnp.stack(local_sums, axis=1), "amp")
    log_weights = jnp.log(totals[:, 1:] / totals[:, :-1])
    amplitudes = amplitudes / jnp.sqrt(totals[:, -1] / total_amps)[:, None, None, None]
    return (amplitudes.reshape(traj_here, amp_local), log_weights)


def partner(index, k):
    result = index
    bit = 1
    while bit <= k:
        if k & bit:
            result = result + bit * (1 - 2 * ((index // bit) % 2))
        bit *= 2
    return result


def split(values):
    high = values.astype(jnp.bfloat16)
    low = (values - high.astype(jnp.float32)).astype(jnp.bfloat16)
    return high, low


def left_form(matrix):
    return jnp.concatenate(split(matrix), axis=1)


def right_form(matrix):
    row = jnp.concatenate(split(matrix), axis=1)
    return jnp.concatenate([row, row], axis=0)


def multiply(left, right):
    both = jnp.dot(left, right, preferred_element_type=jnp.float32)
    half = both.shape[1] // 2
    return both[:, :half] + both[:, half:]


def fold_rows(values):
    squares = values * values
    return jnp.sum(squares.reshape(-1, 8, squares.shape[-1]), axis=0)


def row_factors(picks_ref, section, block, qubits, shape):
    positions = lax.broadcasted_iota(jnp.int32, shape, 0)
    product = jnp.ones(shape, jnp.float32)
    for q in range(qubits):
        pick = picks_ref[0, block, section, q]
        keep = jnp.float32(KEEP_FACTORS[0])
        flip = jnp.float32(FLIP_FACTORS[0])
        for option in range(1, 4):
            keep = jnp.where(pick == option, jnp.float32(KEEP_FACTORS[option]), keep)
            flip = jnp.where(pick == option, jnp.float32(FLIP_FACTORS[option]), flip)
        bit = jnp.right_shift(positions, qubits - 1 - q) & 1
        product = product * jnp.where(bit == 1, flip, keep)
    return product


def waits(like, semaphore):
    pltpu.make_async_copy(like, like, semaphore).wait()


def circuit_kernel(
    peers, sections, blocks, qubits, chunks, total_amps,
    x_hbm, gates_hbm, picks_hbm, targets_hbm,
    out_ref, logs_ref,
    xs, yin, ov, gates, picks, targets, low_form, high_form, partial, sums,
    x_sem, gate_sem, small_sem, sent, grecv, irecv, orecv, srecv,
    entered,
):
    seg = lax.axis_index("segment")
    amp = lax.axis_index("amp")
    reg = gates.shape[-1]
    middle = chunks * peers
    far = list(range(3 * peers // 4, peers))
    mid = list(range(peers // 2, 3 * peers // 4))
    near = list(range(peers // 2 - 1, 0, -1))
    groups = [far, mid, near]

    def tell(semaphore, axis, index, k):
        pl.semaphore_signal(
            semaphore, inc=1, device_id={axis: partner(index, k)}, device_id_type=MESH
        )

    barrier = pltpu.get_barrier_semaphore()
    line = peers == 8 and sections == 4
    pair_at = amp // 2
    inner_pair = (pair_at + 1) // 2 % 2
    is_inner = inner_pair == 1
    late_inner = pair_at // 2 * inner_pair
    early_inner = (1 - pair_at // 2) * inner_pair
    if line:

        for k in (6, 7, 1):
            tell(barrier, "amp", amp, k)

        @pl.when(is_inner)
        def _():
            for k in (2, 3, 4, 5):
                tell(barrier, "amp", amp, k)

        @pl.when(late_inner == 0)
        def _():
            for k in (1, 2):
                tell(barrier, "segment", seg, k)
    else:
        for k in range(peers - 1, 0, -1):
            tell(barrier, "amp", amp, k)
        for k in range(1, sections):
            tell(barrier, "segment", seg, k)

    def load(chunk, k, semaphore):
        m = chunk * peers + partner(amp, k)
        pltpu.make_async_copy(x_hbm.at[:, m, 0], xs.at[chunk, k - 1], semaphore).start()

    for k in far:
        load(0, k, x_sem.at[0])
    for k in mid + near:
        load(0, k, x_sem.at[1])
    for chunk in range(1, chunks):
        for k in far + mid + near:
            load(chunk, k, x_sem.at[2])
    gate_load = pltpu.make_async_copy(gates_hbm, gates.at[seg], gate_sem)
    gate_load.start()
    picks_load = pltpu.make_async_copy(picks_hbm, picks, small_sem.at[0])
    picks_load.start()
    targets_load = pltpu.make_async_copy(targets_hbm, targets, small_sem.at[1])
    targets_load.start()
    for chunk in range(chunks):
        pltpu.make_async_copy(
            x_hbm.at[:, chunk * peers + amp, 0], yin.at[chunk, amp], x_sem.at[1]
        ).start()

    def send_in(chunk, k):
        pltpu.make_async_remote_copy(
            src_ref=xs.at[chunk, k - 1],
            dst_ref=yin.at[chunk, amp],
            send_sem=sent,
            recv_sem=irecv.at[chunk],
            device_id={"amp": partner(amp, k)},
            device_id_type=MESH,
        ).start()

    def far_loaded():
        waits(xs.at[0, : len(far)], x_sem.at[0])

    def near_loaded():
        waits(xs.at[0], x_sem.at[1])

    if line:
        with jax.named_scope("barrier"):
            pl.semaphore_wait(barrier, 9 - 4 * inner_pair - 2 * late_inner)

        @pl.when(late_inner == 0)
        def _():
            for k in (1, 2):
                tell(entered.at[1], "segment", seg, k)

        @pl.when(pair_at == peers // 2 - 1)
        def _():
            tell(entered.at[0], "amp", amp, 2)
            tell(entered.at[0], "amp", amp, 4)

        with jax.named_scope("load0"):
            far_loaded()
        send_in(0, 6)
        send_in(0, 7)
        near_loaded()

        @pl.when(is_inner)
        def _():
            with jax.named_scope("ent0"):
                pl.semaphore_wait(entered.at[0], 1)

        for k in [4, 5] + near:
            send_in(0, k)
        with jax.named_scope("ent1"):

            @pl.when(late_inner == 0)
            def _():
                pl.semaphore_wait(entered.at[1], 2)
                tell(entered.at[2], "segment", seg, 1)

            pl.semaphore_wait(entered.at[2], 1)

            @pl.when(early_inner == 1)
            def _():
                tell(entered.at[2], "amp", amp, 6)
    else:
        pl.semaphore_wait(barrier, peers - 1 + sections - 1)
        far_loaded()
        near_loaded()
        for group in groups:
            for k in group:
                send_in(0, k)
    gate_load.wait()
    for k in range(1, sections):
        pltpu.make_async_remote_copy(
            src_ref=gates.at[seg],
            dst_ref=gates.at[seg],
            send_sem=sent,
            recv_sem=grecv,
            device_id={"segment": partner(seg, k)},
            device_id_type=MESH,
        ).start()
    if chunks > 1:
        waits(xs.at[1:], x_sem.at[2])
    for chunk in range(1, chunks):
        for group in groups:
            for k in group:
                send_in(chunk, k)
    picks_load.wait()
    targets_load.wait()
    with jax.named_scope("gates"):
        waits(gates.at[1:], grecv)

    rows_at = lax.broadcasted_iota(jnp.int32, (reg, reg), 0)
    columns_at = lax.broadcasted_iota(jnp.int32, (reg, reg), 1)
    identity = jnp.where(rows_at == columns_at, jnp.float32(1.0), jnp.float32(0.0))

    def build(section, carry):
        low = high = None
        for b in range(blocks):
            factors = row_factors(picks, section, b, qubits, (reg, reg))
            damped = gates[section, b] * factors
            is_low = targets[section, b] == 0
            for_low = jnp.where(is_low, damped, identity)
            for_high = jnp.where(is_low, identity, damped)
            if b == 0:
                low, high = for_low, for_high
            else:
                low = multiply(left_form(for_low), right_form(low))
                high = multiply(left_form(for_high), right_form(high))
        low_form[section] = right_form(low.T)
        high_form[section] = left_form(high)
        return carry

    with jax.named_scope("build"):
        lax.fori_loop(0, sections, build, 0)

    inner = reg // peers
    partial[...] = jnp.zeros_like(partial)

    def apply_section(chunk, section, swapped):
        low = low_form[section]
        high = high_form[section]
        total = jnp.zeros((8, reg), jnp.float32)
        for slab in range(peers):
            if swapped:
                value = yin[chunk, :, slab * inner : (slab + 1) * inner, :].reshape(reg, reg)
            else:
                value = yin[chunk, slab]
            value = multiply(left_form(value), low)
            value = multiply(high, right_form(value))
            total = total + fold_rows(value)
            if swapped:
                yin[chunk, :, slab * inner : (slab + 1) * inner, :] = value.reshape(
                    peers, inner, reg
                )
            else:
                yin[chunk, slab] = value
        partial[section + 1] = partial[section + 1] + total

    order_out = mid + far + near

    def arrival(chunk, g):
        return chunk + g * (chunk // (chunks - 1)) if chunks > 1 else g

    def run_chunk(chunk, carry):
        with jax.named_scope("in"):
            waits(xs.at[chunk], irecv.at[chunk])
        first = jnp.zeros((8, reg), jnp.float32)
        for slab in range(peers):
            first = first + fold_rows(yin[chunk, slab])
        partial[0] = partial[0] + first

        def pair(i, inner_carry):
            apply_section(chunk, 2 * i, False)
            apply_section(chunk, 2 * i + 1, True)
            return inner_carry

        with jax.named_scope("comp"):
            lax.fori_loop(0, sections // 2, pair, 0)

        @pl.when(chunk == chunks - 1)
        def _():
            for s in range(sections + 1):
                sums[amp, s : s + 1, :] = jnp.sum(partial[s], axis=0, keepdims=True)
            for k in range(peers - 1, 0, -1):
                pltpu.make_async_remote_copy(
                    src_ref=sums.at[amp],
                    dst_ref=sums.at[amp],
                    send_sem=sent,
                    recv_sem=srecv,
                    device_id={"amp": partner(amp, k)},
                    device_id_type=MESH,
                ).start()

        for k in order_out:
            g = [k in group for group in groups].index(True)
            peer = partner(amp, k)
            pltpu.make_async_remote_copy(
                src_ref=yin.at[chunk, peer],
                dst_ref=ov.at[chunk, amp],
                send_sem=sent,
                recv_sem=orecv.at[arrival(chunk, g)],
                device_id={"amp": peer},
                device_id_type=MESH,
            ).start()
        return carry

    lax.fori_loop(0, chunks, run_chunk, 0)

    with jax.named_scope("sums"):
        waits(sums.at[1:], srecv)
    totals = []
    for s in range(sections + 1):
        total = sums[0, s : s + 1, :]
        for d in range(1, peers):
            total = total + sums[d, s : s + 1, :]
        totals.append(jnp.sum(total, axis=1, keepdims=True))
    lanes = lax.broadcasted_iota(jnp.int32, (1, reg), 1)
    logs = jnp.zeros((1, reg), jnp.float32)
    for s in range(sections):
        logs = jnp.where(lanes == s, jnp.log(totals[s + 1] / totals[s]), logs)
    logs_ref[...] = logs[:, :sections]
    scale = 1.0 / jnp.sqrt(totals[sections] / total_amps)
    scale = jnp.broadcast_to(scale, (1, reg))

    for chunk in range(chunks):
        m = chunk * peers + amp
        out_ref[pl.ds(m, reg, stride=middle), :] = yin[chunk, amp] * scale
    def place(chunk, k):
        m = chunk * peers + partner(amp, k)
        out_ref[pl.ds(m, reg, stride=middle), :] = ov[chunk, partner(amp, k)] * scale

    for chunk in range(chunks - 1):
        waits(xs.at[0], orecv.at[chunk])
        for k in order_out:
            place(chunk, k)
    for g in (2, 0, 1):
        with jax.named_scope(f"out_{g}"):
            waits(xs.at[0, : len(groups[g])], orecv.at[chunks - 1 + g])
        for k in groups[g]:
            place(chunks - 1, k)

    with jax.named_scope("sendwait"):
        waits(xs, sent)
        waits(xs, sent)
        waits(gates.at[1:], sent)
        waits(sums.at[1:], sent)


def store_kernel(pieces, out_vmem, logs_vmem, out_hbm, logs_hbm, sems):
    rows = out_vmem.shape[0] // pieces
    copies = [pltpu.make_async_copy(logs_vmem, logs_hbm, sems.at[pieces])]
    for p in range(pieces):
        at = pl.ds(p * rows, rows)
        copies.append(pltpu.make_async_copy(out_vmem.at[at], out_hbm.at[at], sems.at[p]))
    for copy in copies:
        copy.start()
    for copy in copies:
        copy.wait()


def step(states, gate_blocks, kraus_picks, block_targets):
    traj_here, amp_local = states.shape
    reg = gate_blocks.shape[-1]
    blocks = gate_blocks.shape[1]
    qubits = kraus_picks.shape[-1]
    peers = lax.axis_size("amp")
    sections = lax.axis_size("segment")
    middle = amp_local // (reg * reg)
    fits = (
        traj_here == 1
        and gate_blocks.shape[0] == 1
        and middle % peers == 0
        and peers & (peers - 1) == 0
        and peers >= 8
        and middle == peers * (peers // 4)
        and sections & (sections - 1) == 0
        and sections % 2 == 0
        and sections < 8
        and reg == 128
        and reg % (8 * peers) == 0
    )
    if not fits:
        return body(states, gate_blocks, kraus_picks, block_targets)
    chunks = middle // peers
    kernel = functools.partial(
        circuit_kernel, peers, sections, blocks, qubits, chunks, amp_local * peers
    )
    f32 = jnp.float32
    dma = pltpu.SemaphoreType.DMA
    out, logs = pl.pallas_call(
        kernel,
        out_shape=(
            pltpu.VMEM((reg * middle, reg), f32),
            pltpu.VMEM((1, sections), f32),
        ),
        in_specs=[pl.BlockSpec(memory_space=pl.ANY)] * 4,
        out_specs=(
            pl.BlockSpec(memory_space=pltpu.VMEM),
            pl.BlockSpec(memory_space=pltpu.VMEM),
        ),
        scratch_shapes=[
            pltpu.VMEM((chunks, peers - 1, reg, reg), f32),
            pltpu.VMEM((chunks, peers, reg, reg), f32),
            pltpu.VMEM((chunks, peers, reg, reg), f32),
            pltpu.VMEM((sections, blocks, reg, reg), f32),
            pltpu.SMEM((1, blocks, sections, qubits), jnp.int32),
            pltpu.SMEM((sections, blocks), jnp.int32),
            pltpu.VMEM((sections, 2 * reg, 2 * reg), jnp.bfloat16),
            pltpu.VMEM((sections, reg, 2 * reg), jnp.bfloat16),
            pltpu.VMEM((sections + 1, 8, reg), f32),
            pltpu.VMEM((peers, 8, reg), f32),
            dma((3,)),
            dma,
            dma((2,)),
            dma,
            dma,
            dma((chunks,)),
            dma((chunks + 2,)),
            dma,
            pltpu.SemaphoreType.REGULAR((3,)),
        ],
        compiler_params=pltpu.CompilerParams(collective_id=0, has_side_effects=True),
    )(
        states.reshape(reg, middle, 1, reg),
        gate_blocks[0],
        jnp.swapaxes(kraus_picks, 1, 2),
        block_targets,
    )
    pieces = 4
    out, logs = pl.pallas_call(
        functools.partial(store_kernel, pieces),
        out_shape=(
            jax.ShapeDtypeStruct(out.shape, f32),
            jax.ShapeDtypeStruct(logs.shape, f32),
        ),
        in_specs=[pl.BlockSpec(memory_space=pltpu.VMEM)] * 2,
        out_specs=(pl.BlockSpec(memory_space=pl.ANY),) * 2,
        scratch_shapes=[dma((pieces + 1,))],
    )(
        pltpu.with_memory_space_constraint(out, pltpu.VMEM),
        pltpu.with_memory_space_constraint(logs, pltpu.VMEM),
    )
    return out.reshape(1, amp_local), logs


def solution(mesh):
    in_specs = (
        P("segment", "amp"),
        P("segment", None, None, None),
        P("segment", None, None, None),
        P(),
    )
    out_specs = (P("segment", "amp"), P("segment", None))
    return jax.shard_map(step, mesh=mesh, in_specs=in_specs, out_specs=out_specs, check_vma=False)
```

```python
import functools

import jax
import jax.numpy as jnp
from jax import lax
from jax.experimental import pallas as pl
from jax.experimental.pallas import tpu as pltpu
from jax.sharding import PartitionSpec as P

KEEP_FACTORS = (1.0, 0.9, 1.0, 0.97)
FLIP_FACTORS = (0.9, 1.0, 0.97, 1.0)
MESH = pl.DeviceIdType.MESH


def broadcast(block, axis, owner):
    block = jnp.where(lax.axis_index(axis) == owner, block, jnp.zeros_like(block))
    return lax.psum(block, axis)


def noise_factors(kraus_rows):
    qubit_count = kraus_rows.shape[-1]
    register = 2**qubit_count
    positions = jnp.arange(register, dtype=jnp.int32)
    product = jnp.ones(kraus_rows.shape[:-1] + (register,), jnp.float32)
    for qubit_pos in range(qubit_count):
        bit_value = jnp.right_shift(positions, qubit_count - 1 - qubit_pos) & 1
        column = kraus_rows[..., qubit_pos : qubit_pos + 1]
        low_value = jnp.zeros(column.shape, jnp.float32)
        high_value = jnp.zeros(column.shape, jnp.float32)
        for option in range(4):
            picked = (column == option).astype(jnp.float32)
            low_value = low_value + picked * KEEP_FACTORS[option]
            high_value = high_value + picked * FLIP_FACTORS[option]
        product = product * jnp.where(bit_value == 1, high_value, low_value)
    return product


def apply_gate(amplitudes, matrix, factors, target):

    def on_low(values):
        mixed_rows = jnp.einsum("bhmk,ik->bhmi", values, matrix, precision=lax.Precision.HIGHEST)
        return mixed_rows * factors[:, None, None, :]

    def on_high(values):
        mixed_rows = jnp.einsum("bjmk,ij->bimk", values, matrix, precision=lax.Precision.HIGHEST)
        return mixed_rows * factors[:, :, None, None]

    return lax.cond(target == 0, on_low, on_high, amplitudes)


def square_sums(values):
    return (values, jnp.sum(values * values, axis=(1, 2, 3)))


def body(states, gate_blocks, kraus_picks, block_targets):
    traj_here = states.shape[0]
    amp_local = states.shape[1]
    register = gate_blocks.shape[-1]
    blocks = gate_blocks.shape[1]
    middle = amp_local // (register * register)
    total_amps = amp_local * lax.axis_size("amp")
    sections = lax.axis_size("segment")
    amplitudes = states.reshape(traj_here, register, middle, register)
    first_local = jnp.sum(amplitudes * amplitudes, axis=(1, 2, 3))
    local_sums = [first_local]
    for section in range(sections):
        section_gates = broadcast(gate_blocks, "segment", section)[0]
        for block_pos in range(blocks):
            factors = noise_factors(kraus_picks[:, section, block_pos, :])
            amplitudes = apply_gate(
                amplitudes, section_gates[block_pos], factors, block_targets[section, block_pos]
            )
        amplitudes, local_sq = square_sums(
            lax.all_to_all(amplitudes, "amp", split_axis=1, concat_axis=1, tiled=True)
        )
        local_sums.append(local_sq)
    totals = lax.psum(jnp.stack(local_sums, axis=1), "amp")
    log_weights = jnp.log(totals[:, 1:] / totals[:, :-1])
    amplitudes = amplitudes / jnp.sqrt(totals[:, -1] / total_amps)[:, None, None, None]
    return (amplitudes.reshape(traj_here, amp_local), log_weights)


def partner(index, k):
    result = index
    bit = 1
    while bit <= k:
        if k & bit:
            result = result + bit * (1 - 2 * ((index // bit) % 2))
        bit *= 2
    return result


def split(values):
    high = values.astype(jnp.bfloat16)
    low = (values - high.astype(jnp.float32)).astype(jnp.bfloat16)
    return high, low


def left_form(matrix):
    return jnp.concatenate(split(matrix), axis=1)


def right_form(matrix):
    row = jnp.concatenate(split(matrix), axis=1)
    return jnp.concatenate([row, row], axis=0)


def multiply(left, right):
    both = jnp.dot(left, right, preferred_element_type=jnp.float32)
    half = both.shape[1] // 2
    return both[:, :half] + both[:, half:]


def fold_rows(values):
    squares = values * values
    return jnp.sum(squares.reshape(-1, 8, squares.shape[-1]), axis=0)


def row_factors(picks_ref, section, block, qubits, shape):
    positions = lax.broadcasted_iota(jnp.int32, shape, 0)
    product = jnp.ones(shape, jnp.float32)
    for q in range(qubits):
        pick = picks_ref[0, block, section, q]
        keep = jnp.float32(KEEP_FACTORS[0])
        flip = jnp.float32(FLIP_FACTORS[0])
        for option in range(1, 4):
            keep = jnp.where(pick == option, jnp.float32(KEEP_FACTORS[option]), keep)
            flip = jnp.where(pick == option, jnp.float32(FLIP_FACTORS[option]), flip)
        bit = jnp.right_shift(positions, qubits - 1 - q) & 1
        product = product * jnp.where(bit == 1, flip, keep)
    return product


def waits(like, semaphore):
    pltpu.make_async_copy(like, like, semaphore).wait()


def circuit_kernel(
    peers, sections, blocks, qubits, chunks, total_amps,
    x_hbm, gates_hbm, picks_hbm, targets_hbm,
    out_ref, logs_ref,
    xs, yin, ov, gates, picks, targets, low_form, high_form, partial, sums,
    x_sem, small_sem, sent, grecv, irecv, orecv, srecv,
    entered,
):
    seg = lax.axis_index("segment")
    amp = lax.axis_index("amp")
    reg = gates.shape[-1]
    middle = chunks * peers
    far = list(range(3 * peers // 4, peers))
    mid = list(range(peers // 2, 3 * peers // 4))
    near = list(range(peers // 2 - 1, 0, -1))
    groups = [far, mid, near]

    def tell(semaphore, axis, index, k):
        pl.semaphore_signal(
            semaphore, inc=1, device_id={axis: partner(index, k)}, device_id_type=MESH
        )

    def load(chunk, k, semaphore):
        m = chunk * peers + partner(amp, k)
        pltpu.make_async_copy(x_hbm.at[:, m, 0], xs.at[chunk, k - 1], semaphore).start()

    for k in far:
        load(0, k, x_sem.at[0])

    barrier = pltpu.get_barrier_semaphore()
    line = peers == 8 and sections == 4
    pair_at = amp // 2
    inner_pair = (pair_at + 1) // 2 % 2
    is_inner = inner_pair == 1
    late_inner = pair_at // 2 * inner_pair
    early_inner = (1 - pair_at // 2) * inner_pair
    if line:

        for k in (6, 7, 1):
            tell(barrier, "amp", amp, k)

        @pl.when(is_inner)
        def _():
            for k in (2, 3, 4, 5):
                tell(barrier, "amp", amp, k)

        @pl.when(late_inner == 0)
        def _():
            for k in (1, 2):
                tell(barrier, "segment", seg, k)
    else:
        for k in range(peers - 1, 0, -1):
            tell(barrier, "amp", amp, k)
        for k in range(1, sections):
            tell(barrier, "segment", seg, k)

    for k in mid + near:
        load(0, k, x_sem.at[1])
    for chunk in range(1, chunks):
        for k in far + mid + near:
            load(chunk, k, x_sem.at[1])
    pltpu.make_async_copy(gates_hbm, gates.at[seg], x_sem.at[1]).start()
    picks_load = pltpu.make_async_copy(picks_hbm, picks, small_sem.at[0])
    picks_load.start()
    targets_load = pltpu.make_async_copy(targets_hbm, targets, small_sem.at[1])
    targets_load.start()
    for chunk in range(chunks):
        pltpu.make_async_copy(
            x_hbm.at[:, chunk * peers + amp, 0], yin.at[chunk, amp], x_sem.at[1]
        ).start()

    def send_in(chunk, k):
        pltpu.make_async_remote_copy(
            src_ref=xs.at[chunk, k - 1],
            dst_ref=yin.at[chunk, amp],
            send_sem=sent,
            recv_sem=irecv.at[chunk],
            device_id={"amp": partner(amp, k)},
            device_id_type=MESH,
        ).start()

    def far_loaded():
        waits(xs.at[0, : len(far)], x_sem.at[0])

    def rest_loaded():
        waits(xs, x_sem.at[1])
        waits(gates.at[0], x_sem.at[1])

    if line:
        with jax.named_scope("barrier"):
            pl.semaphore_wait(barrier, 9 - 4 * inner_pair - 2 * late_inner)

        @pl.when(late_inner == 0)
        def _():
            for k in (1, 2):
                tell(entered.at[1], "segment", seg, k)

        @pl.when(pair_at == peers // 2 - 1)
        def _():
            tell(entered.at[0], "amp", amp, 2)
            tell(entered.at[0], "amp", amp, 4)

        with jax.named_scope("load0"):
            far_loaded()
        send_in(0, 6)
        send_in(0, 7)
        rest_loaded()

        @pl.when(is_inner)
        def _():
            with jax.named_scope("ent0"):
                pl.semaphore_wait(entered.at[0], 1)

        for k in [4, 5] + near:
            send_in(0, k)
        with jax.named_scope("ent1"):

            @pl.when(late_inner == 0)
            def _():
                pl.semaphore_wait(entered.at[1], 2)
                tell(entered.at[2], "segment", seg, 1)

            pl.semaphore_wait(entered.at[2], 1)

            @pl.when(early_inner == 1)
            def _():
                tell(entered.at[2], "amp", amp, 6)
    else:
        pl.semaphore_wait(barrier, peers - 1 + sections - 1)
        far_loaded()
        rest_loaded()
        for group in groups:
            for k in group:
                send_in(0, k)
    for k in range(1, sections):
        pltpu.make_async_remote_copy(
            src_ref=gates.at[seg],
            dst_ref=gates.at[seg],
            send_sem=sent,
            recv_sem=grecv,
            device_id={"segment": partner(seg, k)},
            device_id_type=MESH,
        ).start()
    for chunk in range(1, chunks):
        for group in groups:
            for k in group:
                send_in(chunk, k)
    picks_load.wait()
    targets_load.wait()
    with jax.named_scope("gates"):
        waits(gates.at[1:], grecv)

    rows_at = lax.broadcasted_iota(jnp.int32, (reg, reg), 0)
    columns_at = lax.broadcasted_iota(jnp.int32, (reg, reg), 1)
    identity = jnp.where(rows_at == columns_at, jnp.float32(1.0), jnp.float32(0.0))

    def build(section, carry):
        low = high = None
        for b in range(blocks):
            factors = row_factors(picks, section, b, qubits, (reg, reg))
            damped = gates[section, b] * factors
            is_low = targets[section, b] == 0
            for_low = jnp.where(is_low, damped, identity)
            for_high = jnp.where(is_low, identity, damped)
            if b == 0:
                low, high = for_low, for_high
            else:
                low = multiply(left_form(for_low), right_form(low))
                high = multiply(left_form(for_high), right_form(high))
        low_form[section] = right_form(low.T)
        high_form[section] = left_form(high)
        return carry

    with jax.named_scope("build"):
        lax.fori_loop(0, sections, build, 0)

    inner = reg // peers
    lanes = lax.broadcasted_iota(jnp.int32, (1, reg), 1)
    partial[...] = jnp.zeros_like(partial)

    def apply_section(chunk, section, swapped):
        low = low_form[section]
        high = high_form[section]
        total = jnp.zeros((8, reg), jnp.float32)
        for slab in range(peers):
            if swapped:
                value = yin[chunk, :, slab * inner : (slab + 1) * inner, :].reshape(reg, reg)
            else:
                value = yin[chunk, slab]
            value = multiply(left_form(value), low)
            value = multiply(high, right_form(value))
            total = total + fold_rows(value)
            if swapped:
                yin[chunk, :, slab * inner : (slab + 1) * inner, :] = value.reshape(
                    peers, inner, reg
                )
            else:
                yin[chunk, slab] = value
        partial[section + 1] = partial[section + 1] + total

    order_out = mid + far + near

    def arrival(chunk, k):
        slot = max(k - peers // 2 + 1, 0)
        return chunk + slot * (chunk // (chunks - 1))

    def run_chunk(chunk, carry):
        with jax.named_scope("in"):
            waits(xs.at[chunk], irecv.at[chunk])
        first = jnp.zeros((8, reg), jnp.float32)
        for slab in range(peers):
            first = first + fold_rows(yin[chunk, slab])
        partial[0] = partial[0] + first

        def pair(i, inner_carry):
            apply_section(chunk, 2 * i, False)
            apply_section(chunk, 2 * i + 1, True)
            return inner_carry

        with jax.named_scope("comp"):
            lax.fori_loop(0, sections // 2, pair, 0)

        @pl.when(chunk == chunks - 1)
        def _():
            row = jnp.zeros((1, reg), jnp.float32)
            for s in range(sections + 1):
                total = jnp.sum(jnp.sum(partial[s], axis=0, keepdims=True), axis=1, keepdims=True)
                row = jnp.where(lanes == s, total, row)
            sums[amp] = row
            for k in range(peers - 1, 0, -1):
                pltpu.make_async_remote_copy(
                    src_ref=sums.at[amp],
                    dst_ref=sums.at[amp],
                    send_sem=sent,
                    recv_sem=srecv,
                    device_id={"amp": partner(amp, k)},
                    device_id_type=MESH,
                ).start()

        for k in order_out:
            peer = partner(amp, k)
            pltpu.make_async_remote_copy(
                src_ref=yin.at[chunk, peer],
                dst_ref=ov.at[chunk, amp],
                send_sem=sent,
                recv_sem=orecv.at[arrival(chunk, k)],
                device_id={"amp": peer},
                device_id_type=MESH,
            ).start()
        return carry

    lax.fori_loop(0, chunks, run_chunk, 0)

    with jax.named_scope("sums"):
        waits(sums.at[1:], srecv)
    row = sums[0]
    for d in range(1, peers):
        row = row + sums[d]
    totals = [
        jnp.sum(jnp.where(lanes == s, row, 0.0), axis=1, keepdims=True)
        for s in range(sections + 1)
    ]
    logs = jnp.zeros((1, reg), jnp.float32)
    for s in range(sections):
        logs = jnp.where(lanes == s, jnp.log(totals[s + 1] / totals[s]), logs)
    logs_ref[...] = logs[:, :sections]
    scale = 1.0 / jnp.sqrt(totals[sections] / total_amps)
    scale = jnp.broadcast_to(scale, (1, reg))

    for chunk in range(chunks):
        m = chunk * peers + amp
        out_ref[pl.ds(m, reg, stride=middle), :] = yin[chunk, amp] * scale
    def place(chunk, peer):
        m = chunk * peers + peer
        out_ref[pl.ds(m, reg, stride=middle), :] = ov[chunk, peer] * scale

    last = chunks - 1
    for chunk in range(last):
        waits(xs.at[0], orecv.at[chunk])
        for k in order_out:
            place(chunk, partner(amp, k))
    with jax.named_scope("out_near"):
        waits(xs.at[0, : len(near)], orecv.at[last])
    for k in near:
        place(last, partner(amp, k))
    half = peers // 2
    for at in range(half):
        ahead = (at + half // 2) % half
        slot = inner_pair * at + (1 - inner_pair) * ahead
        peer = inner_pair * partner(amp, half + at) + (1 - inner_pair) * partner(amp, half + ahead)
        with jax.named_scope(f"out_{at}"):
            waits(xs.at[0, 0], orecv.at[last + 1 + slot])
        place(last, peer)

    with jax.named_scope("sendwait"):
        waits(xs, sent)
        waits(xs, sent)
        waits(gates.at[1:], sent)
        waits(sums.at[1:], sent)


def store_kernel(pieces, out_vmem, logs_vmem, out_hbm, logs_hbm, sems):
    rows = out_vmem.shape[0] // pieces
    copies = [pltpu.make_async_copy(logs_vmem, logs_hbm, sems.at[pieces])]
    for p in range(pieces):
        at = pl.ds(p * rows, rows)
        copies.append(pltpu.make_async_copy(out_vmem.at[at], out_hbm.at[at], sems.at[p]))
    for copy in copies:
        copy.start()
    for copy in copies:
        copy.wait()


def step(states, gate_blocks, kraus_picks, block_targets):
    traj_here, amp_local = states.shape
    reg = gate_blocks.shape[-1]
    blocks = gate_blocks.shape[1]
    qubits = kraus_picks.shape[-1]
    peers = lax.axis_size("amp")
    sections = lax.axis_size("segment")
    middle = amp_local // (reg * reg)
    fits = (
        traj_here == 1
        and gate_blocks.shape[0] == 1
        and middle % peers == 0
        and peers & (peers - 1) == 0
        and peers >= 8
        and middle == peers * (peers // 4)
        and middle > peers
        and sections & (sections - 1) == 0
        and sections % 2 == 0
        and sections < 8
        and reg == 128
        and reg % (8 * peers) == 0
    )
    if not fits:
        return body(states, gate_blocks, kraus_picks, block_targets)
    chunks = middle // peers
    kernel = functools.partial(
        circuit_kernel, peers, sections, blocks, qubits, chunks, amp_local * peers
    )
    f32 = jnp.float32
    dma = pltpu.SemaphoreType.DMA
    out, logs = pl.pallas_call(
        kernel,
        out_shape=(
            pltpu.VMEM((reg * middle, reg), f32),
            pltpu.VMEM((1, sections), f32),
        ),
        in_specs=[pl.BlockSpec(memory_space=pl.ANY)] * 4,
        out_specs=(
            pl.BlockSpec(memory_space=pltpu.VMEM),
            pl.BlockSpec(memory_space=pltpu.VMEM),
        ),
        scratch_shapes=[
            pltpu.VMEM((chunks, peers - 1, reg, reg), f32),
            pltpu.VMEM((chunks, peers, reg, reg), f32),
            pltpu.VMEM((chunks, peers, reg, reg), f32),
            pltpu.VMEM((sections, blocks, reg, reg), f32),
            pltpu.SMEM((1, blocks, sections, qubits), jnp.int32),
            pltpu.SMEM((sections, blocks), jnp.int32),
            pltpu.VMEM((sections, 2 * reg, 2 * reg), jnp.bfloat16),
            pltpu.VMEM((sections, reg, 2 * reg), jnp.bfloat16),
            pltpu.VMEM((sections + 1, 8, reg), f32),
            pltpu.VMEM((peers, 1, reg), f32),
            dma((2,)),
            dma((2,)),
            dma,
            dma,
            dma((chunks,)),
            dma((chunks + peers // 2,)),
            dma,
            pltpu.SemaphoreType.REGULAR((3,)),
        ],
        compiler_params=pltpu.CompilerParams(collective_id=0, has_side_effects=True),
    )(
        states.reshape(reg, middle, 1, reg),
        gate_blocks[0],
        jnp.swapaxes(kraus_picks, 1, 2),
        block_targets,
    )
    pieces = 4
    out, logs = pl.pallas_call(
        functools.partial(store_kernel, pieces),
        out_shape=(
            jax.ShapeDtypeStruct(out.shape, f32),
            jax.ShapeDtypeStruct(logs.shape, f32),
        ),
        in_specs=[pl.BlockSpec(memory_space=pltpu.VMEM)] * 2,
        out_specs=(pl.BlockSpec(memory_space=pl.ANY),) * 2,
        scratch_shapes=[dma((pieces + 1,))],
    )(
        pltpu.with_memory_space_constraint(out, pltpu.VMEM),
        pltpu.with_memory_space_constraint(logs, pltpu.VMEM),
    )
    return out.reshape(1, amp_local), logs


def solution(mesh):
    in_specs = (
        P("segment", "amp"),
        P("segment", None, None, None),
        P("segment", None, None, None),
        P(),
    )
    out_specs = (P("segment", "amp"), P("segment", None))
    return jax.shard_map(step, mesh=mesh, in_specs=in_specs, out_specs=out_specs, check_vma=False)
```

```python
import functools

import jax
import jax.numpy as jnp
from jax import lax
from jax.experimental import pallas as pl
from jax.experimental.pallas import tpu as pltpu
from jax.sharding import PartitionSpec as P

KEEP_FACTORS = (1.0, 0.9, 1.0, 0.97)
FLIP_FACTORS = (0.9, 1.0, 0.97, 1.0)
MESH = pl.DeviceIdType.MESH


def broadcast(block, axis, owner):
    block = jnp.where(lax.axis_index(axis) == owner, block, jnp.zeros_like(block))
    return lax.psum(block, axis)


def noise_factors(kraus_rows):
    qubit_count = kraus_rows.shape[-1]
    register = 2**qubit_count
    positions = jnp.arange(register, dtype=jnp.int32)
    product = jnp.ones(kraus_rows.shape[:-1] + (register,), jnp.float32)
    for qubit_pos in range(qubit_count):
        bit_value = jnp.right_shift(positions, qubit_count - 1 - qubit_pos) & 1
        column = kraus_rows[..., qubit_pos : qubit_pos + 1]
        low_value = jnp.zeros(column.shape, jnp.float32)
        high_value = jnp.zeros(column.shape, jnp.float32)
        for option in range(4):
            picked = (column == option).astype(jnp.float32)
            low_value = low_value + picked * KEEP_FACTORS[option]
            high_value = high_value + picked * FLIP_FACTORS[option]
        product = product * jnp.where(bit_value == 1, high_value, low_value)
    return product


def apply_gate(amplitudes, matrix, factors, target):

    def on_low(values):
        mixed_rows = jnp.einsum("bhmk,ik->bhmi", values, matrix, precision=lax.Precision.HIGHEST)
        return mixed_rows * factors[:, None, None, :]

    def on_high(values):
        mixed_rows = jnp.einsum("bjmk,ij->bimk", values, matrix, precision=lax.Precision.HIGHEST)
        return mixed_rows * factors[:, :, None, None]

    return lax.cond(target == 0, on_low, on_high, amplitudes)


def square_sums(values):
    return (values, jnp.sum(values * values, axis=(1, 2, 3)))


def body(states, gate_blocks, kraus_picks, block_targets):
    traj_here = states.shape[0]
    amp_local = states.shape[1]
    register = gate_blocks.shape[-1]
    blocks = gate_blocks.shape[1]
    middle = amp_local // (register * register)
    total_amps = amp_local * lax.axis_size("amp")
    sections = lax.axis_size("segment")
    amplitudes = states.reshape(traj_here, register, middle, register)
    first_local = jnp.sum(amplitudes * amplitudes, axis=(1, 2, 3))
    local_sums = [first_local]
    for section in range(sections):
        section_gates = broadcast(gate_blocks, "segment", section)[0]
        for block_pos in range(blocks):
            factors = noise_factors(kraus_picks[:, section, block_pos, :])
            amplitudes = apply_gate(
                amplitudes, section_gates[block_pos], factors, block_targets[section, block_pos]
            )
        amplitudes, local_sq = square_sums(
            lax.all_to_all(amplitudes, "amp", split_axis=1, concat_axis=1, tiled=True)
        )
        local_sums.append(local_sq)
    totals = lax.psum(jnp.stack(local_sums, axis=1), "amp")
    log_weights = jnp.log(totals[:, 1:] / totals[:, :-1])
    amplitudes = amplitudes / jnp.sqrt(totals[:, -1] / total_amps)[:, None, None, None]
    return (amplitudes.reshape(traj_here, amp_local), log_weights)


def partner(index, k):
    result = index
    bit = 1
    while bit <= k:
        if k & bit:
            result = result + bit * (1 - 2 * ((index // bit) % 2))
        bit *= 2
    return result


def split(values):
    high = values.astype(jnp.bfloat16)
    low = (values - high.astype(jnp.float32)).astype(jnp.bfloat16)
    return high, low


def left_form(matrix):
    return jnp.concatenate(split(matrix), axis=1)


def right_form(matrix):
    row = jnp.concatenate(split(matrix), axis=1)
    return jnp.concatenate([row, row], axis=0)


def multiply(left, right):
    both = jnp.dot(left, right, preferred_element_type=jnp.float32)
    half = both.shape[1] // 2
    return both[:, :half] + both[:, half:]


def fold_rows(values):
    squares = values * values
    return jnp.sum(squares.reshape(-1, 8, squares.shape[-1]), axis=0)


def row_factors(picks_ref, section, block, qubits, shape):
    positions = lax.broadcasted_iota(jnp.int32, shape, 0)
    product = jnp.ones(shape, jnp.float32)
    for q in range(qubits):
        pick = picks_ref[0, block, section, q]
        keep = jnp.float32(KEEP_FACTORS[0])
        flip = jnp.float32(FLIP_FACTORS[0])
        for option in range(1, 4):
            keep = jnp.where(pick == option, jnp.float32(KEEP_FACTORS[option]), keep)
            flip = jnp.where(pick == option, jnp.float32(FLIP_FACTORS[option]), flip)
        bit = jnp.right_shift(positions, qubits - 1 - q) & 1
        product = product * jnp.where(bit == 1, flip, keep)
    return product


def waits(like, semaphore):
    pltpu.make_async_copy(like, like, semaphore).wait()


def circuit_kernel(
    peers, sections, blocks, qubits, chunks, total_amps,
    x_hbm, gates_hbm, picks_hbm, targets_hbm,
    out_ref, logs_ref,
    xs, yin, ov, gates, picks, targets, low_form, high_form, partial, sums,
    x_sem, small_sem, sent, grecv, irecv, orecv, srecv,
    entered,
):
    seg = lax.axis_index("segment")
    amp = lax.axis_index("amp")
    reg = gates.shape[-1]
    middle = chunks * peers
    far = list(range(3 * peers // 4, peers))
    mid = list(range(peers // 2, 3 * peers // 4))
    near = list(range(peers // 2 - 1, 0, -1))
    groups = [far, mid, near]

    def tell(semaphore, axis, index, k):
        pl.semaphore_signal(
            semaphore, inc=1, device_id={axis: partner(index, k)}, device_id_type=MESH
        )

    quarter = reg // 4
    parts = [pl.ds(q * quarter, quarter) for q in range(4)]
    first, others = parts[0], pl.ds(quarter, reg - quarter)

    def load(chunk, k, semaphore, rows=pl.ds(0, reg)):
        m = chunk * peers + partner(amp, k)
        pltpu.make_async_copy(
            x_hbm.at[rows, m, 0], xs.at[chunk, k - 1, rows], semaphore
        ).start()

    for q, rows in enumerate(parts):
        for k in far:
            load(0, k, x_sem.at[min(q, 1)], rows)

    barrier = pltpu.get_barrier_semaphore()
    line = peers == 8 and sections == 4
    pair_at = amp // 2
    inner_pair = (pair_at + 1) // 2 % 2
    is_inner = inner_pair == 1
    late_inner = pair_at // 2 * inner_pair
    early_inner = (1 - pair_at // 2) * inner_pair
    if line:

        for k in (6, 7, 1):
            tell(barrier, "amp", amp, k)

        @pl.when(is_inner)
        def _():
            for k in (2, 3, 4, 5):
                tell(barrier, "amp", amp, k)

        @pl.when(late_inner == 0)
        def _():
            for k in (1, 2):
                tell(barrier, "segment", seg, k)
    else:
        for k in range(peers - 1, 0, -1):
            tell(barrier, "amp", amp, k)
        for k in range(1, sections):
            tell(barrier, "segment", seg, k)

    for k in mid + near:
        load(0, k, x_sem.at[2])
    for chunk in range(1, chunks):
        for k in far + mid + near:
            load(chunk, k, x_sem.at[2])
    pltpu.make_async_copy(gates_hbm, gates.at[seg], x_sem.at[2]).start()
    picks_load = pltpu.make_async_copy(picks_hbm, picks, small_sem)
    picks_load.start()
    targets_load = pltpu.make_async_copy(targets_hbm, targets, small_sem)
    targets_load.start()
    for chunk in range(chunks):
        pltpu.make_async_copy(
            x_hbm.at[:, chunk * peers + amp, 0], yin.at[chunk, amp], x_sem.at[2]
        ).start()

    def send_in(chunk, k, rows=pl.ds(0, reg)):
        pltpu.make_async_remote_copy(
            src_ref=xs.at[chunk, k - 1, rows],
            dst_ref=yin.at[chunk, amp, rows],
            send_sem=sent,
            recv_sem=irecv.at[chunk],
            device_id={"amp": partner(amp, k)},
            device_id_type=MESH,
        ).start()

    def far_loaded(at):
        waits(xs.at[0, : len(far), [first, others][at]], x_sem.at[at])

    def rest_loaded():
        waits(xs, x_sem.at[2])
        waits(gates.at[0], x_sem.at[2])

    if line:
        with jax.named_scope("barrier"):
            pl.semaphore_wait(barrier, 9 - 4 * inner_pair - 2 * late_inner)

        @pl.when(late_inner == 0)
        def _():
            for k in (1, 2):
                tell(entered.at[1], "segment", seg, k)

        @pl.when(pair_at == peers // 2 - 1)
        def _():
            tell(entered.at[0], "amp", amp, 2)
            tell(entered.at[0], "amp", amp, 4)

        for at, rows in enumerate((first, others)):
            with jax.named_scope("load0"):
                far_loaded(at)
            send_in(0, 6, rows)
            send_in(0, 7, rows)
        rest_loaded()

        @pl.when(is_inner)
        def _():
            with jax.named_scope("ent0"):
                pl.semaphore_wait(entered.at[0], 1)

        for k in [4, 5] + near:
            send_in(0, k)
        with jax.named_scope("ent1"):

            @pl.when(late_inner == 0)
            def _():
                pl.semaphore_wait(entered.at[1], 2)
                tell(entered.at[2], "segment", seg, 1)

            pl.semaphore_wait(entered.at[2], 1)

            @pl.when(early_inner == 1)
            def _():
                tell(entered.at[2], "amp", amp, 6)
    else:
        pl.semaphore_wait(barrier, peers - 1 + sections - 1)
        far_loaded(0)
        far_loaded(1)
        rest_loaded()
        for group in groups:
            for k in group:
                send_in(0, k)
    for k in range(1, sections):
        pltpu.make_async_remote_copy(
            src_ref=gates.at[seg],
            dst_ref=gates.at[seg],
            send_sem=sent,
            recv_sem=grecv,
            device_id={"segment": partner(seg, k)},
            device_id_type=MESH,
        ).start()
    for chunk in range(1, chunks):
        for group in groups:
            for k in group:
                send_in(chunk, k)
    picks_load.wait()
    targets_load.wait()
    with jax.named_scope("gates"):
        waits(gates.at[1:], grecv)

    rows_at = lax.broadcasted_iota(jnp.int32, (reg, reg), 0)
    columns_at = lax.broadcasted_iota(jnp.int32, (reg, reg), 1)
    identity = jnp.where(rows_at == columns_at, jnp.float32(1.0), jnp.float32(0.0))

    def build(section, carry):
        low = high = None
        for b in range(blocks):
            factors = row_factors(picks, section, b, qubits, (reg, reg))
            damped = gates[section, b] * factors
            is_low = targets[section, b] == 0
            for_low = jnp.where(is_low, damped, identity)
            for_high = jnp.where(is_low, identity, damped)
            if b == 0:
                low, high = for_low, for_high
            else:
                low = multiply(left_form(for_low), right_form(low))
                high = multiply(left_form(for_high), right_form(high))
        low_form[section] = right_form(low.T)
        high_form[section] = left_form(high)
        return carry

    with jax.named_scope("build"):
        lax.fori_loop(0, sections, build, 0)

    inner = reg // peers
    lanes = lax.broadcasted_iota(jnp.int32, (1, reg), 1)
    partial[...] = jnp.zeros_like(partial)

    def apply_section(chunk, section, swapped):
        low = low_form[section]
        high = high_form[section]
        total = jnp.zeros((8, reg), jnp.float32)
        for slab in range(peers):
            if swapped:
                value = yin[chunk, :, slab * inner : (slab + 1) * inner, :].reshape(reg, reg)
            else:
                value = yin[chunk, slab]
            value = multiply(left_form(value), low)
            value = multiply(high, right_form(value))
            total = total + fold_rows(value)
            if swapped:
                yin[chunk, :, slab * inner : (slab + 1) * inner, :] = value.reshape(
                    peers, inner, reg
                )
            else:
                yin[chunk, slab] = value
        partial[section + 1] = partial[section + 1] + total

    order_out = mid + far + near

    def arrival(chunk, k):
        slot = max(k - peers // 2 + 1, 0)
        return chunk + slot * (chunk // (chunks - 1))

    def run_chunk(chunk, carry):
        with jax.named_scope("in"):
            waits(xs.at[chunk], irecv.at[chunk])
        first = jnp.zeros((8, reg), jnp.float32)
        for slab in range(peers):
            first = first + fold_rows(yin[chunk, slab])
        partial[0] = partial[0] + first

        def pair(i, inner_carry):
            apply_section(chunk, 2 * i, False)
            apply_section(chunk, 2 * i + 1, True)
            return inner_carry

        with jax.named_scope("comp"):
            lax.fori_loop(0, sections // 2, pair, 0)

        @pl.when(chunk == chunks - 1)
        def _():
            row = jnp.zeros((1, reg), jnp.float32)
            for s in range(sections + 1):
                total = jnp.sum(jnp.sum(partial[s], axis=0, keepdims=True), axis=1, keepdims=True)
                row = jnp.where(lanes == s, total, row)
            sums[amp] = row
            for k in range(peers - 1, 0, -1):
                pltpu.make_async_remote_copy(
                    src_ref=sums.at[amp],
                    dst_ref=sums.at[amp],
                    send_sem=sent,
                    recv_sem=srecv,
                    device_id={"amp": partner(amp, k)},
                    device_id_type=MESH,
                ).start()

        for k in order_out:
            peer = partner(amp, k)
            pltpu.make_async_remote_copy(
                src_ref=yin.at[chunk, peer],
                dst_ref=ov.at[chunk, amp],
                send_sem=sent,
                recv_sem=orecv.at[arrival(chunk, k)],
                device_id={"amp": peer},
                device_id_type=MESH,
            ).start()
        return carry

    lax.fori_loop(0, chunks, run_chunk, 0)

    with jax.named_scope("sums"):
        waits(sums.at[1:], srecv)
    row = sums[0]
    for d in range(1, peers):
        row = row + sums[d]
    totals = [
        jnp.sum(jnp.where(lanes == s, row, 0.0), axis=1, keepdims=True)
        for s in range(sections + 1)
    ]
    logs = jnp.zeros((1, reg), jnp.float32)
    for s in range(sections):
        logs = jnp.where(lanes == s, jnp.log(totals[s + 1] / totals[s]), logs)
    logs_ref[...] = logs[:, :sections]
    scale = 1.0 / jnp.sqrt(totals[sections] / total_amps)
    scale = jnp.broadcast_to(scale, (1, reg))

    for chunk in range(chunks):
        m = chunk * peers + amp
        out_ref[pl.ds(m, reg, stride=middle), :] = yin[chunk, amp] * scale
    def place(chunk, peer):
        m = chunk * peers + peer
        out_ref[pl.ds(m, reg, stride=middle), :] = ov[chunk, peer] * scale

    last = chunks - 1
    for chunk in range(last):
        waits(xs.at[0], orecv.at[chunk])
        for k in order_out:
            place(chunk, partner(amp, k))
    with jax.named_scope("out_near"):
        waits(xs.at[0, : len(near)], orecv.at[last])
    for k in near:
        place(last, partner(amp, k))
    half = peers // 2
    for at in range(half):
        ahead = (at + half // 2) % half
        slot = inner_pair * at + (1 - inner_pair) * ahead
        peer = inner_pair * partner(amp, half + at) + (1 - inner_pair) * partner(amp, half + ahead)
        with jax.named_scope(f"out_{at}"):
            waits(xs.at[0, 0], orecv.at[last + 1 + slot])
        place(last, peer)

    with jax.named_scope("sendwait"):
        waits(xs, sent)
        waits(xs, sent)
        waits(gates.at[1:], sent)
        waits(sums.at[1:], sent)


def store_kernel(pieces, out_vmem, logs_vmem, out_hbm, logs_hbm, out_sem, logs_sem):
    rows = out_vmem.shape[0] // pieces
    for p in range(pieces):
        at = pl.ds(p * rows, rows)
        pltpu.make_async_copy(out_vmem.at[at], out_hbm.at[at], out_sem).start()
    logs_copy = pltpu.make_async_copy(logs_vmem, logs_hbm, logs_sem)
    logs_copy.start()
    pltpu.make_async_copy(out_vmem, out_hbm, out_sem).wait()
    logs_copy.wait()


def step(states, gate_blocks, kraus_picks, block_targets):
    traj_here, amp_local = states.shape
    reg = gate_blocks.shape[-1]
    blocks = gate_blocks.shape[1]
    qubits = kraus_picks.shape[-1]
    peers = lax.axis_size("amp")
    sections = lax.axis_size("segment")
    middle = amp_local // (reg * reg)
    fits = (
        traj_here == 1
        and gate_blocks.shape[0] == 1
        and middle % peers == 0
        and peers & (peers - 1) == 0
        and peers >= 8
        and middle == peers * (peers // 4)
        and middle > peers
        and sections & (sections - 1) == 0
        and sections % 2 == 0
        and sections < 8
        and reg == 128
        and reg % (8 * peers) == 0
    )
    if not fits:
        return body(states, gate_blocks, kraus_picks, block_targets)
    chunks = middle // peers
    kernel = functools.partial(
        circuit_kernel, peers, sections, blocks, qubits, chunks, amp_local * peers
    )
    f32 = jnp.float32
    dma = pltpu.SemaphoreType.DMA
    out, logs = pl.pallas_call(
        kernel,
        out_shape=(
            pltpu.VMEM((reg * middle, reg), f32),
            pltpu.VMEM((1, sections), f32),
        ),
        in_specs=[pl.BlockSpec(memory_space=pl.ANY)] * 4,
        out_specs=(
            pl.BlockSpec(memory_space=pltpu.VMEM),
            pl.BlockSpec(memory_space=pltpu.VMEM),
        ),
        scratch_shapes=[
            pltpu.VMEM((chunks, peers - 1, reg, reg), f32),
            pltpu.VMEM((chunks, peers, reg, reg), f32),
            pltpu.VMEM((chunks, peers, reg, reg), f32),
            pltpu.VMEM((sections, blocks, reg, reg), f32),
            pltpu.SMEM((1, blocks, sections, qubits), jnp.int32),
            pltpu.SMEM((sections, blocks), jnp.int32),
            pltpu.VMEM((sections, 2 * reg, 2 * reg), jnp.bfloat16),
            pltpu.VMEM((sections, reg, 2 * reg), jnp.bfloat16),
            pltpu.VMEM((sections + 1, 8, reg), f32),
            pltpu.VMEM((peers, 1, reg), f32),
            dma((3,)),
            dma,
            dma,
            dma,
            dma((chunks,)),
            dma((chunks + peers // 2,)),
            dma,
            pltpu.SemaphoreType.REGULAR((3,)),
        ],
        compiler_params=pltpu.CompilerParams(collective_id=0, has_side_effects=True),
    )(
        states.reshape(reg, middle, 1, reg),
        gate_blocks[0],
        jnp.swapaxes(kraus_picks, 1, 2),
        block_targets,
    )
    pieces = 8
    out, logs = pl.pallas_call(
        functools.partial(store_kernel, pieces),
        out_shape=(
            jax.ShapeDtypeStruct(out.shape, f32),
            jax.ShapeDtypeStruct(logs.shape, f32),
        ),
        in_specs=[pl.BlockSpec(memory_space=pltpu.VMEM)] * 2,
        out_specs=(pl.BlockSpec(memory_space=pl.ANY),) * 2,
        scratch_shapes=[dma, dma],
    )(
        pltpu.with_memory_space_constraint(out, pltpu.VMEM),
        pltpu.with_memory_space_constraint(logs, pltpu.VMEM),
    )
    return out.reshape(1, amp_local), logs


def solution(mesh):
    in_specs = (
        P("segment", "amp"),
        P("segment", None, None, None),
        P("segment", None, None, None),
        P(),
    )
    out_specs = (P("segment", "amp"), P("segment", None))
    return jax.shard_map(step, mesh=mesh, in_specs=in_specs, out_specs=out_specs, check_vma=False)
```

```python
import functools

import jax
import jax.numpy as jnp
from jax import lax
from jax.experimental import pallas as pl
from jax.experimental.pallas import tpu as pltpu
from jax.sharding import PartitionSpec as P

KEEP_FACTORS = (1.0, 0.9, 1.0, 0.97)
FLIP_FACTORS = (0.9, 1.0, 0.97, 1.0)
MESH = pl.DeviceIdType.MESH


def broadcast(block, axis, owner):
    block = jnp.where(lax.axis_index(axis) == owner, block, jnp.zeros_like(block))
    return lax.psum(block, axis)


def noise_factors(kraus_rows):
    qubit_count = kraus_rows.shape[-1]
    register = 2**qubit_count
    positions = jnp.arange(register, dtype=jnp.int32)
    product = jnp.ones(kraus_rows.shape[:-1] + (register,), jnp.float32)
    for qubit_pos in range(qubit_count):
        bit_value = jnp.right_shift(positions, qubit_count - 1 - qubit_pos) & 1
        column = kraus_rows[..., qubit_pos : qubit_pos + 1]
        low_value = jnp.zeros(column.shape, jnp.float32)
        high_value = jnp.zeros(column.shape, jnp.float32)
        for option in range(4):
            picked = (column == option).astype(jnp.float32)
            low_value = low_value + picked * KEEP_FACTORS[option]
            high_value = high_value + picked * FLIP_FACTORS[option]
        product = product * jnp.where(bit_value == 1, high_value, low_value)
    return product


def apply_gate(amplitudes, matrix, factors, target):

    def on_low(values):
        mixed_rows = jnp.einsum("bhmk,ik->bhmi", values, matrix, precision=lax.Precision.HIGHEST)
        return mixed_rows * factors[:, None, None, :]

    def on_high(values):
        mixed_rows = jnp.einsum("bjmk,ij->bimk", values, matrix, precision=lax.Precision.HIGHEST)
        return mixed_rows * factors[:, :, None, None]

    return lax.cond(target == 0, on_low, on_high, amplitudes)


def square_sums(values):
    return (values, jnp.sum(values * values, axis=(1, 2, 3)))


def body(states, gate_blocks, kraus_picks, block_targets):
    traj_here = states.shape[0]
    amp_local = states.shape[1]
    register = gate_blocks.shape[-1]
    blocks = gate_blocks.shape[1]
    middle = amp_local // (register * register)
    total_amps = amp_local * lax.axis_size("amp")
    sections = lax.axis_size("segment")
    amplitudes = states.reshape(traj_here, register, middle, register)
    first_local = jnp.sum(amplitudes * amplitudes, axis=(1, 2, 3))
    local_sums = [first_local]
    for section in range(sections):
        section_gates = broadcast(gate_blocks, "segment", section)[0]
        for block_pos in range(blocks):
            factors = noise_factors(kraus_picks[:, section, block_pos, :])
            amplitudes = apply_gate(
                amplitudes, section_gates[block_pos], factors, block_targets[section, block_pos]
            )
        amplitudes, local_sq = square_sums(
            lax.all_to_all(amplitudes, "amp", split_axis=1, concat_axis=1, tiled=True)
        )
        local_sums.append(local_sq)
    totals = lax.psum(jnp.stack(local_sums, axis=1), "amp")
    log_weights = jnp.log(totals[:, 1:] / totals[:, :-1])
    amplitudes = amplitudes / jnp.sqrt(totals[:, -1] / total_amps)[:, None, None, None]
    return (amplitudes.reshape(traj_here, amp_local), log_weights)


def partner(index, k):
    result = index
    bit = 1
    while bit <= k:
        if k & bit:
            result = result + bit * (1 - 2 * ((index // bit) % 2))
        bit *= 2
    return result


def split(values):
    high = values.astype(jnp.bfloat16)
    low = (values - high.astype(jnp.float32)).astype(jnp.bfloat16)
    return high, low


def left_form(matrix):
    return jnp.concatenate(split(matrix), axis=1)


def right_form(matrix):
    row = jnp.concatenate(split(matrix), axis=1)
    return jnp.concatenate([row, row], axis=0)


def multiply(left, right):
    both = jnp.dot(left, right, preferred_element_type=jnp.float32)
    half = both.shape[1] // 2
    return both[:, :half] + both[:, half:]


def fold_rows(values):
    squares = values * values
    return jnp.sum(squares.reshape(-1, 8, squares.shape[-1]), axis=0)


def row_factors(picks_ref, section, block, qubits, shape):
    positions = lax.broadcasted_iota(jnp.int32, shape, 0)
    product = jnp.ones(shape, jnp.float32)
    for q in range(qubits):
        pick = picks_ref[0, block, section, q]
        keep = jnp.float32(KEEP_FACTORS[0])
        flip = jnp.float32(FLIP_FACTORS[0])
        for option in range(1, 4):
            keep = jnp.where(pick == option, jnp.float32(KEEP_FACTORS[option]), keep)
            flip = jnp.where(pick == option, jnp.float32(FLIP_FACTORS[option]), flip)
        bit = jnp.right_shift(positions, qubits - 1 - q) & 1
        product = product * jnp.where(bit == 1, flip, keep)
    return product


def waits(like, semaphore):
    pltpu.make_async_copy(like, like, semaphore).wait()


def circuit_kernel(
    peers, sections, blocks, qubits, chunks, total_amps,
    x_hbm, gates_hbm, picks_hbm, targets_hbm,
    out_ref, logs_ref,
    xs, yin, ov, gates, picks, targets, low_form, high_form, partial, sums,
    x_sem, small_sem, sent, grecv, irecv, orecv, srecv,
    entered,
):
    seg = lax.axis_index("segment")
    amp = lax.axis_index("amp")
    reg = gates.shape[-1]
    middle = chunks * peers
    far = list(range(3 * peers // 4, peers))
    mid = list(range(peers // 2, 3 * peers // 4))
    near = list(range(peers // 2 - 1, 0, -1))
    groups = [far, mid, near]

    def tell(semaphore, axis, index, k):
        pl.semaphore_signal(
            semaphore, inc=1, device_id={axis: partner(index, k)}, device_id_type=MESH
        )

    quarter = reg // 4
    parts = [pl.ds(q * quarter, quarter) for q in range(4)]
    first, others = parts[0], pl.ds(quarter, reg - quarter)

    def load(chunk, k, semaphore, rows=pl.ds(0, reg)):
        m = chunk * peers + partner(amp, k)
        pltpu.make_async_copy(
            x_hbm.at[rows, m, 0], xs.at[chunk, k - 1, rows], semaphore
        ).start()

    for q, rows in enumerate(parts):
        for k in far:
            load(0, k, x_sem.at[min(q, 1)], rows)

    barrier = pltpu.get_barrier_semaphore()
    line = peers == 8 and sections == 4
    pair_at = amp // 2
    inner_pair = (pair_at + 1) // 2 % 2
    is_inner = inner_pair == 1
    first_core = amp % 2 * inner_pair
    second_core = inner_pair - first_core
    relays = second_core * (1 - pair_at // 2)
    beside = 1 - inner_pair + relays
    if line:

        tell(barrier, "amp", amp, 6)

        @pl.when(second_core == 0)
        def _():
            tell(barrier, "amp", amp, 7)
            tell(barrier, "amp", amp, 1)

        @pl.when(is_inner)
        def _():
            for k in (2, 3, 4, 5):
                tell(barrier, "amp", amp, k)

        @pl.when(beside == 1)
        def _():
            for k in (1, 2):
                tell(barrier, "segment", seg, k)
    else:
        for k in range(peers - 1, 0, -1):
            tell(barrier, "amp", amp, k)
        for k in range(1, sections):
            tell(barrier, "segment", seg, k)

    for k in mid + near:
        load(0, k, x_sem.at[2])
    for chunk in range(1, chunks):
        for k in far + mid + near:
            load(chunk, k, x_sem.at[2])
    pltpu.make_async_copy(gates_hbm, gates.at[seg], x_sem.at[2]).start()
    picks_load = pltpu.make_async_copy(picks_hbm, picks, small_sem)
    picks_load.start()
    targets_load = pltpu.make_async_copy(targets_hbm, targets, small_sem)
    targets_load.start()
    for chunk in range(chunks):
        pltpu.make_async_copy(
            x_hbm.at[:, chunk * peers + amp, 0], yin.at[chunk, amp], x_sem.at[2]
        ).start()

    def send_in(chunk, k, rows=pl.ds(0, reg)):
        pltpu.make_async_remote_copy(
            src_ref=xs.at[chunk, k - 1, rows],
            dst_ref=yin.at[chunk, amp, rows],
            send_sem=sent,
            recv_sem=irecv.at[chunk],
            device_id={"amp": partner(amp, k)},
            device_id_type=MESH,
        ).start()

    def far_loaded(at):
        waits(xs.at[0, : len(far), [first, others][at]], x_sem.at[at])

    def rest_loaded():
        waits(xs, x_sem.at[2])
        waits(gates.at[0], x_sem.at[2])

    if line:
        with jax.named_scope("barrier"):
            pl.semaphore_wait(
                barrier, 9 - 4 * inner_pair - 4 * first_core - 2 * (second_core - relays)
            )

        @pl.when(beside == 1)
        def _():
            for k in (1, 2):
                tell(entered.at[1], "segment", seg, k)

        @pl.when(pair_at == peers // 2 - 1)
        def _():
            tell(entered.at[0], "amp", amp, 2)
            tell(entered.at[0], "amp", amp, 4)

        for at, rows in enumerate((first, others)):
            with jax.named_scope("load0"):
                far_loaded(at)
            send_in(0, 6, rows)

            @pl.when(first_core == 0)
            def _(rows=rows):
                send_in(0, 7, rows)

        rest_loaded()
        send_in(1, 6)

        @pl.when(is_inner)
        def _():
            with jax.named_scope("ent0"):
                pl.semaphore_wait(entered.at[0], 1)

        @pl.when(first_core == 1)
        def _():
            send_in(0, 7)

        for k in [4, 5] + near:
            send_in(0, k)
        with jax.named_scope("ent1"):

            @pl.when(beside == 1)
            def _():
                pl.semaphore_wait(entered.at[1], 2)
                tell(entered.at[2], "segment", seg, 1)

            pl.semaphore_wait(entered.at[2], 1)

            @pl.when(relays == 1)
            def _():
                for k in (6, 7, 1):
                    tell(entered.at[2], "amp", amp, k)
    else:
        pl.semaphore_wait(barrier, peers - 1 + sections - 1)
        far_loaded(0)
        far_loaded(1)
        rest_loaded()
        for group in groups:
            for k in group:
                send_in(0, k)
    for k in range(1, sections):
        pltpu.make_async_remote_copy(
            src_ref=gates.at[seg],
            dst_ref=gates.at[seg],
            send_sem=sent,
            recv_sem=grecv,
            device_id={"segment": partner(seg, k)},
            device_id_type=MESH,
        ).start()
    for chunk in range(1, chunks):
        for k in far + mid + near:
            if not (line and chunk == 1 and k == 6):
                send_in(chunk, k)
    picks_load.wait()
    targets_load.wait()
    with jax.named_scope("gates"):
        waits(gates.at[1:], grecv)

    rows_at = lax.broadcasted_iota(jnp.int32, (reg, reg), 0)
    columns_at = lax.broadcasted_iota(jnp.int32, (reg, reg), 1)
    identity = jnp.where(rows_at == columns_at, jnp.float32(1.0), jnp.float32(0.0))

    def build(section, carry):
        low = high = None
        for b in range(blocks):
            factors = row_factors(picks, section, b, qubits, (reg, reg))
            damped = gates[section, b] * factors
            is_low = targets[section, b] == 0
            for_low = jnp.where(is_low, damped, identity)
            for_high = jnp.where(is_low, identity, damped)
            if b == 0:
                low, high = for_low, for_high
            else:
                low = multiply(left_form(for_low), right_form(low))
                high = multiply(left_form(for_high), right_form(high))
        low_form[section] = right_form(low.T)
        high_form[section] = left_form(high)
        return carry

    with jax.named_scope("build"):
        lax.fori_loop(0, sections, build, 0)

    inner = reg // peers
    lanes = lax.broadcasted_iota(jnp.int32, (1, reg), 1)
    partial[...] = jnp.zeros_like(partial)

    def apply_section(chunk, section, swapped):
        low = low_form[section]
        high = high_form[section]
        total = jnp.zeros((8, reg), jnp.float32)
        for slab in range(peers):
            if swapped:
                value = yin[chunk, :, slab * inner : (slab + 1) * inner, :].reshape(reg, reg)
            else:
                value = yin[chunk, slab]
            value = multiply(left_form(value), low)
            value = multiply(high, right_form(value))
            total = total + fold_rows(value)
            if swapped:
                yin[chunk, :, slab * inner : (slab + 1) * inner, :] = value.reshape(
                    peers, inner, reg
                )
            else:
                yin[chunk, slab] = value
        partial[section + 1] = partial[section + 1] + total

    order_out = mid + far + near

    def arrival(chunk, k):
        slot = max(k - peers // 2 + 1, 0)
        return chunk + slot * (chunk // (chunks - 1))

    def run_chunk(chunk, carry):
        with jax.named_scope("in"):
            waits(xs.at[chunk], irecv.at[chunk])
        first = jnp.zeros((8, reg), jnp.float32)
        for slab in range(peers):
            first = first + fold_rows(yin[chunk, slab])
        partial[0] = partial[0] + first

        def pair(i, inner_carry):
            apply_section(chunk, 2 * i, False)
            apply_section(chunk, 2 * i + 1, True)
            return inner_carry

        with jax.named_scope("comp"):
            lax.fori_loop(0, sections // 2, pair, 0)

        @pl.when(chunk == chunks - 1)
        def _():
            row = jnp.zeros((1, reg), jnp.float32)
            for s in range(sections + 1):
                total = jnp.sum(jnp.sum(partial[s], axis=0, keepdims=True), axis=1, keepdims=True)
                row = jnp.where(lanes == s, total, row)
            sums[amp] = row
            for k in range(peers - 1, 0, -1):
                pltpu.make_async_remote_copy(
                    src_ref=sums.at[amp],
                    dst_ref=sums.at[amp],
                    send_sem=sent,
                    recv_sem=srecv,
                    device_id={"amp": partner(amp, k)},
                    device_id_type=MESH,
                ).start()

        for k in order_out:
            peer = partner(amp, k)
            pltpu.make_async_remote_copy(
                src_ref=yin.at[chunk, peer],
                dst_ref=ov.at[chunk, amp],
                send_sem=sent,
                recv_sem=orecv.at[arrival(chunk, k)],
                device_id={"amp": peer},
                device_id_type=MESH,
            ).start()
        return carry

    lax.fori_loop(0, chunks, run_chunk, 0)

    with jax.named_scope("sums"):
        waits(sums.at[1:], srecv)
    row = sums[0]
    for d in range(1, peers):
        row = row + sums[d]
    totals = [
        jnp.sum(jnp.where(lanes == s, row, 0.0), axis=1, keepdims=True)
        for s in range(sections + 1)
    ]
    logs = jnp.zeros((1, reg), jnp.float32)
    for s in range(sections):
        logs = jnp.where(lanes == s, jnp.log(totals[s + 1] / totals[s]), logs)
    logs_ref[...] = logs[:, :sections]
    scale = 1.0 / jnp.sqrt(totals[sections] / total_amps)
    scale = jnp.broadcast_to(scale, (1, reg))

    for chunk in range(chunks):
        m = chunk * peers + amp
        out_ref[pl.ds(m, reg, stride=middle), :] = yin[chunk, amp] * scale
    def place(chunk, peer):
        m = chunk * peers + peer
        out_ref[pl.ds(m, reg, stride=middle), :] = ov[chunk, peer] * scale

    last = chunks - 1
    for chunk in range(last):
        waits(xs.at[0], orecv.at[chunk])
        for k in order_out:
            place(chunk, partner(amp, k))
    with jax.named_scope("out_near"):
        waits(xs.at[0, : len(near)], orecv.at[last])
    for k in near:
        place(last, partner(amp, k))
    half = peers // 2
    for at in range(half):
        ahead = (at + half // 2) % half
        slot = inner_pair * at + (1 - inner_pair) * ahead
        peer = inner_pair * partner(amp, half + at) + (1 - inner_pair) * partner(amp, half + ahead)
        with jax.named_scope(f"out_{at}"):
            waits(xs.at[0, 0], orecv.at[last + 1 + slot])
        place(last, peer)

    with jax.named_scope("sendwait"):
        waits(xs, sent)
        waits(xs, sent)
        waits(gates.at[1:], sent)
        waits(sums.at[1:], sent)


def store_kernel(pieces, out_vmem, logs_vmem, out_hbm, logs_hbm, out_sem, logs_sem):
    rows = out_vmem.shape[0] // pieces
    for p in range(pieces):
        at = pl.ds(p * rows, rows)
        pltpu.make_async_copy(out_vmem.at[at], out_hbm.at[at], out_sem).start()
    logs_copy = pltpu.make_async_copy(logs_vmem, logs_hbm, logs_sem)
    logs_copy.start()
    pltpu.make_async_copy(out_vmem, out_hbm, out_sem).wait()
    logs_copy.wait()


def step(states, gate_blocks, kraus_picks, block_targets):
    traj_here, amp_local = states.shape
    reg = gate_blocks.shape[-1]
    blocks = gate_blocks.shape[1]
    qubits = kraus_picks.shape[-1]
    peers = lax.axis_size("amp")
    sections = lax.axis_size("segment")
    middle = amp_local // (reg * reg)
    fits = (
        traj_here == 1
        and gate_blocks.shape[0] == 1
        and middle % peers == 0
        and peers & (peers - 1) == 0
        and peers >= 8
        and middle == peers * (peers // 4)
        and middle > peers
        and sections & (sections - 1) == 0
        and sections % 2 == 0
        and sections < 8
        and reg == 128
        and reg % (8 * peers) == 0
    )
    if not fits:
        return body(states, gate_blocks, kraus_picks, block_targets)
    chunks = middle // peers
    kernel = functools.partial(
        circuit_kernel, peers, sections, blocks, qubits, chunks, amp_local * peers
    )
    f32 = jnp.float32
    dma = pltpu.SemaphoreType.DMA
    out, logs = pl.pallas_call(
        kernel,
        out_shape=(
            pltpu.VMEM((reg * middle, reg), f32),
            pltpu.VMEM((1, sections), f32),
        ),
        in_specs=[pl.BlockSpec(memory_space=pl.ANY)] * 4,
        out_specs=(
            pl.BlockSpec(memory_space=pltpu.VMEM),
            pl.BlockSpec(memory_space=pltpu.VMEM),
        ),
        scratch_shapes=[
            pltpu.VMEM((chunks, peers - 1, reg, reg), f32),
            pltpu.VMEM((chunks, peers, reg, reg), f32),
            pltpu.VMEM((chunks, peers, reg, reg), f32),
            pltpu.VMEM((sections, blocks, reg, reg), f32),
            pltpu.SMEM((1, blocks, sections, qubits), jnp.int32),
            pltpu.SMEM((sections, blocks), jnp.int32),
            pltpu.VMEM((sections, 2 * reg, 2 * reg), jnp.bfloat16),
            pltpu.VMEM((sections, reg, 2 * reg), jnp.bfloat16),
            pltpu.VMEM((sections + 1, 8, reg), f32),
            pltpu.VMEM((peers, 1, reg), f32),
            dma((3,)),
            dma,
            dma,
            dma,
            dma((chunks,)),
            dma((chunks + peers // 2,)),
            dma,
            pltpu.SemaphoreType.REGULAR((3,)),
        ],
        compiler_params=pltpu.CompilerParams(collective_id=0, has_side_effects=True),
    )(
        states.reshape(reg, middle, 1, reg),
        gate_blocks[0],
        jnp.swapaxes(kraus_picks, 1, 2),
        block_targets,
    )
    pieces = 8
    out, logs = pl.pallas_call(
        functools.partial(store_kernel, pieces),
        out_shape=(
            jax.ShapeDtypeStruct(out.shape, f32),
            jax.ShapeDtypeStruct(logs.shape, f32),
        ),
        in_specs=[pl.BlockSpec(memory_space=pltpu.VMEM)] * 2,
        out_specs=(pl.BlockSpec(memory_space=pl.ANY),) * 2,
        scratch_shapes=[dma, dma],
    )(
        pltpu.with_memory_space_constraint(out, pltpu.VMEM),
        pltpu.with_memory_space_constraint(logs, pltpu.VMEM),
    )
    return out.reshape(1, amp_local), logs


def solution(mesh):
    in_specs = (
        P("segment", "amp"),
        P("segment", None, None, None),
        P("segment", None, None, None),
        P(),
    )
    out_specs = (P("segment", "amp"), P("segment", None))
    return jax.shard_map(step, mesh=mesh, in_specs=in_specs, out_specs=out_specs, check_vma=False)
```

```python
import functools

import jax
import jax.numpy as jnp
from jax import lax
from jax.experimental import pallas as pl
from jax.experimental.pallas import tpu as pltpu
from jax.sharding import PartitionSpec as P

KEEP_FACTORS = (1.0, 0.9, 1.0, 0.97)
FLIP_FACTORS = (0.9, 1.0, 0.97, 1.0)
MESH = pl.DeviceIdType.MESH


def broadcast(block, axis, owner):
    block = jnp.where(lax.axis_index(axis) == owner, block, jnp.zeros_like(block))
    return lax.psum(block, axis)


def noise_factors(kraus_rows):
    qubit_count = kraus_rows.shape[-1]
    register = 2**qubit_count
    positions = jnp.arange(register, dtype=jnp.int32)
    product = jnp.ones(kraus_rows.shape[:-1] + (register,), jnp.float32)
    for qubit_pos in range(qubit_count):
        bit_value = jnp.right_shift(positions, qubit_count - 1 - qubit_pos) & 1
        column = kraus_rows[..., qubit_pos : qubit_pos + 1]
        low_value = jnp.zeros(column.shape, jnp.float32)
        high_value = jnp.zeros(column.shape, jnp.float32)
        for option in range(4):
            picked = (column == option).astype(jnp.float32)
            low_value = low_value + picked * KEEP_FACTORS[option]
            high_value = high_value + picked * FLIP_FACTORS[option]
        product = product * jnp.where(bit_value == 1, high_value, low_value)
    return product


def apply_gate(amplitudes, matrix, factors, target):

    def on_low(values):
        mixed_rows = jnp.einsum("bhmk,ik->bhmi", values, matrix, precision=lax.Precision.HIGHEST)
        return mixed_rows * factors[:, None, None, :]

    def on_high(values):
        mixed_rows = jnp.einsum("bjmk,ij->bimk", values, matrix, precision=lax.Precision.HIGHEST)
        return mixed_rows * factors[:, :, None, None]

    return lax.cond(target == 0, on_low, on_high, amplitudes)


def square_sums(values):
    return (values, jnp.sum(values * values, axis=(1, 2, 3)))


def body(states, gate_blocks, kraus_picks, block_targets):
    traj_here = states.shape[0]
    amp_local = states.shape[1]
    register = gate_blocks.shape[-1]
    blocks = gate_blocks.shape[1]
    middle = amp_local // (register * register)
    total_amps = amp_local * lax.axis_size("amp")
    sections = lax.axis_size("segment")
    amplitudes = states.reshape(traj_here, register, middle, register)
    first_local = jnp.sum(amplitudes * amplitudes, axis=(1, 2, 3))
    local_sums = [first_local]
    for section in range(sections):
        section_gates = broadcast(gate_blocks, "segment", section)[0]
        for block_pos in range(blocks):
            factors = noise_factors(kraus_picks[:, section, block_pos, :])
            amplitudes = apply_gate(
                amplitudes, section_gates[block_pos], factors, block_targets[section, block_pos]
            )
        amplitudes, local_sq = square_sums(
            lax.all_to_all(amplitudes, "amp", split_axis=1, concat_axis=1, tiled=True)
        )
        local_sums.append(local_sq)
    totals = lax.psum(jnp.stack(local_sums, axis=1), "amp")
    log_weights = jnp.log(totals[:, 1:] / totals[:, :-1])
    amplitudes = amplitudes / jnp.sqrt(totals[:, -1] / total_amps)[:, None, None, None]
    return (amplitudes.reshape(traj_here, amp_local), log_weights)


def quotient(index, divisor):
    return index if divisor == 1 else lax.div(index, jnp.int32(divisor))


def partner(index, k):
    result = index
    bit = 1
    while bit <= k:
        if k & bit:
            result = result + bit * (1 - 2 * lax.rem(quotient(index, bit), jnp.int32(2)))
        bit *= 2
    return result


def split(values):
    high = values.astype(jnp.bfloat16)
    low = (values - high.astype(jnp.float32)).astype(jnp.bfloat16)
    return high, low


def left_form(matrix):
    return jnp.concatenate(split(matrix), axis=1)


def right_form(matrix):
    row = jnp.concatenate(split(matrix), axis=1)
    return jnp.concatenate([row, row], axis=0)


def multiply(left, right):
    both = jnp.dot(left, right, preferred_element_type=jnp.float32)
    half = both.shape[1] // 2
    return both[:, :half] + both[:, half:]


def fold_rows(values):
    squares = values * values
    return jnp.sum(squares.reshape(-1, 8, squares.shape[-1]), axis=0)


def row_factors(picks_ref, section, block, qubits, shape):
    positions = lax.broadcasted_iota(jnp.int32, shape, 0)
    product = jnp.ones(shape, jnp.float32)
    for q in range(qubits):
        pick = picks_ref[0, block, section, q]
        keep = jnp.float32(KEEP_FACTORS[0])
        flip = jnp.float32(FLIP_FACTORS[0])
        for option in range(1, 4):
            keep = jnp.where(pick == option, jnp.float32(KEEP_FACTORS[option]), keep)
            flip = jnp.where(pick == option, jnp.float32(FLIP_FACTORS[option]), flip)
        bit = jnp.right_shift(positions, qubits - 1 - q) & 1
        product = product * jnp.where(bit == 1, flip, keep)
    return product


def waits(like, semaphore):
    pltpu.make_async_copy(like, like, semaphore).wait()


def circuit_kernel(
    peers, sections, blocks, qubits, chunks, total_amps,
    x_hbm, gates_hbm, picks_hbm, targets_hbm,
    out_ref, logs_ref,
    xs, yin, ov, gates, picks, targets, low_form, high_form, partial, sums,
    x_sem, sent, grecv, irecv, orecv, srecv,
    entered,
):
    seg = lax.axis_index("segment")
    amp = lax.axis_index("amp")
    reg = gates.shape[-1]
    middle = chunks * peers
    far = list(range(3 * peers // 4, peers))
    mid = list(range(peers // 2, 3 * peers // 4))
    near = list(range(peers // 2 - 1, 0, -1))
    groups = [far, mid, near]

    def tell(semaphore, axis, index, k):
        pl.semaphore_signal(
            semaphore, inc=1, device_id={axis: partner(index, k)}, device_id_type=MESH
        )

    quarter = reg // 4
    parts = [pl.ds(q * quarter, quarter) for q in range(4)]
    first, others = parts[0], pl.ds(quarter, reg - quarter)

    def load(chunk, k, semaphore, rows=pl.ds(0, reg)):
        m = chunk * peers + partner(amp, k)
        pltpu.make_async_copy(
            x_hbm.at[rows, m, 0], xs.at[chunk, k - 1, rows], semaphore
        ).start()

    for q, rows in enumerate(parts):
        for k in far:
            load(0, k, x_sem.at[min(q, 1)], rows)

    barrier = pltpu.get_barrier_semaphore()
    line = peers == 8 and sections == 4
    pair_at = quotient(amp, 2)
    inner_pair = lax.rem(quotient(pair_at + 1, 2), jnp.int32(2))
    is_inner = inner_pair == 1
    first_core = lax.rem(amp, jnp.int32(2)) * inner_pair
    second_core = inner_pair - first_core
    relays = second_core * (1 - quotient(pair_at, 2))
    beside = 1 - inner_pair + relays
    if line:

        tell(barrier, "amp", amp, 6)

        @pl.when(second_core == 0)
        def _():
            tell(barrier, "amp", amp, 7)
            tell(barrier, "amp", amp, 1)

        @pl.when(is_inner)
        def _():
            for k in (2, 3, 4, 5):
                tell(barrier, "amp", amp, k)

        @pl.when(beside == 1)
        def _():
            for k in (1, 2):
                tell(barrier, "segment", seg, k)
    else:
        for k in range(peers - 1, 0, -1):
            tell(barrier, "amp", amp, k)
        for k in range(1, sections):
            tell(barrier, "segment", seg, k)

    for k in mid + near:
        load(0, k, x_sem.at[2])
    for chunk in range(1, chunks):
        for k in far + mid + near:
            load(chunk, k, x_sem.at[2])
    pltpu.make_async_copy(gates_hbm, gates.at[seg], x_sem.at[2]).start()
    picks_load = pltpu.make_async_copy(picks_hbm, picks, x_sem.at[2])
    picks_load.start()
    targets_load = pltpu.make_async_copy(targets_hbm, targets, x_sem.at[2])
    targets_load.start()
    for chunk in range(chunks):
        pltpu.make_async_copy(
            x_hbm.at[:, chunk * peers + amp, 0], yin.at[chunk, amp], x_sem.at[2]
        ).start()

    def send_in(chunk, k, rows=pl.ds(0, reg)):
        pltpu.make_async_remote_copy(
            src_ref=xs.at[chunk, k - 1, rows],
            dst_ref=yin.at[chunk, amp, rows],
            send_sem=sent,
            recv_sem=irecv.at[chunk],
            device_id={"amp": partner(amp, k)},
            device_id_type=MESH,
        ).start()

    def far_loaded(at):
        waits(xs.at[0, : len(far), [first, others][at]], x_sem.at[at])

    def rest_loaded():
        waits(xs, x_sem.at[2])
        waits(gates.at[0], x_sem.at[2])
        picks_load.wait()
        targets_load.wait()

    if line:
        with jax.named_scope("barrier"):
            pl.semaphore_wait(
                barrier, 9 - 4 * inner_pair - 4 * first_core - 2 * (second_core - relays)
            )

        @pl.when(beside == 1)
        def _():
            for k in (1, 2):
                tell(entered.at[1], "segment", seg, k)

        @pl.when(pair_at == peers // 2 - 1)
        def _():
            tell(entered.at[0], "amp", amp, 2)
            tell(entered.at[0], "amp", amp, 4)

        for at, rows in enumerate((first, others)):
            with jax.named_scope("load0"):
                far_loaded(at)
            send_in(0, 6, rows)

            @pl.when(first_core == 0)
            def _(rows=rows):
                send_in(0, 7, rows)

        rest_loaded()
        send_in(1, 6)

        @pl.when(is_inner)
        def _():
            with jax.named_scope("ent0"):
                pl.semaphore_wait(entered.at[0], 1)

        @pl.when(first_core == 1)
        def _():
            send_in(0, 7)

        for k in [4, 5] + near:
            send_in(0, k)
        with jax.named_scope("ent1"):

            @pl.when(beside == 1)
            def _():
                pl.semaphore_wait(entered.at[1], 2)
                tell(entered.at[2], "segment", seg, 1)

            pl.semaphore_wait(entered.at[2], 1)

            @pl.when(relays == 1)
            def _():
                for k in (6, 7, 1):
                    tell(entered.at[2], "amp", amp, k)
    else:
        pl.semaphore_wait(barrier, peers - 1 + sections - 1)
        far_loaded(0)
        far_loaded(1)
        rest_loaded()
        for group in groups:
            for k in group:
                send_in(0, k)
    for k in range(1, sections):
        pltpu.make_async_remote_copy(
            src_ref=gates.at[seg],
            dst_ref=gates.at[seg],
            send_sem=sent,
            recv_sem=grecv,
            device_id={"segment": partner(seg, k)},
            device_id_type=MESH,
        ).start()
    for chunk in range(1, chunks):
        for k in far + mid + near:
            if not (line and chunk == 1 and k == 6):
                send_in(chunk, k)
    with jax.named_scope("gates"):
        waits(gates.at[1:], grecv)

    rows_at = lax.broadcasted_iota(jnp.int32, (reg, reg), 0)
    columns_at = lax.broadcasted_iota(jnp.int32, (reg, reg), 1)
    identity = jnp.where(rows_at == columns_at, jnp.float32(1.0), jnp.float32(0.0))

    def build(section, carry):
        low = high = None
        for b in range(blocks):
            factors = row_factors(picks, section, b, qubits, (reg, reg))
            damped = gates[section, b] * factors
            is_low = targets[section, b] == 0
            for_low = jnp.where(is_low, damped, identity)
            for_high = jnp.where(is_low, identity, damped)
            if b == 0:
                low, high = for_low, for_high
            else:
                low = multiply(left_form(for_low), right_form(low))
                high = multiply(left_form(for_high), right_form(high))
        low_form[section] = right_form(low.T)
        high_form[section] = left_form(high)
        return carry

    with jax.named_scope("build"):
        lax.fori_loop(0, sections, build, 0)

    inner = reg // peers
    lanes = lax.broadcasted_iota(jnp.int32, (1, reg), 1)
    partial[...] = jnp.zeros_like(partial)

    def apply_section(chunk, section, swapped):
        low = low_form[section]
        high = high_form[section]
        total = jnp.zeros((8, reg), jnp.float32)
        for slab in range(peers):
            if swapped:
                value = yin[chunk, :, slab * inner : (slab + 1) * inner, :].reshape(reg, reg)
            else:
                value = yin[chunk, slab]
            value = multiply(left_form(value), low)
            value = multiply(high, right_form(value))
            total = total + fold_rows(value)
            if swapped:
                yin[chunk, :, slab * inner : (slab + 1) * inner, :] = value.reshape(
                    peers, inner, reg
                )
            else:
                yin[chunk, slab] = value
        partial[section + 1] = partial[section + 1] + total

    order_out = mid + far + near

    def arrival(chunk, k):
        slot = 0
        if k >= peers // 2:
            slot = 1 + inner_pair * (1 + k % 2) if line else 1
        return chunk + slot * quotient(chunk, chunks - 1)

    def run_chunk(chunk, carry):
        with jax.named_scope("in"):
            waits(xs.at[chunk], irecv.at[chunk])
        first = jnp.zeros((8, reg), jnp.float32)
        for slab in range(peers):
            first = first + fold_rows(yin[chunk, slab])
        partial[0] = partial[0] + first

        def pair(i, inner_carry):
            apply_section(chunk, 2 * i, False)
            apply_section(chunk, 2 * i + 1, True)
            return inner_carry

        with jax.named_scope("comp"):
            lax.fori_loop(0, sections // 2, pair, 0)

        @pl.when(chunk == chunks - 1)
        def _():
            row = jnp.zeros((1, reg), jnp.float32)
            for s in range(sections + 1):
                total = jnp.sum(jnp.sum(partial[s], axis=0, keepdims=True), axis=1, keepdims=True)
                row = jnp.where(lanes == s, total, row)
            sums[amp] = row
            for k in range(peers - 1, 0, -1):
                pltpu.make_async_remote_copy(
                    src_ref=sums.at[amp],
                    dst_ref=sums.at[amp],
                    send_sem=sent,
                    recv_sem=srecv,
                    device_id={"amp": partner(amp, k)},
                    device_id_type=MESH,
                ).start()

        for k in order_out:
            peer = partner(amp, k)
            pltpu.make_async_remote_copy(
                src_ref=yin.at[chunk, peer],
                dst_ref=ov.at[chunk, amp],
                send_sem=sent,
                recv_sem=orecv.at[arrival(chunk, k)],
                device_id={"amp": peer},
                device_id_type=MESH,
            ).start()
        return carry

    lax.fori_loop(0, chunks, run_chunk, 0)

    with jax.named_scope("sums"):
        waits(sums.at[1:], srecv)
    row = sums[0]
    for d in range(1, peers):
        row = row + sums[d]
    totals = [
        jnp.sum(jnp.where(lanes == s, row, 0.0), axis=1, keepdims=True)
        for s in range(sections + 1)
    ]
    logs = jnp.zeros((1, reg), jnp.float32)
    for s in range(sections):
        logs = jnp.where(lanes == s, jnp.log(totals[s + 1] / totals[s]), logs)
    logs_ref[...] = logs[:, :sections]
    scale = 1.0 / jnp.sqrt(totals[sections] / total_amps)
    scale = jnp.broadcast_to(scale, (1, reg))

    for chunk in range(chunks):
        m = chunk * peers + amp
        out_ref[pl.ds(m, reg, stride=middle), :] = yin[chunk, amp] * scale
    def place(chunk, peer):
        m = chunk * peers + peer
        out_ref[pl.ds(m, reg, stride=middle), :] = ov[chunk, peer] * scale

    last = chunks - 1
    for chunk in range(last):
        waits(xs.at[0], orecv.at[chunk])
        for k in order_out:
            place(chunk, partner(amp, k))
    with jax.named_scope("out_near"):
        waits(xs.at[0, : len(near)], orecv.at[last])
    for k in near:
        place(last, partner(amp, k))
    if line:
        late = [
            inner_pair * partner(amp, 6 + at) + (1 - inner_pair) * partner(amp, 4 + at)
            for at in range(2)
        ]
        soon = [
            inner_pair * partner(amp, 4 + at) + (1 - inner_pair) * partner(amp, 6 + at)
            for at in range(2)
        ]
        with jax.named_scope("out_soon"):
            waits(xs.at[0, :2], orecv.at[last + 1])
        for peer in soon:
            place(last, peer)
        for at in range(2):
            with jax.named_scope(f"out_{at}"):
                waits(xs.at[0, 0], orecv.at[last + 2 + at])
            place(last, late[at])
    else:
        waits(xs.at[0, : peers // 2], orecv.at[last + 1])
        for k in far + mid:
            place(last, partner(amp, k))

    with jax.named_scope("sendwait"):
        waits(xs, sent)
        waits(xs, sent)
        waits(gates.at[1:], sent)
        waits(sums.at[1:], sent)


def store_kernel(pieces, out_vmem, logs_vmem, out_hbm, logs_hbm, out_sem, logs_sem):
    rows = out_vmem.shape[0] // pieces
    for p in range(pieces):
        at = pl.ds(p * rows, rows)
        pltpu.make_async_copy(out_vmem.at[at], out_hbm.at[at], out_sem).start()
    logs_copy = pltpu.make_async_copy(logs_vmem, logs_hbm, logs_sem)
    logs_copy.start()
    pltpu.make_async_copy(out_vmem, out_hbm, out_sem).wait()
    logs_copy.wait()


def step(states, gate_blocks, kraus_picks, block_targets):
    traj_here, amp_local = states.shape
    reg = gate_blocks.shape[-1]
    blocks = gate_blocks.shape[1]
    qubits = kraus_picks.shape[-1]
    peers = lax.axis_size("amp")
    sections = lax.axis_size("segment")
    middle = amp_local // (reg * reg)
    fits = (
        traj_here == 1
        and gate_blocks.shape[0] == 1
        and middle % peers == 0
        and peers & (peers - 1) == 0
        and peers >= 8
        and middle == peers * (peers // 4)
        and middle > peers
        and sections & (sections - 1) == 0
        and sections % 2 == 0
        and sections < 8
        and reg == 128
        and reg % (8 * peers) == 0
    )
    if not fits:
        return body(states, gate_blocks, kraus_picks, block_targets)
    chunks = middle // peers
    kernel = functools.partial(
        circuit_kernel, peers, sections, blocks, qubits, chunks, amp_local * peers
    )
    f32 = jnp.float32
    dma = pltpu.SemaphoreType.DMA
    out, logs = pl.pallas_call(
        kernel,
        out_shape=(
            pltpu.VMEM((reg * middle, reg), f32),
            pltpu.VMEM((1, sections), f32),
        ),
        in_specs=[pl.BlockSpec(memory_space=pl.ANY)] * 4,
        out_specs=(
            pl.BlockSpec(memory_space=pltpu.VMEM),
            pl.BlockSpec(memory_space=pltpu.VMEM),
        ),
        scratch_shapes=[
            pltpu.VMEM((chunks, peers - 1, reg, reg), f32),
            pltpu.VMEM((chunks, peers, reg, reg), f32),
            pltpu.VMEM((chunks, peers, reg, reg), f32),
            pltpu.VMEM((sections, blocks, reg, reg), f32),
            pltpu.SMEM((1, blocks, sections, qubits), jnp.int32),
            pltpu.SMEM((sections, blocks), jnp.int32),
            pltpu.VMEM((sections, 2 * reg, 2 * reg), jnp.bfloat16),
            pltpu.VMEM((sections, reg, 2 * reg), jnp.bfloat16),
            pltpu.VMEM((sections + 1, 8, reg), f32),
            pltpu.VMEM((peers, 1, reg), f32),
            dma((3,)),
            dma,
            dma,
            dma((chunks,)),
            dma((chunks + 3,)),
            dma,
            pltpu.SemaphoreType.REGULAR((3,)),
        ],
        compiler_params=pltpu.CompilerParams(collective_id=0, has_side_effects=True),
    )(
        states.reshape(reg, middle, 1, reg),
        gate_blocks[0],
        jnp.swapaxes(kraus_picks, 1, 2),
        block_targets,
    )
    pieces = 8
    out, logs = pl.pallas_call(
        functools.partial(store_kernel, pieces),
        out_shape=(
            jax.ShapeDtypeStruct(out.shape, f32),
            jax.ShapeDtypeStruct(logs.shape, f32),
        ),
        in_specs=[pl.BlockSpec(memory_space=pltpu.VMEM)] * 2,
        out_specs=(pl.BlockSpec(memory_space=pl.ANY),) * 2,
        scratch_shapes=[dma, dma],
    )(
        pltpu.with_memory_space_constraint(out, pltpu.VMEM),
        pltpu.with_memory_space_constraint(logs, pltpu.VMEM),
    )
    return out.reshape(1, amp_local), logs


def solution(mesh):
    in_specs = (
        P("segment", "amp"),
        P("segment", None, None, None),
        P("segment", None, None, None),
        P(),
    )
    out_specs = (P("segment", "amp"), P("segment", None))
    return jax.shard_map(step, mesh=mesh, in_specs=in_specs, out_specs=out_specs, check_vma=False)
```

```python
import functools

import jax
import jax.numpy as jnp
from jax import lax
from jax.experimental import pallas as pl
from jax.experimental.pallas import tpu as pltpu
from jax.sharding import PartitionSpec as P

KEEP_FACTORS = (1.0, 0.9, 1.0, 0.97)
FLIP_FACTORS = (0.9, 1.0, 0.97, 1.0)
MESH = pl.DeviceIdType.MESH


def broadcast(block, axis, owner):
    block = jnp.where(lax.axis_index(axis) == owner, block, jnp.zeros_like(block))
    return lax.psum(block, axis)


def noise_factors(kraus_rows):
    qubit_count = kraus_rows.shape[-1]
    register = 2**qubit_count
    positions = jnp.arange(register, dtype=jnp.int32)
    product = jnp.ones(kraus_rows.shape[:-1] + (register,), jnp.float32)
    for qubit_pos in range(qubit_count):
        bit_value = jnp.right_shift(positions, qubit_count - 1 - qubit_pos) & 1
        column = kraus_rows[..., qubit_pos : qubit_pos + 1]
        low_value = jnp.zeros(column.shape, jnp.float32)
        high_value = jnp.zeros(column.shape, jnp.float32)
        for option in range(4):
            picked = (column == option).astype(jnp.float32)
            low_value = low_value + picked * KEEP_FACTORS[option]
            high_value = high_value + picked * FLIP_FACTORS[option]
        product = product * jnp.where(bit_value == 1, high_value, low_value)
    return product


def apply_gate(amplitudes, matrix, factors, target):

    def on_low(values):
        mixed_rows = jnp.einsum("bhmk,ik->bhmi", values, matrix, precision=lax.Precision.HIGHEST)
        return mixed_rows * factors[:, None, None, :]

    def on_high(values):
        mixed_rows = jnp.einsum("bjmk,ij->bimk", values, matrix, precision=lax.Precision.HIGHEST)
        return mixed_rows * factors[:, :, None, None]

    return lax.cond(target == 0, on_low, on_high, amplitudes)


def square_sums(values):
    return (values, jnp.sum(values * values, axis=(1, 2, 3)))


def body(states, gate_blocks, kraus_picks, block_targets):
    traj_here = states.shape[0]
    amp_local = states.shape[1]
    register = gate_blocks.shape[-1]
    blocks = gate_blocks.shape[1]
    middle = amp_local // (register * register)
    total_amps = amp_local * lax.axis_size("amp")
    sections = lax.axis_size("segment")
    amplitudes = states.reshape(traj_here, register, middle, register)
    first_local = jnp.sum(amplitudes * amplitudes, axis=(1, 2, 3))
    local_sums = [first_local]
    for section in range(sections):
        section_gates = broadcast(gate_blocks, "segment", section)[0]
        for block_pos in range(blocks):
            factors = noise_factors(kraus_picks[:, section, block_pos, :])
            amplitudes = apply_gate(
                amplitudes, section_gates[block_pos], factors, block_targets[section, block_pos]
            )
        amplitudes, local_sq = square_sums(
            lax.all_to_all(amplitudes, "amp", split_axis=1, concat_axis=1, tiled=True)
        )
        local_sums.append(local_sq)
    totals = lax.psum(jnp.stack(local_sums, axis=1), "amp")
    log_weights = jnp.log(totals[:, 1:] / totals[:, :-1])
    amplitudes = amplitudes / jnp.sqrt(totals[:, -1] / total_amps)[:, None, None, None]
    return (amplitudes.reshape(traj_here, amp_local), log_weights)


def quotient(index, divisor):
    return index if divisor == 1 else lax.div(index, jnp.int32(divisor))


def partner(index, k):
    result = index
    bit = 1
    while bit <= k:
        if k & bit:
            result = result + bit * (1 - 2 * lax.rem(quotient(index, bit), jnp.int32(2)))
        bit *= 2
    return result


def split(values):
    high = values.astype(jnp.bfloat16)
    low = (values - high.astype(jnp.float32)).astype(jnp.bfloat16)
    return high, low


def left_form(matrix):
    return jnp.concatenate(split(matrix), axis=1)


def right_form(matrix):
    row = jnp.concatenate(split(matrix), axis=1)
    return jnp.concatenate([row, row], axis=0)


def multiply(left, right):
    both = jnp.dot(left, right, preferred_element_type=jnp.float32)
    half = both.shape[1] // 2
    return both[:, :half] + both[:, half:]


def fold_rows(values):
    squares = values * values
    return jnp.sum(squares.reshape(-1, 8, squares.shape[-1]), axis=0)


def row_factors(picks_ref, section, block, qubits, shape):
    positions = lax.broadcasted_iota(jnp.int32, shape, 0)
    product = jnp.ones(shape, jnp.float32)
    for q in range(qubits):
        pick = picks_ref[0, block, section, q]
        keep = jnp.float32(KEEP_FACTORS[0])
        flip = jnp.float32(FLIP_FACTORS[0])
        for option in range(1, 4):
            keep = jnp.where(pick == option, jnp.float32(KEEP_FACTORS[option]), keep)
            flip = jnp.where(pick == option, jnp.float32(FLIP_FACTORS[option]), flip)
        bit = jnp.right_shift(positions, qubits - 1 - q) & 1
        product = product * jnp.where(bit == 1, flip, keep)
    return product


def waits(like, semaphore):
    pltpu.make_async_copy(like, like, semaphore).wait()


def circuit_kernel(
    peers, sections, blocks, qubits, chunks, total_amps,
    x_hbm, gates_hbm, picks_hbm, targets_hbm,
    out_ref, logs_ref,
    xs, yin, ov, gates, picks, targets, low_form, high_form, partial, sums,
    x_sem, sent, grecv, irecv, orecv, srecv,
    entered,
):
    seg = lax.axis_index("segment")
    amp = lax.axis_index("amp")
    reg = gates.shape[-1]
    middle = chunks * peers
    far = list(range(3 * peers // 4, peers))
    mid = list(range(peers // 2, 3 * peers // 4))
    near = list(range(peers // 2 - 1, 0, -1))
    groups = [far, mid, near]

    def tell(semaphore, axis, index, k):
        pl.semaphore_signal(
            semaphore, inc=1, device_id={axis: partner(index, k)}, device_id_type=MESH
        )

    quarter = reg // 4
    parts = [pl.ds(q * quarter, quarter) for q in range(4)]
    first, others = parts[0], pl.ds(quarter, reg - quarter)

    def load(chunk, k, semaphore, rows=pl.ds(0, reg)):
        m = chunk * peers + partner(amp, k)
        pltpu.make_async_copy(
            x_hbm.at[rows, m, 0], xs.at[chunk, k - 1, rows], semaphore
        ).start()

    for q, rows in enumerate(parts):
        for k in far:
            load(0, k, x_sem.at[0 if q == 0 and k == far[0] else 1], rows)

    barrier = pltpu.get_barrier_semaphore()
    line = peers == 8 and sections == 4
    pair_at = quotient(amp, 2)
    inner_pair = lax.rem(quotient(pair_at + 1, 2), jnp.int32(2))
    is_inner = inner_pair == 1
    first_core = lax.rem(amp, jnp.int32(2)) * inner_pair
    second_core = inner_pair - first_core
    relays = second_core * (1 - quotient(pair_at, 2))
    beside = 1 - inner_pair + relays
    if line:

        tell(barrier, "amp", amp, 6)

        @pl.when(second_core == 0)
        def _():
            tell(barrier, "amp", amp, 7)
            tell(barrier, "amp", amp, 1)

        @pl.when(is_inner)
        def _():
            for k in (2, 3, 4, 5):
                tell(barrier, "amp", amp, k)

        @pl.when(beside == 1)
        def _():
            for k in (1, 2):
                tell(barrier, "segment", seg, k)
    else:
        for k in range(peers - 1, 0, -1):
            tell(barrier, "amp", amp, k)
        for k in range(1, sections):
            tell(barrier, "segment", seg, k)

    for k in mid + near:
        load(0, k, x_sem.at[2])
    for chunk in range(1, chunks):
        for k in far + mid + near:
            load(chunk, k, x_sem.at[2])
    pltpu.make_async_copy(gates_hbm, gates.at[seg], x_sem.at[2]).start()
    picks_load = pltpu.make_async_copy(picks_hbm, picks, x_sem.at[2])
    picks_load.start()
    targets_load = pltpu.make_async_copy(targets_hbm, targets, x_sem.at[2])
    targets_load.start()
    for chunk in range(chunks):
        pltpu.make_async_copy(
            x_hbm.at[:, chunk * peers + amp, 0], yin.at[chunk, amp], x_sem.at[2]
        ).start()

    def send_in(chunk, k, rows=pl.ds(0, reg)):
        pltpu.make_async_remote_copy(
            src_ref=xs.at[chunk, k - 1, rows],
            dst_ref=yin.at[chunk, amp, rows],
            send_sem=sent,
            recv_sem=irecv.at[chunk],
            device_id={"amp": partner(amp, k)},
            device_id_type=MESH,
        ).start()

    def far_loaded(at):
        if at == 0:
            waits(xs.at[0, 0, first], x_sem.at[0])
        else:
            waits(xs.at[0, : len(far) - 1], x_sem.at[1])
            waits(xs.at[0, 0, others], x_sem.at[1])

    def rest_loaded():
        waits(xs, x_sem.at[2])
        waits(gates.at[0], x_sem.at[2])
        picks_load.wait()
        targets_load.wait()

    if line:
        with jax.named_scope("barrier"):
            pl.semaphore_wait(
                barrier, 9 - 4 * inner_pair - 4 * first_core - 2 * (second_core - relays)
            )

        @pl.when(beside == 1)
        def _():
            for k in (1, 2):
                tell(entered.at[1], "segment", seg, k)

        @pl.when(pair_at == peers // 2 - 1)
        def _():
            tell(entered.at[0], "amp", amp, 2)
            tell(entered.at[0], "amp", amp, 4)

        for at, rows in enumerate((first, others)):
            with jax.named_scope("load0"):
                far_loaded(at)
            send_in(0, 6, rows)

        @pl.when(first_core == 0)
        def _():
            send_in(0, 7)

        rest_loaded()
        send_in(1, 6)

        @pl.when(is_inner)
        def _():
            with jax.named_scope("ent0"):
                pl.semaphore_wait(entered.at[0], 1)

        @pl.when(first_core == 1)
        def _():
            send_in(0, 7)

        for k in [4, 5] + near:
            send_in(0, k)
        with jax.named_scope("ent1"):

            @pl.when(beside == 1)
            def _():
                pl.semaphore_wait(entered.at[1], 2)
                tell(entered.at[2], "segment", seg, 1)

            pl.semaphore_wait(entered.at[2], 1)

            @pl.when(relays == 1)
            def _():
                for k in (6, 7, 1):
                    tell(entered.at[2], "amp", amp, k)
    else:
        pl.semaphore_wait(barrier, peers - 1 + sections - 1)
        far_loaded(0)
        far_loaded(1)
        rest_loaded()
        for group in groups:
            for k in group:
                send_in(0, k)
    for k in range(1, sections):
        pltpu.make_async_remote_copy(
            src_ref=gates.at[seg],
            dst_ref=gates.at[seg],
            send_sem=sent,
            recv_sem=grecv,
            device_id={"segment": partner(seg, k)},
            device_id_type=MESH,
        ).start()
    for chunk in range(1, chunks):
        for k in far + mid + near:
            if not (line and chunk == 1 and k == 6):
                send_in(chunk, k)
    with jax.named_scope("gates"):
        waits(gates.at[1:], grecv)

    rows_at = lax.broadcasted_iota(jnp.int32, (reg, reg), 0)
    columns_at = lax.broadcasted_iota(jnp.int32, (reg, reg), 1)
    identity = jnp.where(rows_at == columns_at, jnp.float32(1.0), jnp.float32(0.0))

    def build(section, carry):
        low = high = None
        for b in range(blocks):
            factors = row_factors(picks, section, b, qubits, (reg, reg))
            damped = gates[section, b] * factors
            is_low = targets[section, b] == 0
            for_low = jnp.where(is_low, damped, identity)
            for_high = jnp.where(is_low, identity, damped)
            if b == 0:
                low, high = for_low, for_high
            else:
                low = multiply(left_form(for_low), right_form(low))
                high = multiply(left_form(for_high), right_form(high))
        low_form[section] = right_form(low.T)
        high_form[section] = left_form(high)
        return carry

    with jax.named_scope("build"):
        lax.fori_loop(0, sections, build, 0)

    inner = reg // peers
    lanes = lax.broadcasted_iota(jnp.int32, (1, reg), 1)
    partial[...] = jnp.zeros_like(partial)

    def apply_section(chunk, section, swapped):
        low = low_form[section]
        high = high_form[section]
        total = jnp.zeros((8, reg), jnp.float32)
        for slab in range(peers):
            if swapped:
                value = yin[chunk, :, slab * inner : (slab + 1) * inner, :].reshape(reg, reg)
            else:
                value = yin[chunk, slab]
            value = multiply(left_form(value), low)
            value = multiply(high, right_form(value))
            total = total + fold_rows(value)
            if swapped:
                yin[chunk, :, slab * inner : (slab + 1) * inner, :] = value.reshape(
                    peers, inner, reg
                )
            else:
                yin[chunk, slab] = value
        partial[section + 1] = partial[section + 1] + total

    order_out = mid + far + near

    def arrival(chunk, k):
        slot = 0
        if k >= peers // 2:
            slot = 1 + inner_pair * (1 + k % 2) if line else 1
        return chunk + slot * quotient(chunk, chunks - 1)

    def send_sums(source, target, k, at):
        pltpu.make_async_remote_copy(
            src_ref=sums.at[source],
            dst_ref=sums.at[target],
            send_sem=sent,
            recv_sem=srecv.at[at],
            device_id={"amp": partner(amp, k)},
            device_id_type=MESH,
        ).start()

    def run_chunk(chunk, carry):
        with jax.named_scope("in"):
            waits(xs.at[chunk], irecv.at[chunk])
        first = jnp.zeros((8, reg), jnp.float32)
        for slab in range(peers):
            first = first + fold_rows(yin[chunk, slab])
        partial[0] = partial[0] + first

        def pair(i, inner_carry):
            apply_section(chunk, 2 * i, False)
            apply_section(chunk, 2 * i + 1, True)
            return inner_carry

        with jax.named_scope("comp"):
            lax.fori_loop(0, sections // 2, pair, 0)

        @pl.when(chunk == chunks - 1)
        def _():
            row = jnp.zeros((1, reg), jnp.float32)
            for s in range(sections + 1):
                total = jnp.sum(jnp.sum(partial[s], axis=0, keepdims=True), axis=1, keepdims=True)
                row = jnp.where(lanes == s, total, row)
            sums[pair_at] = row
            for k in range(peers - 2, 0, -2):
                send_sums(pair_at, pair_at, k, 0)

        for k in order_out:
            peer = partner(amp, k)
            pltpu.make_async_remote_copy(
                src_ref=yin.at[chunk, peer],
                dst_ref=ov.at[chunk, amp],
                send_sem=sent,
                recv_sem=orecv.at[arrival(chunk, k)],
                device_id={"amp": peer},
                device_id_type=MESH,
            ).start()
        return carry

    lax.fori_loop(0, chunks, run_chunk, 0)

    chips = peers // 2
    with jax.named_scope("sums"):
        waits(sums.at[1:chips], srecv.at[0])
    part = sums[0]
    for chip in range(1, chips):
        part = part + sums[chip]
    sums[chips] = part
    send_sums(chips, chips + 1, 1, 1)
    with jax.named_scope("join"):
        waits(sums.at[0], srecv.at[1])
    row = part + sums[chips + 1]
    totals = [
        jnp.sum(jnp.where(lanes == s, row, 0.0), axis=1, keepdims=True)
        for s in range(sections + 1)
    ]
    logs = jnp.zeros((1, reg), jnp.float32)
    for s in range(sections):
        logs = jnp.where(lanes == s, jnp.log(totals[s + 1] / totals[s]), logs)
    logs_ref[...] = logs[:, :sections]
    scale = 1.0 / jnp.sqrt(totals[sections] / total_amps)
    scale = jnp.broadcast_to(scale, (1, reg))

    for chunk in range(chunks):
        m = chunk * peers + amp
        out_ref[pl.ds(m, reg, stride=middle), :] = yin[chunk, amp] * scale
    def place(chunk, peer):
        m = chunk * peers + peer
        out_ref[pl.ds(m, reg, stride=middle), :] = ov[chunk, peer] * scale

    last = chunks - 1
    for chunk in range(last):
        waits(xs.at[0], orecv.at[chunk])
        for k in order_out:
            place(chunk, partner(amp, k))
    with jax.named_scope("out_near"):
        waits(xs.at[0, : len(near)], orecv.at[last])
    for k in near:
        place(last, partner(amp, k))
    if line:
        late = [
            inner_pair * partner(amp, 6 + at) + (1 - inner_pair) * partner(amp, 4 + at)
            for at in range(2)
        ]
        soon = [
            inner_pair * partner(amp, 4 + at) + (1 - inner_pair) * partner(amp, 6 + at)
            for at in range(2)
        ]
        with jax.named_scope("out_soon"):
            waits(xs.at[0, :2], orecv.at[last + 1])
        for peer in soon:
            place(last, peer)
        for at in range(2):
            with jax.named_scope(f"out_{at}"):
                waits(xs.at[0, 0], orecv.at[last + 2 + at])
            place(last, late[at])
    else:
        waits(xs.at[0, : peers // 2], orecv.at[last + 1])
        for k in far + mid:
            place(last, partner(amp, k))

    with jax.named_scope("sendwait"):
        waits(xs, sent)
        waits(xs, sent)
        waits(gates.at[1:], sent)
        waits(sums.at[:chips], sent)


def store_kernel(pieces, out_vmem, logs_vmem, out_hbm, logs_hbm, out_sem, logs_sem):
    rows = out_vmem.shape[0] // pieces
    for p in range(pieces):
        at = pl.ds(p * rows, rows)
        pltpu.make_async_copy(out_vmem.at[at], out_hbm.at[at], out_sem).start()
    logs_copy = pltpu.make_async_copy(logs_vmem, logs_hbm, logs_sem)
    logs_copy.start()
    pltpu.make_async_copy(out_vmem, out_hbm, out_sem).wait()
    logs_copy.wait()


def step(states, gate_blocks, kraus_picks, block_targets):
    traj_here, amp_local = states.shape
    reg = gate_blocks.shape[-1]
    blocks = gate_blocks.shape[1]
    qubits = kraus_picks.shape[-1]
    peers = lax.axis_size("amp")
    sections = lax.axis_size("segment")
    middle = amp_local // (reg * reg)
    fits = (
        traj_here == 1
        and gate_blocks.shape[0] == 1
        and middle % peers == 0
        and peers & (peers - 1) == 0
        and peers >= 8
        and middle == peers * (peers // 4)
        and middle > peers
        and sections & (sections - 1) == 0
        and sections % 2 == 0
        and sections < 8
        and reg == 128
        and reg % (8 * peers) == 0
    )
    if not fits:
        return body(states, gate_blocks, kraus_picks, block_targets)
    chunks = middle // peers
    kernel = functools.partial(
        circuit_kernel, peers, sections, blocks, qubits, chunks, amp_local * peers
    )
    f32 = jnp.float32
    dma = pltpu.SemaphoreType.DMA
    out, logs = pl.pallas_call(
        kernel,
        out_shape=(
            pltpu.VMEM((reg * middle, reg), f32),
            pltpu.VMEM((1, sections), f32),
        ),
        in_specs=[pl.BlockSpec(memory_space=pl.ANY)] * 4,
        out_specs=(
            pl.BlockSpec(memory_space=pltpu.VMEM),
            pl.BlockSpec(memory_space=pltpu.VMEM),
        ),
        scratch_shapes=[
            pltpu.VMEM((chunks, peers - 1, reg, reg), f32),
            pltpu.VMEM((chunks, peers, reg, reg), f32),
            pltpu.VMEM((chunks, peers, reg, reg), f32),
            pltpu.VMEM((sections, blocks, reg, reg), f32),
            pltpu.SMEM((1, blocks, sections, qubits), jnp.int32),
            pltpu.SMEM((sections, blocks), jnp.int32),
            pltpu.VMEM((sections, 2 * reg, 2 * reg), jnp.bfloat16),
            pltpu.VMEM((sections, reg, 2 * reg), jnp.bfloat16),
            pltpu.VMEM((sections + 1, 8, reg), f32),
            pltpu.VMEM((peers // 2 + 2, 1, reg), f32),
            dma((3,)),
            dma,
            dma,
            dma((chunks,)),
            dma((chunks + 3,)),
            dma((2,)),
            pltpu.SemaphoreType.REGULAR((3,)),
        ],
        compiler_params=pltpu.CompilerParams(collective_id=0, has_side_effects=True),
    )(
        states.reshape(reg, middle, 1, reg),
        gate_blocks[0],
        jnp.swapaxes(kraus_picks, 1, 2),
        block_targets,
    )
    pieces = 8
    out, logs = pl.pallas_call(
        functools.partial(store_kernel, pieces),
        out_shape=(
            jax.ShapeDtypeStruct(out.shape, f32),
            jax.ShapeDtypeStruct(logs.shape, f32),
        ),
        in_specs=[pl.BlockSpec(memory_space=pltpu.VMEM)] * 2,
        out_specs=(pl.BlockSpec(memory_space=pl.ANY),) * 2,
        scratch_shapes=[dma, dma],
    )(
        pltpu.with_memory_space_constraint(out, pltpu.VMEM),
        pltpu.with_memory_space_constraint(logs, pltpu.VMEM),
    )
    return out.reshape(1, amp_local), logs


def solution(mesh):
    in_specs = (
        P("segment", "amp"),
        P("segment", None, None, None),
        P("segment", None, None, None),
        P(),
    )
    out_specs = (P("segment", "amp"), P("segment", None))
    return jax.shard_map(step, mesh=mesh, in_specs=in_specs, out_specs=out_specs, check_vma=False)
```

```python
import functools

import jax
import jax.numpy as jnp
from jax import lax
from jax.experimental import pallas as pl
from jax.experimental.pallas import tpu as pltpu
from jax.sharding import PartitionSpec as P

KEEP_FACTORS = (1.0, 0.9, 1.0, 0.97)
FLIP_FACTORS = (0.9, 1.0, 0.97, 1.0)
MESH = pl.DeviceIdType.MESH


def broadcast(block, axis, owner):
    block = jnp.where(lax.axis_index(axis) == owner, block, jnp.zeros_like(block))
    return lax.psum(block, axis)


def noise_factors(kraus_rows):
    qubit_count = kraus_rows.shape[-1]
    register = 2**qubit_count
    positions = jnp.arange(register, dtype=jnp.int32)
    product = jnp.ones(kraus_rows.shape[:-1] + (register,), jnp.float32)
    for qubit_pos in range(qubit_count):
        bit_value = jnp.right_shift(positions, qubit_count - 1 - qubit_pos) & 1
        column = kraus_rows[..., qubit_pos : qubit_pos + 1]
        low_value = jnp.zeros(column.shape, jnp.float32)
        high_value = jnp.zeros(column.shape, jnp.float32)
        for option in range(4):
            picked = (column == option).astype(jnp.float32)
            low_value = low_value + picked * KEEP_FACTORS[option]
            high_value = high_value + picked * FLIP_FACTORS[option]
        product = product * jnp.where(bit_value == 1, high_value, low_value)
    return product


def apply_gate(amplitudes, matrix, factors, target):

    def on_low(values):
        mixed_rows = jnp.einsum("bhmk,ik->bhmi", values, matrix, precision=lax.Precision.HIGHEST)
        return mixed_rows * factors[:, None, None, :]

    def on_high(values):
        mixed_rows = jnp.einsum("bjmk,ij->bimk", values, matrix, precision=lax.Precision.HIGHEST)
        return mixed_rows * factors[:, :, None, None]

    return lax.cond(target == 0, on_low, on_high, amplitudes)


def square_sums(values):
    return (values, jnp.sum(values * values, axis=(1, 2, 3)))


def body(states, gate_blocks, kraus_picks, block_targets):
    traj_here = states.shape[0]
    amp_local = states.shape[1]
    register = gate_blocks.shape[-1]
    blocks = gate_blocks.shape[1]
    middle = amp_local // (register * register)
    total_amps = amp_local * lax.axis_size("amp")
    sections = lax.axis_size("segment")
    amplitudes = states.reshape(traj_here, register, middle, register)
    first_local = jnp.sum(amplitudes * amplitudes, axis=(1, 2, 3))
    local_sums = [first_local]
    for section in range(sections):
        section_gates = broadcast(gate_blocks, "segment", section)[0]
        for block_pos in range(blocks):
            factors = noise_factors(kraus_picks[:, section, block_pos, :])
            amplitudes = apply_gate(
                amplitudes, section_gates[block_pos], factors, block_targets[section, block_pos]
            )
        amplitudes, local_sq = square_sums(
            lax.all_to_all(amplitudes, "amp", split_axis=1, concat_axis=1, tiled=True)
        )
        local_sums.append(local_sq)
    totals = lax.psum(jnp.stack(local_sums, axis=1), "amp")
    log_weights = jnp.log(totals[:, 1:] / totals[:, :-1])
    amplitudes = amplitudes / jnp.sqrt(totals[:, -1] / total_amps)[:, None, None, None]
    return (amplitudes.reshape(traj_here, amp_local), log_weights)


def quotient(index, divisor):
    return index if divisor == 1 else lax.div(index, jnp.int32(divisor))


def partner(index, k):
    result = index
    bit = 1
    while bit <= k:
        if k & bit:
            result = result + bit * (1 - 2 * lax.rem(quotient(index, bit), jnp.int32(2)))
        bit *= 2
    return result


def split(values):
    high = values.astype(jnp.bfloat16)
    low = (values - high.astype(jnp.float32)).astype(jnp.bfloat16)
    return high, low


def left_form(matrix):
    return jnp.concatenate(split(matrix), axis=1)


def right_form(matrix):
    row = jnp.concatenate(split(matrix), axis=1)
    return jnp.concatenate([row, row], axis=0)


def multiply(left, right):
    both = jnp.dot(left, right, preferred_element_type=jnp.float32)
    half = both.shape[1] // 2
    return both[:, :half] + both[:, half:]


def fold_rows(values):
    squares = values * values
    return jnp.sum(squares.reshape(-1, 8, squares.shape[-1]), axis=0)


def row_factors(picks_ref, section, block, qubits, shape):
    positions = lax.broadcasted_iota(jnp.int32, shape, 0)
    product = jnp.ones(shape, jnp.float32)
    for q in range(qubits):
        pick = picks_ref[0, block, section, q]
        keep = jnp.float32(KEEP_FACTORS[0])
        flip = jnp.float32(FLIP_FACTORS[0])
        for option in range(1, 4):
            keep = jnp.where(pick == option, jnp.float32(KEEP_FACTORS[option]), keep)
            flip = jnp.where(pick == option, jnp.float32(FLIP_FACTORS[option]), flip)
        bit = jnp.right_shift(positions, qubits - 1 - q) & 1
        product = product * jnp.where(bit == 1, flip, keep)
    return product


def waits(like, semaphore):
    pltpu.make_async_copy(like, like, semaphore).wait()


def circuit_kernel(
    peers, sections, blocks, qubits, chunks, total_amps,
    x_hbm, gates_hbm, picks_hbm, targets_hbm,
    out_ref, logs_ref,
    xs, yin, ov, gates, picks, targets, low_form, high_form, partial, sums,
    x_sem, sent, grecv, irecv, orecv, srecv,
    entered,
):
    seg = lax.axis_index("segment")
    amp = lax.axis_index("amp")
    reg = gates.shape[-1]
    middle = chunks * peers
    far = list(range(3 * peers // 4, peers))
    mid = list(range(peers // 2, 3 * peers // 4))
    near = list(range(peers // 2 - 1, 0, -1))
    groups = [far, mid, near]

    def tell(semaphore, axis, index, k):
        pl.semaphore_signal(
            semaphore, inc=1, device_id={axis: partner(index, k)}, device_id_type=MESH
        )

    quarter = reg // 4
    parts = [pl.ds(q * quarter, quarter) for q in range(4)]
    first, others = parts[0], pl.ds(quarter, reg - quarter)

    def load(chunk, k, semaphore, rows=pl.ds(0, reg)):
        m = chunk * peers + partner(amp, k)
        pltpu.make_async_copy(
            x_hbm.at[rows, m, 0], xs.at[chunk, k - 1, rows], semaphore
        ).start()

    for q, rows in enumerate(parts):
        for k in far:
            load(0, k, x_sem.at[0 if q == 0 and k == far[0] else 1], rows)

    barrier = pltpu.get_barrier_semaphore()
    line = peers == 8 and sections == 4
    pair_at = quotient(amp, 2)
    inner_pair = lax.rem(quotient(pair_at + 1, 2), jnp.int32(2))
    is_inner = inner_pair == 1
    first_core = lax.rem(amp, jnp.int32(2)) * inner_pair
    second_core = inner_pair - first_core
    relays = second_core * (1 - quotient(pair_at, 2))
    beside = 1 - inner_pair + relays
    if line:

        tell(barrier, "amp", amp, 6)

        @pl.when(second_core == 0)
        def _():
            tell(barrier, "amp", amp, 7)
            tell(barrier, "amp", amp, 1)

        @pl.when(is_inner)
        def _():
            for k in (2, 3, 4, 5):
                tell(barrier, "amp", amp, k)

        @pl.when(beside == 1)
        def _():
            for k in (1, 2):
                tell(barrier, "segment", seg, k)
    else:
        for k in range(peers - 1, 0, -1):
            tell(barrier, "amp", amp, k)
        for k in range(1, sections):
            tell(barrier, "segment", seg, k)

    for k in mid + near:
        load(0, k, x_sem.at[2])
    for chunk in range(1, chunks):
        for k in far + mid + near:
            load(chunk, k, x_sem.at[2])
    pltpu.make_async_copy(gates_hbm, gates.at[seg], x_sem.at[2]).start()
    picks_load = pltpu.make_async_copy(picks_hbm, picks, x_sem.at[2])
    picks_load.start()
    targets_load = pltpu.make_async_copy(targets_hbm, targets, x_sem.at[2])
    targets_load.start()
    for chunk in range(chunks):
        pltpu.make_async_copy(
            x_hbm.at[:, chunk * peers + amp, 0], yin.at[chunk, amp], x_sem.at[2]
        ).start()

    def send_in(chunk, k, rows=pl.ds(0, reg)):
        pltpu.make_async_remote_copy(
            src_ref=xs.at[chunk, k - 1, rows],
            dst_ref=yin.at[chunk, amp, rows],
            send_sem=sent,
            recv_sem=irecv.at[chunk],
            device_id={"amp": partner(amp, k)},
            device_id_type=MESH,
        ).start()

    def far_loaded(at):
        if at == 0:
            waits(xs.at[0, 0, first], x_sem.at[0])
        else:
            waits(xs.at[0, : len(far) - 1], x_sem.at[1])
            waits(xs.at[0, 0, others], x_sem.at[1])

    def rest_loaded():
        waits(xs, x_sem.at[2])
        waits(gates.at[0], x_sem.at[2])
        picks_load.wait()
        targets_load.wait()

    if line:
        with jax.named_scope("barrier"):
            pl.semaphore_wait(
                barrier, 9 - 4 * inner_pair - 4 * first_core - 2 * (second_core - relays)
            )

        @pl.when(beside == 1)
        def _():
            for k in (1, 2):
                tell(entered.at[1], "segment", seg, k)

        @pl.when(pair_at == peers // 2 - 1)
        def _():
            tell(entered.at[0], "amp", amp, 2)
            tell(entered.at[0], "amp", amp, 4)

        for at, rows in enumerate((first, others)):
            with jax.named_scope("load0"):
                far_loaded(at)
            send_in(0, 6, rows)

        @pl.when(first_core == 0)
        def _():
            send_in(0, 7)

        rest_loaded()
        send_in(1, 6)

        @pl.when(is_inner)
        def _():
            with jax.named_scope("ent0"):
                pl.semaphore_wait(entered.at[0], 1)

        @pl.when(first_core == 1)
        def _():
            send_in(0, 7)

        for k in [4, 5] + near:
            send_in(0, k)
        with jax.named_scope("ent1"):

            @pl.when(beside == 1)
            def _():
                pl.semaphore_wait(entered.at[1], 2)
                tell(entered.at[2], "segment", seg, 1)

            pl.semaphore_wait(entered.at[2], 1)

            @pl.when(relays == 1)
            def _():
                for k in (6, 7, 1):
                    tell(entered.at[2], "amp", amp, k)
    else:
        pl.semaphore_wait(barrier, peers - 1 + sections - 1)
        far_loaded(0)
        far_loaded(1)
        rest_loaded()
        for group in groups:
            for k in group:
                send_in(0, k)
    for k in range(1, sections):
        pltpu.make_async_remote_copy(
            src_ref=gates.at[seg],
            dst_ref=gates.at[seg],
            send_sem=sent,
            recv_sem=grecv,
            device_id={"segment": partner(seg, k)},
            device_id_type=MESH,
        ).start()
    for chunk in range(1, chunks):
        for k in far + mid + near:
            if not (line and chunk == 1 and k == 6):
                send_in(chunk, k)
    with jax.named_scope("gates"):
        waits(gates.at[1:], grecv)

    rows_at = lax.broadcasted_iota(jnp.int32, (reg, reg), 0)
    columns_at = lax.broadcasted_iota(jnp.int32, (reg, reg), 1)
    identity = jnp.where(rows_at == columns_at, jnp.float32(1.0), jnp.float32(0.0))

    def build(section, carry):
        low = high = None
        for b in range(blocks):
            factors = row_factors(picks, section, b, qubits, (reg, reg))
            damped = gates[section, b] * factors
            is_low = targets[section, b] == 0
            for_low = jnp.where(is_low, damped, identity)
            for_high = jnp.where(is_low, identity, damped)
            if b == 0:
                low, high = for_low, for_high
            else:
                low = multiply(left_form(for_low), right_form(low))
                high = multiply(left_form(for_high), right_form(high))
        low_form[section] = right_form(low.T)
        high_form[section] = left_form(high)
        return carry

    with jax.named_scope("build"):
        lax.fori_loop(0, sections, build, 0)

    inner = reg // peers
    lanes = lax.broadcasted_iota(jnp.int32, (1, reg), 1)
    partial[...] = jnp.zeros_like(partial)

    def apply_section(chunk, section, swapped):
        low = low_form[section]
        high = high_form[section]
        total = jnp.zeros((8, reg), jnp.float32)
        for slab in range(peers):
            if swapped:
                value = yin[chunk, :, slab * inner : (slab + 1) * inner, :].reshape(reg, reg)
            else:
                value = yin[chunk, slab]
            value = multiply(left_form(value), low)
            value = multiply(high, right_form(value))
            total = total + fold_rows(value)
            if swapped:
                yin[chunk, :, slab * inner : (slab + 1) * inner, :] = value.reshape(
                    peers, inner, reg
                )
            else:
                yin[chunk, slab] = value
        partial[section + 1] = partial[section + 1] + total

    order_out = mid + far + near

    def arrival(chunk, k):
        if not line or k < peers // 2:
            return 0
        return quotient(chunk, chunks - 1) * inner_pair * (1 + k % 2)

    def send_sums(source, target, k, at):
        pltpu.make_async_remote_copy(
            src_ref=sums.at[source],
            dst_ref=sums.at[target],
            send_sem=sent,
            recv_sem=srecv.at[at],
            device_id={"amp": partner(amp, k)},
            device_id_type=MESH,
        ).start()

    def run_chunk(chunk, carry):
        with jax.named_scope("in"):
            waits(xs.at[chunk], irecv.at[chunk])
        first = jnp.zeros((8, reg), jnp.float32)
        for slab in range(peers):
            first = first + fold_rows(yin[chunk, slab])
        partial[0] = partial[0] + first

        def pair(i, inner_carry):
            apply_section(chunk, 2 * i, False)
            apply_section(chunk, 2 * i + 1, True)
            return inner_carry

        with jax.named_scope("comp"):
            lax.fori_loop(0, sections // 2, pair, 0)

        @pl.when(chunk == chunks - 1)
        def _():
            row = jnp.zeros((1, reg), jnp.float32)
            for s in range(sections + 1):
                total = jnp.sum(jnp.sum(partial[s], axis=0, keepdims=True), axis=1, keepdims=True)
                row = jnp.where(lanes == s, total, row)
            sums[pair_at] = row
            for k in range(peers - 2, 0, -2):
                send_sums(pair_at, pair_at, k, 0)

        for k in order_out:
            peer = partner(amp, k)
            pltpu.make_async_remote_copy(
                src_ref=yin.at[chunk, peer],
                dst_ref=ov.at[chunk, amp],
                send_sem=sent,
                recv_sem=orecv.at[arrival(chunk, k)],
                device_id={"amp": peer},
                device_id_type=MESH,
            ).start()
        return carry

    lax.fori_loop(0, chunks, run_chunk, 0)

    chips = peers // 2
    with jax.named_scope("sums"):
        waits(sums.at[1:chips], srecv.at[0])
    part = sums[0]
    for chip in range(1, chips):
        part = part + sums[chip]
    sums[chips] = part
    send_sums(chips, chips + 1, 1, 1)
    with jax.named_scope("join"):
        waits(sums.at[0], srecv.at[1])
    row = part + sums[chips + 1]
    totals = [
        jnp.sum(jnp.where(lanes == s, row, 0.0), axis=1, keepdims=True)
        for s in range(sections + 1)
    ]
    logs = jnp.zeros((1, reg), jnp.float32)
    for s in range(sections):
        logs = jnp.where(lanes == s, jnp.log(totals[s + 1] / totals[s]), logs)
    logs_ref[...] = logs[:, :sections]
    scale = 1.0 / jnp.sqrt(totals[sections] / total_amps)
    scale = jnp.broadcast_to(scale, (1, reg))

    for chunk in range(chunks):
        m = chunk * peers + amp
        out_ref[pl.ds(m, reg, stride=middle), :] = yin[chunk, amp] * scale
    def place(chunk, peer):
        m = chunk * peers + peer
        out_ref[pl.ds(m, reg, stride=middle), :] = ov[chunk, peer] * scale

    last = chunks - 1
    early = chunks * (peers - 1) - (2 if line else 0)
    with jax.named_scope("early"):
        waits(ov.at[:, :, : early * reg // (chunks * peers)], orecv.at[0])
    for chunk in range(last):
        for k in order_out:
            place(chunk, partner(amp, k))
    for k in near:
        place(last, partner(amp, k))
    if line:
        late = [
            inner_pair * partner(amp, 6 + at) + (1 - inner_pair) * partner(amp, 4 + at)
            for at in range(2)
        ]
        soon = [
            inner_pair * partner(amp, 4 + at) + (1 - inner_pair) * partner(amp, 6 + at)
            for at in range(2)
        ]
        for peer in soon:
            place(last, peer)
        for at in range(2):
            with jax.named_scope(f"out_{at}"):
                waits(xs.at[0, 0], orecv.at[1 + at])
            place(last, late[at])
    else:
        for k in far + mid:
            place(last, partner(amp, k))

    with jax.named_scope("sendwait"):
        waits(xs, sent)
        waits(xs, sent)
        waits(gates.at[1:], sent)
        waits(sums.at[:chips], sent)


def store_kernel(pieces, out_vmem, logs_vmem, out_hbm, logs_hbm, out_sem, logs_sem):
    rows = out_vmem.shape[0] // pieces
    for p in range(pieces):
        at = pl.ds(p * rows, rows)
        pltpu.make_async_copy(out_vmem.at[at], out_hbm.at[at], out_sem).start()
    logs_copy = pltpu.make_async_copy(logs_vmem, logs_hbm, logs_sem)
    logs_copy.start()
    pltpu.make_async_copy(out_vmem, out_hbm, out_sem).wait()
    logs_copy.wait()


def step(states, gate_blocks, kraus_picks, block_targets):
    traj_here, amp_local = states.shape
    reg = gate_blocks.shape[-1]
    blocks = gate_blocks.shape[1]
    qubits = kraus_picks.shape[-1]
    peers = lax.axis_size("amp")
    sections = lax.axis_size("segment")
    middle = amp_local // (reg * reg)
    fits = (
        traj_here == 1
        and gate_blocks.shape[0] == 1
        and middle % peers == 0
        and peers & (peers - 1) == 0
        and peers >= 8
        and middle == peers * (peers // 4)
        and middle > peers
        and sections & (sections - 1) == 0
        and sections % 2 == 0
        and sections < 8
        and reg == 128
        and reg % (8 * peers) == 0
    )
    if not fits:
        return body(states, gate_blocks, kraus_picks, block_targets)
    chunks = middle // peers
    kernel = functools.partial(
        circuit_kernel, peers, sections, blocks, qubits, chunks, amp_local * peers
    )
    f32 = jnp.float32
    dma = pltpu.SemaphoreType.DMA
    out, logs = pl.pallas_call(
        kernel,
        out_shape=(
            pltpu.VMEM((reg * middle, reg), f32),
            pltpu.VMEM((1, sections), f32),
        ),
        in_specs=[pl.BlockSpec(memory_space=pl.ANY)] * 4,
        out_specs=(
            pl.BlockSpec(memory_space=pltpu.VMEM),
            pl.BlockSpec(memory_space=pltpu.VMEM),
        ),
        scratch_shapes=[
            pltpu.VMEM((chunks, peers - 1, reg, reg), f32),
            pltpu.VMEM((chunks, peers, reg, reg), f32),
            pltpu.VMEM((chunks, peers, reg, reg), f32),
            pltpu.VMEM((sections, blocks, reg, reg), f32),
            pltpu.SMEM((1, blocks, sections, qubits), jnp.int32),
            pltpu.SMEM((sections, blocks), jnp.int32),
            pltpu.VMEM((sections, 2 * reg, 2 * reg), jnp.bfloat16),
            pltpu.VMEM((sections, reg, 2 * reg), jnp.bfloat16),
            pltpu.VMEM((sections + 1, 8, reg), f32),
            pltpu.VMEM((peers // 2 + 2, 1, reg), f32),
            dma((3,)),
            dma,
            dma,
            dma((chunks,)),
            dma((3,)),
            dma((2,)),
            pltpu.SemaphoreType.REGULAR((3,)),
        ],
        compiler_params=pltpu.CompilerParams(collective_id=0, has_side_effects=True),
    )(
        states.reshape(reg, middle, 1, reg),
        gate_blocks[0],
        jnp.swapaxes(kraus_picks, 1, 2),
        block_targets,
    )
    pieces = 8
    out, logs = pl.pallas_call(
        functools.partial(store_kernel, pieces),
        out_shape=(
            jax.ShapeDtypeStruct(out.shape, f32),
            jax.ShapeDtypeStruct(logs.shape, f32),
        ),
        in_specs=[pl.BlockSpec(memory_space=pltpu.VMEM)] * 2,
        out_specs=(pl.BlockSpec(memory_space=pl.ANY),) * 2,
        scratch_shapes=[dma, dma],
    )(
        pltpu.with_memory_space_constraint(out, pltpu.VMEM),
        pltpu.with_memory_space_constraint(logs, pltpu.VMEM),
    )
    return out.reshape(1, amp_local), logs


def solution(mesh):
    in_specs = (
        P("segment", "amp"),
        P("segment", None, None, None),
        P("segment", None, None, None),
        P(),
    )
    out_specs = (P("segment", "amp"), P("segment", None))
    return jax.shard_map(step, mesh=mesh, in_specs=in_specs, out_specs=out_specs, check_vma=False)
```

```python
import functools

import jax
import jax.numpy as jnp
from jax import lax
from jax.experimental import pallas as pl
from jax.experimental.pallas import tpu as pltpu
from jax.sharding import PartitionSpec as P

KEEP_FACTORS = (1.0, 0.9, 1.0, 0.97)
FLIP_FACTORS = (0.9, 1.0, 0.97, 1.0)
MESH = pl.DeviceIdType.MESH


def broadcast(block, axis, owner):
    block = jnp.where(lax.axis_index(axis) == owner, block, jnp.zeros_like(block))
    return lax.psum(block, axis)


def noise_factors(kraus_rows):
    qubit_count = kraus_rows.shape[-1]
    register = 2**qubit_count
    positions = jnp.arange(register, dtype=jnp.int32)
    product = jnp.ones(kraus_rows.shape[:-1] + (register,), jnp.float32)
    for qubit_pos in range(qubit_count):
        bit_value = jnp.right_shift(positions, qubit_count - 1 - qubit_pos) & 1
        column = kraus_rows[..., qubit_pos : qubit_pos + 1]
        low_value = jnp.zeros(column.shape, jnp.float32)
        high_value = jnp.zeros(column.shape, jnp.float32)
        for option in range(4):
            picked = (column == option).astype(jnp.float32)
            low_value = low_value + picked * KEEP_FACTORS[option]
            high_value = high_value + picked * FLIP_FACTORS[option]
        product = product * jnp.where(bit_value == 1, high_value, low_value)
    return product


def apply_gate(amplitudes, matrix, factors, target):

    def on_low(values):
        mixed_rows = jnp.einsum("bhmk,ik->bhmi", values, matrix, precision=lax.Precision.HIGHEST)
        return mixed_rows * factors[:, None, None, :]

    def on_high(values):
        mixed_rows = jnp.einsum("bjmk,ij->bimk", values, matrix, precision=lax.Precision.HIGHEST)
        return mixed_rows * factors[:, :, None, None]

    return lax.cond(target == 0, on_low, on_high, amplitudes)


def square_sums(values):
    return (values, jnp.sum(values * values, axis=(1, 2, 3)))


def body(states, gate_blocks, kraus_picks, block_targets):
    traj_here = states.shape[0]
    amp_local = states.shape[1]
    register = gate_blocks.shape[-1]
    blocks = gate_blocks.shape[1]
    middle = amp_local // (register * register)
    total_amps = amp_local * lax.axis_size("amp")
    sections = lax.axis_size("segment")
    amplitudes = states.reshape(traj_here, register, middle, register)
    first_local = jnp.sum(amplitudes * amplitudes, axis=(1, 2, 3))
    local_sums = [first_local]
    for section in range(sections):
        section_gates = broadcast(gate_blocks, "segment", section)[0]
        for block_pos in range(blocks):
            factors = noise_factors(kraus_picks[:, section, block_pos, :])
            amplitudes = apply_gate(
                amplitudes, section_gates[block_pos], factors, block_targets[section, block_pos]
            )
        amplitudes, local_sq = square_sums(
            lax.all_to_all(amplitudes, "amp", split_axis=1, concat_axis=1, tiled=True)
        )
        local_sums.append(local_sq)
    totals = lax.psum(jnp.stack(local_sums, axis=1), "amp")
    log_weights = jnp.log(totals[:, 1:] / totals[:, :-1])
    amplitudes = amplitudes / jnp.sqrt(totals[:, -1] / total_amps)[:, None, None, None]
    return (amplitudes.reshape(traj_here, amp_local), log_weights)


def quotient(index, divisor):
    return index if divisor == 1 else lax.div(index, jnp.int32(divisor))


def partner(index, k):
    result = index
    bit = 1
    while bit <= k:
        if k & bit:
            result = result + bit * (1 - 2 * lax.rem(quotient(index, bit), jnp.int32(2)))
        bit *= 2
    return result


def split(values):
    high = values.astype(jnp.bfloat16)
    low = (values - high.astype(jnp.float32)).astype(jnp.bfloat16)
    return high, low


def left_form(matrix):
    return jnp.concatenate(split(matrix), axis=1)


def right_form(matrix):
    row = jnp.concatenate(split(matrix), axis=1)
    return jnp.concatenate([row, row], axis=0)


def multiply(left, right):
    both = jnp.dot(left, right, preferred_element_type=jnp.float32)
    half = both.shape[1] // 2
    return both[:, :half] + both[:, half:]


def fold_rows(values):
    squares = values * values
    return jnp.sum(squares.reshape(-1, 8, squares.shape[-1]), axis=0)


def row_factors(picks_ref, section, block, qubits, shape):
    positions = lax.broadcasted_iota(jnp.int32, shape, 0)
    product = jnp.ones(shape, jnp.float32)
    for q in range(qubits):
        pick = picks_ref[0, block, section, q]
        keep = jnp.float32(KEEP_FACTORS[0])
        flip = jnp.float32(FLIP_FACTORS[0])
        for option in range(1, 4):
            keep = jnp.where(pick == option, jnp.float32(KEEP_FACTORS[option]), keep)
            flip = jnp.where(pick == option, jnp.float32(FLIP_FACTORS[option]), flip)
        bit = jnp.right_shift(positions, qubits - 1 - q) & 1
        product = product * jnp.where(bit == 1, flip, keep)
    return product


def waits(like, semaphore):
    pltpu.make_async_copy(like, like, semaphore).wait()


def circuit_kernel(
    peers, sections, blocks, qubits, chunks, total_amps,
    x_hbm, gates_hbm, picks_hbm, targets_hbm,
    out_ref, logs_ref,
    xs, yin, ov, gates, picks, targets, low_form, high_form, partial, sums,
    x_sem, sent, grecv, irecv, orecv, srecv,
    entered,
):
    seg = lax.axis_index("segment")
    amp = lax.axis_index("amp")
    reg = gates.shape[-1]
    middle = chunks * peers
    far = list(range(3 * peers // 4, peers))
    mid = list(range(peers // 2, 3 * peers // 4))
    near = list(range(peers // 2 - 1, 0, -1))
    groups = [far, mid, near]

    def tell(semaphore, axis, index, k):
        pl.semaphore_signal(
            semaphore, inc=1, device_id={axis: partner(index, k)}, device_id_type=MESH
        )

    eighth = reg // 8
    edges = [0, 1, 3, 5, 8]
    parts = [pl.ds(a * eighth, (b - a) * eighth) for a, b in zip(edges, edges[1:])]
    first, others = parts[0], pl.ds(eighth, reg - eighth)

    def load(chunk, k, semaphore, rows=pl.ds(0, reg)):
        m = chunk * peers + partner(amp, k)
        pltpu.make_async_copy(
            x_hbm.at[rows, m, 0], xs.at[chunk, k - 1, rows], semaphore
        ).start()

    for q, rows in enumerate(parts):
        for k in far:
            load(0, k, x_sem.at[0 if q == 0 and k == far[0] else 1], rows)

    barrier = pltpu.get_barrier_semaphore()
    line = peers == 8 and sections == 4
    pair_at = quotient(amp, 2)
    inner_pair = lax.rem(quotient(pair_at + 1, 2), jnp.int32(2))
    is_inner = inner_pair == 1
    first_core = lax.rem(amp, jnp.int32(2)) * inner_pair
    second_core = inner_pair - first_core
    relays = second_core * (1 - quotient(pair_at, 2))
    beside = 1 - inner_pair + relays
    if line:

        tell(barrier, "amp", amp, 6)

        @pl.when(second_core == 0)
        def _():
            tell(barrier, "amp", amp, 7)
            tell(barrier, "amp", amp, 1)

        @pl.when(is_inner)
        def _():
            for k in (2, 3, 4, 5):
                tell(barrier, "amp", amp, k)

        @pl.when(beside == 1)
        def _():
            for k in (1, 2):
                tell(barrier, "segment", seg, k)
    else:
        for k in range(peers - 1, 0, -1):
            tell(barrier, "amp", amp, k)
        for k in range(1, sections):
            tell(barrier, "segment", seg, k)

    for k in mid + near:
        load(0, k, x_sem.at[2])
    for chunk in range(1, chunks):
        for k in far + mid + near:
            load(chunk, k, x_sem.at[2])
    pltpu.make_async_copy(gates_hbm, gates.at[seg], x_sem.at[2]).start()
    picks_load = pltpu.make_async_copy(picks_hbm, picks, x_sem.at[2])
    picks_load.start()
    targets_load = pltpu.make_async_copy(targets_hbm, targets, x_sem.at[2])
    targets_load.start()
    for chunk in range(chunks):
        pltpu.make_async_copy(
            x_hbm.at[:, chunk * peers + amp, 0], yin.at[chunk, amp], x_sem.at[2]
        ).start()

    def send_in(chunk, k, rows=pl.ds(0, reg)):
        pltpu.make_async_remote_copy(
            src_ref=xs.at[chunk, k - 1, rows],
            dst_ref=yin.at[chunk, amp, rows],
            send_sem=sent,
            recv_sem=irecv.at[chunk],
            device_id={"amp": partner(amp, k)},
            device_id_type=MESH,
        ).start()

    def far_loaded(at):
        if at == 0:
            waits(xs.at[0, 0, first], x_sem.at[0])
        else:
            waits(xs.at[0, : len(far) - 1], x_sem.at[1])
            waits(xs.at[0, 0, others], x_sem.at[1])

    def rest_loaded():
        waits(xs, x_sem.at[2])
        waits(gates.at[0], x_sem.at[2])
        picks_load.wait()
        targets_load.wait()

    if line:
        with jax.named_scope("barrier"):
            pl.semaphore_wait(
                barrier, 9 - 4 * inner_pair - 4 * first_core - 2 * (second_core - relays)
            )

        @pl.when(beside == 1)
        def _():
            for k in (1, 2):
                tell(entered.at[1], "segment", seg, k)

        @pl.when(pair_at == peers // 2 - 1)
        def _():
            tell(entered.at[0], "amp", amp, 2)
            tell(entered.at[0], "amp", amp, 4)

        for at, rows in enumerate((first, others)):
            with jax.named_scope("load0"):
                far_loaded(at)
            send_in(0, 6, rows)

        @pl.when(first_core == 0)
        def _():
            send_in(0, 7)

        rest_loaded()
        send_in(1, 6)

        @pl.when(is_inner)
        def _():
            with jax.named_scope("ent0"):
                pl.semaphore_wait(entered.at[0], 1)

        @pl.when(first_core == 1)
        def _():
            send_in(0, 7)

        for k in [4, 5] + near:
            send_in(0, k)
        with jax.named_scope("ent1"):

            @pl.when(beside == 1)
            def _():
                pl.semaphore_wait(entered.at[1], 2)
                tell(entered.at[2], "segment", seg, 1)

            pl.semaphore_wait(entered.at[2], 1)

            @pl.when(relays == 1)
            def _():
                for k in (6, 7, 1):
                    tell(entered.at[2], "amp", amp, k)
    else:
        pl.semaphore_wait(barrier, peers - 1 + sections - 1)
        far_loaded(0)
        far_loaded(1)
        rest_loaded()
        for group in groups:
            for k in group:
                send_in(0, k)
    for k in range(1, sections):
        pltpu.make_async_remote_copy(
            src_ref=gates.at[seg],
            dst_ref=gates.at[seg],
            send_sem=sent,
            recv_sem=grecv,
            device_id={"segment": partner(seg, k)},
            device_id_type=MESH,
        ).start()
    for chunk in range(1, chunks):
        for k in far + mid + near:
            if not (line and chunk == 1 and k == 6):
                send_in(chunk, k)
    with jax.named_scope("gates"):
        waits(gates.at[1:], grecv)

    rows_at = lax.broadcasted_iota(jnp.int32, (reg, reg), 0)
    columns_at = lax.broadcasted_iota(jnp.int32, (reg, reg), 1)
    identity = jnp.where(rows_at == columns_at, jnp.float32(1.0), jnp.float32(0.0))

    def build(section, carry):
        low = high = None
        for b in range(blocks):
            factors = row_factors(picks, section, b, qubits, (reg, reg))
            damped = gates[section, b] * factors
            is_low = targets[section, b] == 0
            for_low = jnp.where(is_low, damped, identity)
            for_high = jnp.where(is_low, identity, damped)
            if b == 0:
                low, high = for_low, for_high
            else:
                low = multiply(left_form(for_low), right_form(low))
                high = multiply(left_form(for_high), right_form(high))
        low_form[section] = right_form(low.T)
        high_form[section] = left_form(high)
        return carry

    with jax.named_scope("build"):
        lax.fori_loop(0, sections, build, 0)

    inner = reg // peers
    lanes = lax.broadcasted_iota(jnp.int32, (1, reg), 1)
    partial[...] = jnp.zeros_like(partial)

    def apply_section(chunk, section, swapped):
        low = low_form[section]
        high = high_form[section]
        total = jnp.zeros((8, reg), jnp.float32)
        for slab in range(peers):
            if swapped:
                value = yin[chunk, :, slab * inner : (slab + 1) * inner, :].reshape(reg, reg)
            else:
                value = yin[chunk, slab]
            value = multiply(left_form(value), low)
            value = multiply(high, right_form(value))
            total = total + fold_rows(value)
            if swapped:
                yin[chunk, :, slab * inner : (slab + 1) * inner, :] = value.reshape(
                    peers, inner, reg
                )
            else:
                yin[chunk, slab] = value
        partial[section + 1] = partial[section + 1] + total

    order_out = mid + far + near

    def arrival(chunk, k):
        if not line or k < peers // 2:
            return 0
        return quotient(chunk, chunks - 1) * inner_pair * (1 + k % 2)

    def send_sums(source, target, k, at):
        pltpu.make_async_remote_copy(
            src_ref=sums.at[source],
            dst_ref=sums.at[target],
            send_sem=sent,
            recv_sem=srecv.at[at],
            device_id={"amp": partner(amp, k)},
            device_id_type=MESH,
        ).start()

    def run_chunk(chunk, carry):
        with jax.named_scope("in"):
            waits(xs.at[chunk], irecv.at[chunk])
        first = jnp.zeros((8, reg), jnp.float32)
        for slab in range(peers):
            first = first + fold_rows(yin[chunk, slab])
        partial[0] = partial[0] + first

        def pair(i, inner_carry):
            apply_section(chunk, 2 * i, False)
            apply_section(chunk, 2 * i + 1, True)
            return inner_carry

        with jax.named_scope("comp"):
            lax.fori_loop(0, sections // 2, pair, 0)

        @pl.when(chunk == chunks - 1)
        def _():
            row = jnp.zeros((1, reg), jnp.float32)
            for s in range(sections + 1):
                total = jnp.sum(jnp.sum(partial[s], axis=0, keepdims=True), axis=1, keepdims=True)
                row = jnp.where(lanes == s, total, row)
            sums[pair_at] = row
            for k in range(peers - 2, 0, -2):
                send_sums(pair_at, pair_at, k, 0)

        for k in order_out:
            peer = partner(amp, k)
            pltpu.make_async_remote_copy(
                src_ref=yin.at[chunk, peer],
                dst_ref=ov.at[chunk, amp],
                send_sem=sent,
                recv_sem=orecv.at[arrival(chunk, k)],
                device_id={"amp": peer},
                device_id_type=MESH,
            ).start()
        return carry

    lax.fori_loop(0, chunks, run_chunk, 0)

    chips = peers // 2
    with jax.named_scope("sums"):
        waits(sums.at[1:chips], srecv.at[0])
    part = sums[0]
    for chip in range(1, chips):
        part = part + sums[chip]
    sums[chips] = part
    send_sums(chips, chips + 1, 1, 1)
    with jax.named_scope("join"):
        waits(sums.at[0], srecv.at[1])
    row = part + sums[chips + 1]
    totals = [
        jnp.sum(jnp.where(lanes == s, row, 0.0), axis=1, keepdims=True)
        for s in range(sections + 1)
    ]
    logs = jnp.zeros((1, reg), jnp.float32)
    for s in range(sections):
        logs = jnp.where(lanes == s, jnp.log(totals[s + 1] / totals[s]), logs)
    logs_ref[...] = logs[:, :sections]
    scale = 1.0 / jnp.sqrt(totals[sections] / total_amps)
    scale = jnp.broadcast_to(scale, (1, reg))

    for chunk in range(chunks):
        m = chunk * peers + amp
        out_ref[pl.ds(m, reg, stride=middle), :] = yin[chunk, amp] * scale
    def place(chunk, peer):
        m = chunk * peers + peer
        out_ref[pl.ds(m, reg, stride=middle), :] = ov[chunk, peer] * scale

    last = chunks - 1
    early = chunks * (peers - 1) - (2 if line else 0)
    with jax.named_scope("early"):
        waits(ov.at[:, :, : early * reg // (chunks * peers)], orecv.at[0])
    for chunk in range(last):
        for k in order_out:
            place(chunk, partner(amp, k))
    for k in near:
        place(last, partner(amp, k))
    if line:
        late = [
            inner_pair * partner(amp, 6 + at) + (1 - inner_pair) * partner(amp, 4 + at)
            for at in range(2)
        ]
        soon = [
            inner_pair * partner(amp, 4 + at) + (1 - inner_pair) * partner(amp, 6 + at)
            for at in range(2)
        ]
        for peer in soon:
            place(last, peer)
        for at in range(2):
            with jax.named_scope(f"out_{at}"):
                waits(xs.at[0, 0], orecv.at[1 + at])
            place(last, late[at])
    else:
        for k in far + mid:
            place(last, partner(amp, k))

    with jax.named_scope("sendwait"):
        waits(xs, sent)
        waits(xs, sent)
        waits(gates.at[1:], sent)
        waits(sums.at[:chips], sent)


def store_kernel(pieces, out_vmem, logs_vmem, out_hbm, logs_hbm, out_sem, logs_sem):
    rows = out_vmem.shape[0] // pieces
    for p in range(pieces):
        at = pl.ds(p * rows, rows)
        pltpu.make_async_copy(out_vmem.at[at], out_hbm.at[at], out_sem).start()
    logs_copy = pltpu.make_async_copy(logs_vmem, logs_hbm, logs_sem)
    logs_copy.start()
    pltpu.make_async_copy(out_vmem, out_hbm, out_sem).wait()
    logs_copy.wait()


def step(states, gate_blocks, kraus_picks, block_targets):
    traj_here, amp_local = states.shape
    reg = gate_blocks.shape[-1]
    blocks = gate_blocks.shape[1]
    qubits = kraus_picks.shape[-1]
    peers = lax.axis_size("amp")
    sections = lax.axis_size("segment")
    middle = amp_local // (reg * reg)
    fits = (
        traj_here == 1
        and gate_blocks.shape[0] == 1
        and middle % peers == 0
        and peers & (peers - 1) == 0
        and peers >= 8
        and middle == peers * (peers // 4)
        and middle > peers
        and sections & (sections - 1) == 0
        and sections % 2 == 0
        and sections < 8
        and reg == 128
        and reg % (8 * peers) == 0
    )
    if not fits:
        return body(states, gate_blocks, kraus_picks, block_targets)
    chunks = middle // peers
    kernel = functools.partial(
        circuit_kernel, peers, sections, blocks, qubits, chunks, amp_local * peers
    )
    f32 = jnp.float32
    dma = pltpu.SemaphoreType.DMA
    out, logs = pl.pallas_call(
        kernel,
        out_shape=(
            pltpu.VMEM((reg * middle, reg), f32),
            pltpu.VMEM((1, sections), f32),
        ),
        in_specs=[pl.BlockSpec(memory_space=pl.ANY)] * 4,
        out_specs=(
            pl.BlockSpec(memory_space=pltpu.VMEM),
            pl.BlockSpec(memory_space=pltpu.VMEM),
        ),
        scratch_shapes=[
            pltpu.VMEM((chunks, peers - 1, reg, reg), f32),
            pltpu.VMEM((chunks, peers, reg, reg), f32),
            pltpu.VMEM((chunks, peers, reg, reg), f32),
            pltpu.VMEM((sections, blocks, reg, reg), f32),
            pltpu.SMEM((1, blocks, sections, qubits), jnp.int32),
            pltpu.SMEM((sections, blocks), jnp.int32),
            pltpu.VMEM((sections, 2 * reg, 2 * reg), jnp.bfloat16),
            pltpu.VMEM((sections, reg, 2 * reg), jnp.bfloat16),
            pltpu.VMEM((sections + 1, 8, reg), f32),
            pltpu.VMEM((peers // 2 + 2, 1, reg), f32),
            dma((3,)),
            dma,
            dma,
            dma((chunks,)),
            dma((3,)),
            dma((2,)),
            pltpu.SemaphoreType.REGULAR((3,)),
        ],
        compiler_params=pltpu.CompilerParams(collective_id=0, has_side_effects=True),
    )(
        states.reshape(reg, middle, 1, reg),
        gate_blocks[0],
        jnp.swapaxes(kraus_picks, 1, 2),
        block_targets,
    )
    pieces = 8
    out, logs = pl.pallas_call(
        functools.partial(store_kernel, pieces),
        out_shape=(
            jax.ShapeDtypeStruct(out.shape, f32),
            jax.ShapeDtypeStruct(logs.shape, f32),
        ),
        in_specs=[pl.BlockSpec(memory_space=pltpu.VMEM)] * 2,
        out_specs=(pl.BlockSpec(memory_space=pl.ANY),) * 2,
        scratch_shapes=[dma, dma],
    )(
        pltpu.with_memory_space_constraint(out, pltpu.VMEM),
        pltpu.with_memory_space_constraint(logs, pltpu.VMEM),
    )
    return out.reshape(1, amp_local), logs


def solution(mesh):
    in_specs = (
        P("segment", "amp"),
        P("segment", None, None, None),
        P("segment", None, None, None),
        P(),
    )
    out_specs = (P("segment", "amp"), P("segment", None))
    return jax.shard_map(step, mesh=mesh, in_specs=in_specs, out_specs=out_specs, check_vma=False)
```

```python
import functools

import jax
import jax.numpy as jnp
from jax import lax
from jax.experimental import pallas as pl
from jax.experimental.pallas import tpu as pltpu
from jax.sharding import PartitionSpec as P

KEEP_FACTORS = (1.0, 0.9, 1.0, 0.97)
FLIP_FACTORS = (0.9, 1.0, 0.97, 1.0)
MESH = pl.DeviceIdType.MESH


def broadcast(block, axis, owner):
    block = jnp.where(lax.axis_index(axis) == owner, block, jnp.zeros_like(block))
    return lax.psum(block, axis)


def noise_factors(kraus_rows):
    qubit_count = kraus_rows.shape[-1]
    register = 2**qubit_count
    positions = jnp.arange(register, dtype=jnp.int32)
    product = jnp.ones(kraus_rows.shape[:-1] + (register,), jnp.float32)
    for qubit_pos in range(qubit_count):
        bit_value = jnp.right_shift(positions, qubit_count - 1 - qubit_pos) & 1
        column = kraus_rows[..., qubit_pos : qubit_pos + 1]
        low_value = jnp.zeros(column.shape, jnp.float32)
        high_value = jnp.zeros(column.shape, jnp.float32)
        for option in range(4):
            picked = (column == option).astype(jnp.float32)
            low_value = low_value + picked * KEEP_FACTORS[option]
            high_value = high_value + picked * FLIP_FACTORS[option]
        product = product * jnp.where(bit_value == 1, high_value, low_value)
    return product


def apply_gate(amplitudes, matrix, factors, target):

    def on_low(values):
        mixed_rows = jnp.einsum("bhmk,ik->bhmi", values, matrix, precision=lax.Precision.HIGHEST)
        return mixed_rows * factors[:, None, None, :]

    def on_high(values):
        mixed_rows = jnp.einsum("bjmk,ij->bimk", values, matrix, precision=lax.Precision.HIGHEST)
        return mixed_rows * factors[:, :, None, None]

    return lax.cond(target == 0, on_low, on_high, amplitudes)


def square_sums(values):
    return (values, jnp.sum(values * values, axis=(1, 2, 3)))


def body(states, gate_blocks, kraus_picks, block_targets):
    traj_here = states.shape[0]
    amp_local = states.shape[1]
    register = gate_blocks.shape[-1]
    blocks = gate_blocks.shape[1]
    middle = amp_local // (register * register)
    total_amps = amp_local * lax.axis_size("amp")
    sections = lax.axis_size("segment")
    amplitudes = states.reshape(traj_here, register, middle, register)
    first_local = jnp.sum(amplitudes * amplitudes, axis=(1, 2, 3))
    local_sums = [first_local]
    for section in range(sections):
        section_gates = broadcast(gate_blocks, "segment", section)[0]
        for block_pos in range(blocks):
            factors = noise_factors(kraus_picks[:, section, block_pos, :])
            amplitudes = apply_gate(
                amplitudes, section_gates[block_pos], factors, block_targets[section, block_pos]
            )
        amplitudes, local_sq = square_sums(
            lax.all_to_all(amplitudes, "amp", split_axis=1, concat_axis=1, tiled=True)
        )
        local_sums.append(local_sq)
    totals = lax.psum(jnp.stack(local_sums, axis=1), "amp")
    log_weights = jnp.log(totals[:, 1:] / totals[:, :-1])
    amplitudes = amplitudes / jnp.sqrt(totals[:, -1] / total_amps)[:, None, None, None]
    return (amplitudes.reshape(traj_here, amp_local), log_weights)


def quotient(index, divisor):
    return index if divisor == 1 else lax.div(index, jnp.int32(divisor))


def partner(index, k):
    result = index
    bit = 1
    while bit <= k:
        if k & bit:
            result = result + bit * (1 - 2 * lax.rem(quotient(index, bit), jnp.int32(2)))
        bit *= 2
    return result


def split(values):
    high = values.astype(jnp.bfloat16)
    low = (values - high.astype(jnp.float32)).astype(jnp.bfloat16)
    return high, low


def left_form(matrix):
    return jnp.concatenate(split(matrix), axis=1)


def right_form(matrix):
    row = jnp.concatenate(split(matrix), axis=1)
    return jnp.concatenate([row, row], axis=0)


def multiply(left, right):
    both = jnp.dot(left, right, preferred_element_type=jnp.float32)
    half = both.shape[1] // 2
    return both[:, :half] + both[:, half:]


def fold_rows(values):
    squares = values * values
    return jnp.sum(squares.reshape(-1, 8, squares.shape[-1]), axis=0)


def row_factors(picks_ref, section, block, qubits, shape):
    positions = lax.broadcasted_iota(jnp.int32, shape, 0)
    product = jnp.ones(shape, jnp.float32)
    for q in range(qubits):
        pick = picks_ref[0, block, section, q]
        keep = jnp.float32(KEEP_FACTORS[0])
        flip = jnp.float32(FLIP_FACTORS[0])
        for option in range(1, 4):
            keep = jnp.where(pick == option, jnp.float32(KEEP_FACTORS[option]), keep)
            flip = jnp.where(pick == option, jnp.float32(FLIP_FACTORS[option]), flip)
        bit = jnp.right_shift(positions, qubits - 1 - q) & 1
        product = product * jnp.where(bit == 1, flip, keep)
    return product


def waits(like, semaphore):
    pltpu.make_async_copy(like, like, semaphore).wait()


def circuit_kernel(
    peers, sections, blocks, qubits, chunks, total_amps,
    x_hbm, gates_hbm, picks_hbm, targets_hbm,
    out_ref, logs_ref,
    xs, yin, ov, gates, picks, targets, low_form, high_form, partial, sums,
    x_sem, sent, grecv, irecv, orecv, srecv,
    entered,
):
    seg = lax.axis_index("segment")
    amp = lax.axis_index("amp")
    reg = gates.shape[-1]
    middle = chunks * peers
    far = list(range(3 * peers // 4, peers))
    mid = list(range(peers // 2, 3 * peers // 4))
    near = list(range(peers // 2 - 1, 0, -1))
    groups = [far, mid, near]

    def tell(semaphore, axis, index, k):
        pl.semaphore_signal(
            semaphore, inc=1, device_id={axis: partner(index, k)}, device_id_type=MESH
        )

    eighth = reg // 8
    edges = [0, 1, 3, 5, 8]
    parts = [pl.ds(a * eighth, (b - a) * eighth) for a, b in zip(edges, edges[1:])]
    first, others = parts[0], pl.ds(eighth, reg - eighth)

    def load(chunk, k, semaphore, rows=pl.ds(0, reg)):
        m = chunk * peers + partner(amp, k)
        pltpu.make_async_copy(
            x_hbm.at[rows, m, 0], xs.at[chunk, k - 1, rows], semaphore
        ).start()

    for q, rows in enumerate(parts):
        load(0, far[0], x_sem.at[min(q, 1)], rows)
    for k in far[1:]:
        for rows in parts[1:] + parts[:1]:
            load(0, k, x_sem.at[3], rows)

    barrier = pltpu.get_barrier_semaphore()
    line = peers == 8 and sections == 4
    pair_at = quotient(amp, 2)
    inner_pair = lax.rem(quotient(pair_at + 1, 2), jnp.int32(2))
    is_inner = inner_pair == 1
    first_core = lax.rem(amp, jnp.int32(2)) * inner_pair
    second_core = inner_pair - first_core
    relays = second_core * (1 - quotient(pair_at, 2))
    beside = 1 - inner_pair + relays
    if line:

        tell(barrier, "amp", amp, 6)

        @pl.when(second_core == 0)
        def _():
            tell(barrier, "amp", amp, 7)
            tell(barrier, "amp", amp, 1)

        @pl.when(is_inner)
        def _():
            for k in (2, 3, 4, 5):
                tell(barrier, "amp", amp, k)

        @pl.when(beside == 1)
        def _():
            for k in (1, 2):
                tell(barrier, "segment", seg, k)
    else:
        for k in range(peers - 1, 0, -1):
            tell(barrier, "amp", amp, k)
        for k in range(1, sections):
            tell(barrier, "segment", seg, k)

    for k in mid + near:
        load(0, k, x_sem.at[2])
    for chunk in range(1, chunks):
        for k in far + mid + near:
            load(chunk, k, x_sem.at[2])
    pltpu.make_async_copy(gates_hbm, gates.at[seg], x_sem.at[2]).start()
    picks_load = pltpu.make_async_copy(picks_hbm, picks, x_sem.at[2])
    picks_load.start()
    targets_load = pltpu.make_async_copy(targets_hbm, targets, x_sem.at[2])
    targets_load.start()
    for chunk in range(chunks):
        pltpu.make_async_copy(
            x_hbm.at[:, chunk * peers + amp, 0], yin.at[chunk, amp], x_sem.at[2]
        ).start()

    def send_in(chunk, k, rows=pl.ds(0, reg)):
        pltpu.make_async_remote_copy(
            src_ref=xs.at[chunk, k - 1, rows],
            dst_ref=yin.at[chunk, amp, rows],
            send_sem=sent,
            recv_sem=irecv.at[chunk],
            device_id={"amp": partner(amp, k)},
            device_id_type=MESH,
        ).start()

    def far_loaded(at):
        if at == 0:
            waits(xs.at[0, 0, first], x_sem.at[0])
        else:
            waits(xs.at[0, 0, others], x_sem.at[1])

    def rest_loaded():
        waits(xs, x_sem.at[2])
        waits(gates.at[0], x_sem.at[2])
        picks_load.wait()
        targets_load.wait()

    if line:
        with jax.named_scope("barrier"):
            pl.semaphore_wait(
                barrier, 9 - 4 * inner_pair - 4 * first_core - 2 * (second_core - relays)
            )

        @pl.when(beside == 1)
        def _():
            for k in (1, 2):
                tell(entered.at[1], "segment", seg, k)

        @pl.when(pair_at == peers // 2 - 1)
        def _():
            tell(entered.at[0], "amp", amp, 2)
            tell(entered.at[0], "amp", amp, 4)

        for at, rows in enumerate((first, others)):
            with jax.named_scope("load0"):
                far_loaded(at)
            send_in(0, 6, rows)
        waits(xs.at[0, : len(far) - 1], x_sem.at[3])

        @pl.when(first_core == 0)
        def _():
            send_in(0, 7)

        rest_loaded()
        send_in(1, 6)

        @pl.when(is_inner)
        def _():
            with jax.named_scope("ent0"):
                pl.semaphore_wait(entered.at[0], 1)

        @pl.when(first_core == 1)
        def _():
            send_in(0, 7)

        for k in [4, 5] + near:
            send_in(0, k)
        with jax.named_scope("ent1"):

            @pl.when(beside == 1)
            def _():
                pl.semaphore_wait(entered.at[1], 2)
                tell(entered.at[2], "segment", seg, 1)

            pl.semaphore_wait(entered.at[2], 1)

            @pl.when(relays == 1)
            def _():
                for k in (6, 7, 1):
                    tell(entered.at[2], "amp", amp, k)
    else:
        pl.semaphore_wait(barrier, peers - 1 + sections - 1)
        far_loaded(0)
        far_loaded(1)
        waits(xs.at[0, : len(far) - 1], x_sem.at[3])
        rest_loaded()
        for group in groups:
            for k in group:
                send_in(0, k)
    for k in range(1, sections):
        pltpu.make_async_remote_copy(
            src_ref=gates.at[seg],
            dst_ref=gates.at[seg],
            send_sem=sent,
            recv_sem=grecv,
            device_id={"segment": partner(seg, k)},
            device_id_type=MESH,
        ).start()
    for chunk in range(1, chunks):
        for k in far + mid + near:
            if not (line and chunk == 1 and k == 6):
                send_in(chunk, k)
    with jax.named_scope("gates"):
        waits(gates.at[1:], grecv)

    rows_at = lax.broadcasted_iota(jnp.int32, (reg, reg), 0)
    columns_at = lax.broadcasted_iota(jnp.int32, (reg, reg), 1)
    identity = jnp.where(rows_at == columns_at, jnp.float32(1.0), jnp.float32(0.0))

    def build(section, carry):
        low = high = None
        for b in range(blocks):
            factors = row_factors(picks, section, b, qubits, (reg, reg))
            damped = gates[section, b] * factors
            is_low = targets[section, b] == 0
            for_low = jnp.where(is_low, damped, identity)
            for_high = jnp.where(is_low, identity, damped)
            if b == 0:
                low, high = for_low, for_high
            else:
                low = multiply(left_form(for_low), right_form(low))
                high = multiply(left_form(for_high), right_form(high))
        low_form[section] = right_form(low.T)
        high_form[section] = left_form(high)
        return carry

    with jax.named_scope("build"):
        lax.fori_loop(0, sections, build, 0)

    inner = reg // peers
    lanes = lax.broadcasted_iota(jnp.int32, (1, reg), 1)
    partial[...] = jnp.zeros_like(partial)

    def apply_section(chunk, section, swapped):
        low = low_form[section]
        high = high_form[section]
        total = jnp.zeros((8, reg), jnp.float32)
        for slab in range(peers):
            if swapped:
                value = yin[chunk, :, slab * inner : (slab + 1) * inner, :].reshape(reg, reg)
            else:
                value = yin[chunk, slab]
            value = multiply(left_form(value), low)
            value = multiply(high, right_form(value))
            total = total + fold_rows(value)
            if swapped:
                yin[chunk, :, slab * inner : (slab + 1) * inner, :] = value.reshape(
                    peers, inner, reg
                )
            else:
                yin[chunk, slab] = value
        partial[section + 1] = partial[section + 1] + total

    order_out = mid + far + near

    def arrival(chunk, k):
        if not line or k < peers // 2:
            return 0
        return quotient(chunk, chunks - 1) * inner_pair * (1 + k % 2)

    def send_sums(source, target, k, at):
        pltpu.make_async_remote_copy(
            src_ref=sums.at[source],
            dst_ref=sums.at[target],
            send_sem=sent,
            recv_sem=srecv.at[at],
            device_id={"amp": partner(amp, k)},
            device_id_type=MESH,
        ).start()

    def run_chunk(chunk, carry):
        with jax.named_scope("in"):
            waits(xs.at[chunk], irecv.at[chunk])
        first = jnp.zeros((8, reg), jnp.float32)
        for slab in range(peers):
            first = first + fold_rows(yin[chunk, slab])
        partial[0] = partial[0] + first

        def pair(i, inner_carry):
            apply_section(chunk, 2 * i, False)
            apply_section(chunk, 2 * i + 1, True)
            return inner_carry

        with jax.named_scope("comp"):
            lax.fori_loop(0, sections // 2, pair, 0)

        @pl.when(chunk == chunks - 1)
        def _():
            row = jnp.zeros((1, reg), jnp.float32)
            for s in range(sections + 1):
                total = jnp.sum(jnp.sum(partial[s], axis=0, keepdims=True), axis=1, keepdims=True)
                row = jnp.where(lanes == s, total, row)
            sums[pair_at] = row
            for k in range(peers - 2, 0, -2):
                send_sums(pair_at, pair_at, k, 0)

        for k in order_out:
            peer = partner(amp, k)
            pltpu.make_async_remote_copy(
                src_ref=yin.at[chunk, peer],
                dst_ref=ov.at[chunk, amp],
                send_sem=sent,
                recv_sem=orecv.at[arrival(chunk, k)],
                device_id={"amp": peer},
                device_id_type=MESH,
            ).start()
        return carry

    lax.fori_loop(0, chunks, run_chunk, 0)

    chips = peers // 2
    with jax.named_scope("sums"):
        waits(sums.at[1:chips], srecv.at[0])
    part = sums[0]
    for chip in range(1, chips):
        part = part + sums[chip]
    sums[chips] = part
    send_sums(chips, chips + 1, 1, 1)
    with jax.named_scope("join"):
        waits(sums.at[0], srecv.at[1])
    row = part + sums[chips + 1]
    totals = [
        jnp.sum(jnp.where(lanes == s, row, 0.0), axis=1, keepdims=True)
        for s in range(sections + 1)
    ]
    logs = jnp.zeros((1, reg), jnp.float32)
    for s in range(sections):
        logs = jnp.where(lanes == s, jnp.log(totals[s + 1] / totals[s]), logs)
    logs_ref[...] = logs[:, :sections]
    scale = 1.0 / jnp.sqrt(totals[sections] / total_amps)
    scale = jnp.broadcast_to(scale, (1, reg))

    for chunk in range(chunks):
        m = chunk * peers + amp
        out_ref[pl.ds(m, reg, stride=middle), :] = yin[chunk, amp] * scale
    def place(chunk, peer):
        m = chunk * peers + peer
        out_ref[pl.ds(m, reg, stride=middle), :] = ov[chunk, peer] * scale

    last = chunks - 1
    early = chunks * (peers - 1) - (2 if line else 0)
    with jax.named_scope("early"):
        waits(ov.at[:, :, : early * reg // (chunks * peers)], orecv.at[0])
    for chunk in range(last):
        for k in order_out:
            place(chunk, partner(amp, k))
    for k in near:
        place(last, partner(amp, k))
    if line:
        late = [
            inner_pair * partner(amp, 6 + at) + (1 - inner_pair) * partner(amp, 4 + at)
            for at in range(2)
        ]
        soon = [
            inner_pair * partner(amp, 4 + at) + (1 - inner_pair) * partner(amp, 6 + at)
            for at in range(2)
        ]
        for peer in soon:
            place(last, peer)
        for at in range(2):
            with jax.named_scope(f"out_{at}"):
                waits(xs.at[0, 0], orecv.at[1 + at])
            place(last, late[at])
    else:
        for k in far + mid:
            place(last, partner(amp, k))

    with jax.named_scope("sendwait"):
        waits(xs, sent)
        waits(xs, sent)
        waits(gates.at[1:], sent)
        waits(sums.at[:chips], sent)


def store_kernel(pieces, out_vmem, logs_vmem, out_hbm, logs_hbm, out_sem, logs_sem):
    rows = out_vmem.shape[0] // pieces
    for p in range(pieces):
        at = pl.ds(p * rows, rows)
        pltpu.make_async_copy(out_vmem.at[at], out_hbm.at[at], out_sem).start()
    logs_copy = pltpu.make_async_copy(logs_vmem, logs_hbm, logs_sem)
    logs_copy.start()
    pltpu.make_async_copy(out_vmem, out_hbm, out_sem).wait()
    logs_copy.wait()


def step(states, gate_blocks, kraus_picks, block_targets):
    traj_here, amp_local = states.shape
    reg = gate_blocks.shape[-1]
    blocks = gate_blocks.shape[1]
    qubits = kraus_picks.shape[-1]
    peers = lax.axis_size("amp")
    sections = lax.axis_size("segment")
    middle = amp_local // (reg * reg)
    fits = (
        traj_here == 1
        and gate_blocks.shape[0] == 1
        and middle % peers == 0
        and peers & (peers - 1) == 0
        and peers >= 8
        and middle == peers * (peers // 4)
        and middle > peers
        and sections & (sections - 1) == 0
        and sections % 2 == 0
        and sections < 8
        and reg == 128
        and reg % (8 * peers) == 0
    )
    if not fits:
        return body(states, gate_blocks, kraus_picks, block_targets)
    chunks = middle // peers
    kernel = functools.partial(
        circuit_kernel, peers, sections, blocks, qubits, chunks, amp_local * peers
    )
    f32 = jnp.float32
    dma = pltpu.SemaphoreType.DMA
    out, logs = pl.pallas_call(
        kernel,
        out_shape=(
            pltpu.VMEM((reg * middle, reg), f32),
            pltpu.VMEM((1, sections), f32),
        ),
        in_specs=[pl.BlockSpec(memory_space=pl.ANY)] * 4,
        out_specs=(
            pl.BlockSpec(memory_space=pltpu.VMEM),
            pl.BlockSpec(memory_space=pltpu.VMEM),
        ),
        scratch_shapes=[
            pltpu.VMEM((chunks, peers - 1, reg, reg), f32),
            pltpu.VMEM((chunks, peers, reg, reg), f32),
            pltpu.VMEM((chunks, peers, reg, reg), f32),
            pltpu.VMEM((sections, blocks, reg, reg), f32),
            pltpu.SMEM((1, blocks, sections, qubits), jnp.int32),
            pltpu.SMEM((sections, blocks), jnp.int32),
            pltpu.VMEM((sections, 2 * reg, 2 * reg), jnp.bfloat16),
            pltpu.VMEM((sections, reg, 2 * reg), jnp.bfloat16),
            pltpu.VMEM((sections + 1, 8, reg), f32),
            pltpu.VMEM((peers // 2 + 2, 1, reg), f32),
            dma((4,)),
            dma,
            dma,
            dma((chunks,)),
            dma((3,)),
            dma((2,)),
            pltpu.SemaphoreType.REGULAR((3,)),
        ],
        compiler_params=pltpu.CompilerParams(collective_id=0, has_side_effects=True),
    )(
        states.reshape(reg, middle, 1, reg),
        gate_blocks[0],
        jnp.swapaxes(kraus_picks, 1, 2),
        block_targets,
    )
    pieces = 8
    out, logs = pl.pallas_call(
        functools.partial(store_kernel, pieces),
        out_shape=(
            jax.ShapeDtypeStruct(out.shape, f32),
            jax.ShapeDtypeStruct(logs.shape, f32),
        ),
        in_specs=[pl.BlockSpec(memory_space=pltpu.VMEM)] * 2,
        out_specs=(pl.BlockSpec(memory_space=pl.ANY),) * 2,
        scratch_shapes=[dma, dma],
    )(
        pltpu.with_memory_space_constraint(out, pltpu.VMEM),
        pltpu.with_memory_space_constraint(logs, pltpu.VMEM),
    )
    return out.reshape(1, amp_local), logs


def solution(mesh):
    in_specs = (
        P("segment", "amp"),
        P("segment", None, None, None),
        P("segment", None, None, None),
        P(),
    )
    out_specs = (P("segment", "amp"), P("segment", None))
    return jax.shard_map(step, mesh=mesh, in_specs=in_specs, out_specs=out_specs, check_vma=False)
```
